512 devices in a mesh: gx: 16 (over z, core), gy: 8 (over y), ea: 4 (over x).
Axes of the slice: x: 4, y: 8, z: 8, core: 2. Of those that a mesh axis runs over, the one named last changes fastest.
Arguments:
- load_displacement: float32 [3, 64, 128, 512], P(None, 'gx', 'gy', 'ea'), may hold values from -6 to 6
- load_enriched: float32 [15, 131072], P(None, ('gx', 'gy', 'ea')), may hold values from -24 to 24
- stiffness_shift: float32 [64, 128, 512], P('gx', 'gy', 'ea'), may hold values from 2 to 8
- enriched_diag: float32 [15, 131072], P(None, ('gx', 'gy', 'ea')), may hold values from 11 to 17
- enriched_off: float32 [15, 15, 131072], P(None, None, ('gx', 'gy', 'ea')), may hold values from -0.4 to 0.4
- coupling: float32 [3, 15, 262144], P(None, None, ('gx', 'gy', 'ea')), may hold values from -0.15 to 0.15
- slot_kind: int32 [512, 4, 128], P(('gx', 'gy', 'ea')), may hold values from 0 to 2, as said below
- slot_cell: int32 [512, 4, 128], P(('gx', 'gy', 'ea')), may hold values from 0 to 8191, as said below
- slot_node: int32 [512, 4, 128], P(('gx', 'gy', 'ea')), may hold values from 0 to 255, as said below
Outputs:
- solution_displacement: float32 [3, 64, 128, 512], P(None, 'gx', 'gy', 'ea')
- residual_displacement: float32 [3, 64, 128, 512], P(None, 'gx', 'gy', 'ea')
- solution_enriched: float32 [15, 131072], P(None, ('gx', 'gy', 'ea'))
- residual_enriched: float32 [15, 131072], P(None, ('gx', 'gy', 'ea'))
The draws below stay inside these ranges and needn't reach their ends.
Inputs may be any that keep to these rules, and one draw needn't show every extreme that they name: `slot_kind`: within each block of 128 slots of one device to one owner the slots of kind 1 or 2 come first; in every draw some owner receives 128 such slots from each of the 4 devices of its column. `slot_cell`: distinct within one device. `slot_node`: distinct within each block of 128 slots of one device to one owner.
All inputs are finite; a program needn't handle non-finite values.
Results may differ from the reference program's by a relative error of at most 0.0003.
Values sent between devices are 32-bit elements; how exact they have to be, the bound alone decides.
A program may use at most 64 MiB of HBM per device.

```python
import jax
import jax.numpy as jnp
from jax import lax

CX = 4
CY = 16
CZ = 128
ENB = 256
CAP = 128
ECOMP = 15
ITERS = 3
NX = 64
NY = 128
NZ = 512
NE = 131072
SLOTS = 262144
N_GX = 16
N_GY = 8
N_EA = 4
DEVICES = 512


def draw_slot_cell(key, part):
    device_keys = jax.random.split(jax.random.fold_in(key, 11), DEVICES)

    def one_device(device_key):
        return jax.random.permutation(device_key, CX * CY * CZ)[:N_EA * CAP].astype(jnp.int32)
    return jax.vmap(one_device)(device_keys).reshape(DEVICES, N_EA, CAP)


def draw_slot_node(key, part):
    block_keys = jax.random.split(jax.random.fold_in(key, 17), DEVICES * N_EA)

    def one_block(block_key):
        return jax.random.permutation(block_key, ENB)[:CAP].astype(jnp.int32)
    return jax.vmap(one_block)(block_keys).reshape(DEVICES, N_EA, CAP)


def draw_slot_kind(key, part):
    live_key, kind_key, column_key, owner_key = jax.random.split(jax.random.fold_in(key, 29), 4)
    live_count = jax.random.randint(live_key, (DEVICES, N_EA), CAP // 8, CAP + 1)
    columns = DEVICES // N_EA
    column = jax.random.randint(column_key, (), 0, columns)
    target = jax.random.randint(owner_key, (), 0, N_EA)
    device_ids = jnp.arange(DEVICES, dtype=jnp.int32)[:, None]
    owner_ids = jnp.arange(N_EA, dtype=jnp.int32)[None, :]
    full_block = (device_ids // N_EA == column) & (owner_ids == target)
    live_count = jnp.where(full_block, CAP, live_count)
    slot_kinds = jax.random.randint(kind_key, (DEVICES, N_EA, CAP), 1, 3)
    position = jnp.arange(CAP, dtype=jnp.int32)[None, None, :]
    return jnp.where(position < live_count[:, :, None], slot_kinds, 0).astype(jnp.int32)


def shard_levels(own_key, extent, cuts, low, largest):
    gain, own = 1.0, jax.random.fold_in(own_key, 6)
    for dim, blocks in cuts:
        steps = jnp.exp(jax.random.uniform(jax.random.fold_in(own, dim), (blocks,), jnp.float32, low / len(cuts), largest / len(cuts)))
        gain = gain * jnp.repeat(steps, extent[dim] // blocks).reshape([-1 if axis == dim else 1 for axis in range(len(extent))])
    return gain


def gaussian(own_key, extent, spread, limit, cuts=(), kind=jnp.bfloat16):
    loudness = shard_levels(own_key, extent, cuts, -0.22, 0.18) if cuts else 1.0
    entries = jax.random.normal(own_key, extent, jnp.float32) * spread * loudness
    return jnp.minimum(jnp.maximum(entries, -limit), limit).astype(kind)


def setup_inputs(seed: int = 0) -> dict:
    seeds = jax.random.split(jax.random.key(seed), 10)
    load_displacement = gaussian(seeds[0], (3, NX, NY, NZ), 1.0, 6.0, ((1, 16), (2, 8), (3, 4)), jnp.float32)
    load_enriched = gaussian(seeds[1], (ECOMP, NE), 4.0, 24.0, ((1, 512),), jnp.float32)
    stiffness_shift = jnp.clip(2.0 + 6.0 * jax.random.uniform(seeds[2], (NX, NY, NZ), jnp.float32) ** shard_levels(seeds[2], (NX, NY, NZ), ((0, 16), (1, 8), (2, 4)), -0.2, 0.2), 2.0, 8.0)
    enriched_diag = jnp.clip(11.0 + 6.0 * jax.random.uniform(seeds[3], (ECOMP, NE), jnp.float32) ** shard_levels(seeds[3], (ECOMP, NE), ((1, 512),), -0.2, 0.2), 11.0, 17.0)
    enriched_off = jnp.clip(jax.random.uniform(seeds[4], (ECOMP, ECOMP, NE), jnp.float32, -0.4, 0.4) * shard_levels(seeds[4], (ECOMP, ECOMP, NE), ((2, 512),), -0.4, 0.0), -0.4, 0.4)
    coupling = jnp.clip(jax.random.uniform(seeds[5], (3, ECOMP, SLOTS), jnp.float32, -0.15, 0.15) * shard_levels(seeds[5], (3, ECOMP, SLOTS), ((2, 512),), -0.4, 0.0), -0.15, 0.15)
    slot_kind = draw_slot_kind(jax.random.fold_in(seeds[9], 71), 0)
    slot_cell = draw_slot_cell(jax.random.fold_in(seeds[9], 71), 0)
    slot_node = draw_slot_node(jax.random.fold_in(seeds[9], 71), 0)
    return {"load_displacement": load_displacement, "load_enriched": load_enriched, "stiffness_shift": stiffness_shift, "enriched_diag": enriched_diag, "enriched_off": enriched_off, "coupling": coupling, "slot_kind": slot_kind, "slot_cell": slot_cell, "slot_node": slot_node}


HIGHEST_PRECISION = lax.Precision.HIGHEST


def stencil(displacement, stiffness_shift):
    padded = jnp.pad(displacement, ((0, 0), (1, 1), (1, 1), (1, 1)))
    beside = padded[:, 2:, 1:-1, 1:-1] + padded[:, :-2, 1:-1, 1:-1]
    beside = beside + padded[:, 1:-1, 2:, 1:-1] + padded[:, 1:-1, :-2, 1:-1]
    beside = beside + padded[:, 1:-1, 1:-1, 2:] + padded[:, 1:-1, 1:-1, :-2]
    return (6.0 + stiffness_shift)[None] * displacement - beside


def enriched_block(enriched_diag, enriched_off):
    components = enriched_diag.shape[0]
    identity = jnp.eye(components, dtype=jnp.float32)
    symmetric = 0.5 * (enriched_off + jnp.transpose(enriched_off, (1, 0, 2)))
    return symmetric * (1.0 - identity)[:, :, None] + identity[:, :, None] * enriched_diag[:, None, :]


def slot_columns(kinds_flat):
    heaviside = (kinds_flat >= 1).astype(jnp.float32)
    tip_mask = (kinds_flat == 2).astype(jnp.float32)
    return jnp.concatenate([jnp.broadcast_to(heaviside, (3, heaviside.shape[0])), jnp.broadcast_to(tip_mask, (12, tip_mask.shape[0]))], axis=0)


def inner(first, second):
    return jnp.sum(first[0] * second[0]) + jnp.sum(first[1] * second[1])


def reference(load_displacement, load_enriched, stiffness_shift, enriched_diag, enriched_off, coupling, slot_kind, slot_cell, slot_node):
    device_ids = jnp.arange(N_GX * N_GY * N_EA, dtype=jnp.int32)[:, None, None]
    owners = jnp.arange(N_EA, dtype=jnp.int32)[None, :, None]
    column_i = device_ids // (N_GY * N_EA)
    column_j = (device_ids // N_EA) % N_GY
    layer_k = device_ids % N_EA
    cell_x = slot_cell // (CY * CZ)
    cell_y = (slot_cell // CZ) % CY
    cell_z = slot_cell % CZ
    global_cell = (((column_i * CX + cell_x) * NY + column_j * CY + cell_y) * NZ + layer_k * CZ + cell_z).reshape(-1).astype(jnp.int32)
    global_node = ((device_ids - layer_k + owners) * ENB + slot_node).reshape(-1).astype(jnp.int32)
    slot_weights = coupling * slot_columns(slot_kind.reshape(-1))[None]
    enriched_stiff = enriched_block(enriched_diag, enriched_off)
    cell_total = NX * NY * NZ

    def operate(direction):
        displacement, enriched = direction
        flat = displacement.reshape(3, cell_total)
        picked = flat[:, global_cell]
        to_nodes = jnp.einsum('ijs,is->js', slot_weights, picked, precision=HIGHEST_PRECISION)
        pushed_enriched = jnp.einsum('ijn,jn->in', enriched_stiff, enriched, precision=HIGHEST_PRECISION)
        pushed_enriched = pushed_enriched + jnp.zeros(enriched.shape, jnp.float32).at[:, global_node].add(to_nodes)
        values = enriched[:, global_node]
        to_cells = jnp.einsum('ijs,js->is', slot_weights, values, precision=HIGHEST_PRECISION)
        added = jnp.zeros((3, cell_total), jnp.float32).at[:, global_cell].add(to_cells)
        pushed_displacement = stencil(displacement, stiffness_shift) + added.reshape(displacement.shape)
        return (pushed_displacement, pushed_enriched)

    solution = (jnp.zeros_like(load_displacement), jnp.zeros_like(load_enriched))
    residual = (load_displacement, load_enriched)
    direction = residual
    norm_now = inner(residual, residual)
    for iteration in range(ITERS):
        image = operate(direction)
        alpha = norm_now / inner(direction, image)
        solution = jax.tree.map(lambda member, partner: member + alpha * partner, solution, direction)
        residual = jax.tree.map(lambda member, partner: member - alpha * partner, residual, image)
        norm_next = inner(residual, residual)
        ratio = norm_next / norm_now
        direction = jax.tree.map(lambda member, partner: member + ratio * partner, residual, direction)
        norm_now = norm_next
    return solution[0], residual[0], solution[1], residual[1]
```

```python
import functools

import jax
import jax.numpy as jnp
from jax import lax
from jax.experimental import pallas as pl
from jax.experimental.pallas import tpu as pltpu
from jax.sharding import PartitionSpec as P

ITERS = 3
COMP = 3
CX = 4
CY = 16
CZ = 128
ROWS = CX * CY
FACES = COMP * CX
ECOMP = 15
EPAD = 16
ENB = 256
OWNERS = 4
CAP = 128
SLOTS = OWNERS * CAP
MOMENTS = 6

CENTER = 12.0
SPREAD = 8.0
INV = 1.0 / SPREAD

F32 = jnp.float32
BF16 = jnp.bfloat16
GX_GY_EA = ("gx", "gy", "ea")
AXES = ("gx", "gy", "ea")


def two_parts(x):
    high = x.astype(BF16)
    low = (x - high.astype(F32)).astype(BF16)
    return high, low


def dot_nn(a, b):
    return lax.dot_general(a, b, (((1,), (0,)), ((), ())), preferred_element_type=F32)


def dot_nt(a, b):
    return lax.dot_general(a, b, (((1,), (1,)), ((), ())), preferred_element_type=F32)


def iota(shape, dim):
    return lax.broadcasted_iota(jnp.int32, shape, dim)


def kernel(
    sizes,
    v_in,
    w_in,
    shift_in,
    diag_in,
    off_in,
    coup_in,
    kind_in,
    cell_in,
    node_in,
    sol_v,
    res_v,
    sol_w,
    res_w,
    v,
    w_first,
    shift,
    diag,
    off,
    coup,
    kind,
    cell,
    node,
    acc,
    wbuf,
    weights,
    stiff,
    lane_hot,
    row_hot,
    node_hot,
    spread_rows,
    tsend,
    trecv,
    hx,
    hy,
    hz,
    sy,
    sz,
    red_gx,
    red_gy,
    red_ea,
    in_sem,
    halo_send,
    halo_recv,
    w_send,
    w_recv,
    t_send,
    t_recv,
    gx_send,
    gx_recv,
    gy_send,
    gy_recv,
    ea_send,
    ea_recv,
):
    me = {a: lax.axis_index(a) for a in AXES}
    ea = me["ea"]

    def other(axis, d):
        return lax.rem(me[axis] + d, sizes[axis])

    loads = [
        pltpu.make_async_copy(src, dst, in_sem.at[n])
        for n, (src, dst) in enumerate(
            (
                (cell_in, cell),
                (node_in, node),
                (kind_in, kind),
                (v_in, v.at[0]),
                (w_in, w_first),
                (coup_in, coup),
                (shift_in, shift),
                (diag_in, diag),
                (off_in, off),
            )
        )
    ]
    for load in loads:
        load.start()

    low_edge = [me[a] == 0 for a in AXES]
    high_edge = [me[a] == sizes[a] - 1 for a in AXES]
    halos = (hx, hy, hz)
    for n in range(3):

        @pl.when(low_edge[n])
        def _():
            halos[n][:, 0] = jnp.zeros_like(halos[n][:, 0])

        @pl.when(high_edge[n])
        def _():
            halos[n][:, 1] = jnp.zeros_like(halos[n][:, 1])

    barrier = pltpu.get_barrier_semaphore()
    peers = 0
    for a in AXES:
        for d in range(1, sizes[a]):
            pl.semaphore_signal(
                barrier,
                inc=1,
                device_id={a: other(a, d)},
                device_id_type=pl.DeviceIdType.MESH,
            )
            peers += 1

    def remote(src, dst, send_sem, recv_sem, axis, d):
        return pltpu.make_async_remote_copy(
            src_ref=src,
            dst_ref=dst,
            send_sem=send_sem,
            recv_sem=recv_sem,
            device_id={axis: other(axis, d)},
            device_id_type=pl.DeviceIdType.MESH,
        )

    def halo_copies(k):
        sources = (
            (v.at[k, :, CX - 1], v.at[k, :, 0]),
            (sy.at[k, 0], sy.at[k, 1]),
            (sz.at[k, 0], sz.at[k, 1]),
        )
        copies = []
        for n, a in enumerate(AXES):
            for side, d in ((0, 1), (1, sizes[a] - 1)):
                copies.append(
                    remote(
                        sources[n][side],
                        halos[n].at[k, side],
                        halo_send.at[k, 2 * n + side],
                        halo_recv.at[k, 2 * n + side],
                        a,
                        d,
                    )
                )
        return copies

    def w_copies(k):
        return [
            remote(
                wbuf.at[k, ea], wbuf.at[k, ea], w_send.at[k, d - 1], w_recv.at[k, d - 1], "ea", d
            )
            for d in range(1, OWNERS)
        ]

    def t_copies(k):
        return [
            remote(
                tsend.at[k, other("ea", d)],
                trecv.at[k, d - 1],
                t_send.at[k, d - 1],
                t_recv.at[k, d - 1],
                "ea",
                d,
            )
            for d in range(1, OWNERS)
        ]

    def start_halos(k):
        for n, copy in enumerate(halo_copies(k)):
            edge = high_edge[n // 2] if n % 2 == 0 else low_edge[n // 2]

            @pl.when(jnp.logical_not(edge))
            def _():
                copy.start()

    def wait_halos(k):
        for n, copy in enumerate(halo_copies(k)):
            edge = low_edge[n // 2] if n % 2 == 0 else high_edge[n // 2]

            @pl.when(jnp.logical_not(edge))
            def _():
                copy.wait_recv()

    def end_halos(k):
        for n, copy in enumerate(halo_copies(k)):
            edge = high_edge[n // 2] if n % 2 == 0 else low_edge[n // 2]

            @pl.when(jnp.logical_not(edge))
            def _():
                copy.wait_send()

    lane = iota((CY, CZ), 1)
    row = iota((CY, CZ), 0)

    def pack_faces(k):
        last = jnp.zeros((CY, CZ), F32)
        first = jnp.zeros((CY, CZ), F32)
        for g in range(FACES):
            i, x = divmod(g, CX)
            tile = v[k, i, x]
            sy[k, 0, pl.ds(g, 1), :] = v[k, i, x, pl.ds(CY - 1, 1), :]
            sy[k, 1, pl.ds(g, 1), :] = v[k, i, x, pl.ds(0, 1), :]
            last = jnp.where(lane == g, pltpu.roll(tile, g + 1, 1), last)
            first = jnp.where(lane == g, pltpu.roll(tile, g, 1) if g else tile, first)
        sz[k, 0] = last
        sz[k, 1] = first

    row_of = [None] * OWNERS

    def terms_for_nodes(k):
        high, low = two_parts(v[k].reshape(COMP * ROWS, CZ))
        spread = dot_nn(jnp.concatenate([high, low], axis=1), lane_hot[...])
        for o in range(OWNERS):
            cols = slice(o * CAP, (o + 1) * CAP)
            here = iota((ROWS, CAP), 0) == row_of[o]
            term = jnp.zeros((EPAD, CAP), F32)
            for i in range(COMP):
                picked = jnp.sum(
                    jnp.where(here, spread[i * ROWS : (i + 1) * ROWS, cols], 0.0),
                    axis=0,
                    keepdims=True,
                )
                term = term + weights[i, :, cols] * picked
            both = dot_nt(jnp.concatenate(two_parts(term), axis=0), node_hot[o])
            tsend[k, o] = both[:EPAD] + both[EPAD:]

    def terms_for_cells(k):
        for o in range(OWNERS):
            cols = slice(o * CAP, (o + 1) * CAP)
            both = dot_nn(jnp.concatenate(two_parts(wbuf[k, o]), axis=0), node_hot[o])
            value = both[:EPAD] + both[EPAD:]
            for i in range(COMP):
                total = jnp.sum(weights[i, :, cols] * value, axis=0, keepdims=True)
                for part, piece in enumerate(two_parts(jnp.broadcast_to(total, (CY, CAP)))):
                    for x in range(CX):
                        spread_rows[part, i, x, :, cols] = (
                            row_hot[x * CY : (x + 1) * CY, cols] * piece
                        )
        hot = lane_hot[0:CZ, :]
        high = spread_rows[0].reshape(COMP * ROWS, SLOTS)
        low = spread_rows[1].reshape(COMP * ROWS, SLOTS)
        return (dot_nt(high, hot) + dot_nt(low, hot)).reshape(COMP, CX, CY, CZ)

    def inner_part(k):
        for i in range(COMP):
            for x in range(CX):
                tile = v[k, i, x]
                beside = jnp.where(row > 0, pltpu.roll(tile, 1, 0), 0.0)
                beside += jnp.where(row < CY - 1, pltpu.roll(tile, CY - 1, 0), 0.0)
                beside += jnp.where(lane > 0, pltpu.roll(tile, 1, 1), 0.0)
                beside += jnp.where(lane < CZ - 1, pltpu.roll(tile, CZ - 1, 1), 0.0)
                if x > 0:
                    beside += v[k, i, x - 1]
                if x < CX - 1:
                    beside += v[k, i, x + 1]
                acc[i, x] = ((shift[x] + (6.0 - CENTER)) * tile - beside) * INV

    def outer_part(k, added):
        low_z, high_z = hz[k, 0], hz[k, 1]
        for i in range(COMP):
            for x in range(CX):
                g = i * CX + x
                beside = jnp.where(row == 0, hy[k, 0, pl.ds(g, 1), :], 0.0)
                beside += jnp.where(row == CY - 1, hy[k, 1, pl.ds(g, 1), :], 0.0)
                beside += jnp.where(
                    lane == 0, pltpu.roll(low_z, CZ - g, 1) if g else low_z, 0.0
                )
                beside += jnp.where(lane == CZ - 1, pltpu.roll(high_z, CZ - 1 - g, 1), 0.0)
                if x == 0:
                    beside += hx[k, 0, i]
                if x == CX - 1:
                    beside += hx[k, 1, i]
                v[k + 1, i, x] = acc[i, x] + added[i, x] - beside * INV

    def local_product(j, k):
        sum_v = jnp.sum((v[j] * v[k]).reshape(FACES * CY // 8, 8, CZ), axis=0)
        prod = wbuf[j, ea] * wbuf[k, ea]
        sum_w = prod[0:8, 0:128] + prod[0:8, 128:256] + prod[8:16, 0:128] + prod[8:16, 128:256]
        return sum_v + sum_w

    loads[0].wait()
    loads[1].wait()
    loads[2].wait()
    for o in range(OWNERS):
        cols = slice(o * CAP, (o + 1) * CAP)
        cells = cell[0, o : o + 1, :]
        row_of[o] = lax.shift_right_logical(cells, 7)
        hot = (iota((CZ, CAP), 0) == jnp.bitwise_and(cells, CZ - 1)).astype(F32).astype(BF16)
        lane_hot[0:CZ, cols] = hot
        lane_hot[CZ : 2 * CZ, cols] = hot
        row_hot[:, cols] = (iota((ROWS, CAP), 0) == row_of[o]).astype(F32).astype(BF16)
        node_hot[o] = (iota((ENB, CAP), 0) == node[0, o : o + 1, :]).astype(F32).astype(BF16)

    loads[3].wait()
    loads[4].wait()
    for k in range(ITERS + 1):
        wbuf[k, ea, 8:16, :] = jnp.zeros((8, ENB), F32)
    wbuf[0, ea, 0:ECOMP, :] = w_first[...]
    pack_faces(0)
    pl.semaphore_wait(barrier, peers)
    for copy in w_copies(0):
        copy.start()
    start_halos(0)

    loads[5].wait()
    needed = jnp.where(iota((ECOMP, CAP), 0) < 3, 1, 2)
    for o in range(OWNERS):
        cols = slice(o * CAP, (o + 1) * CAP)
        live = kind[0, o : o + 1, :] >= needed
        for i in range(COMP):
            weights[i, 8:16, cols] = jnp.zeros((8, CAP), F32)
            weights[i, 0:ECOMP, cols] = jnp.where(live, coup[i, :, cols], 0.0)

    parts = [None] * MOMENTS
    for k in range(ITERS):
        if k > 0:
            pack_faces(k)
            start_halos(k)
        terms_for_nodes(k)
        for copy in t_copies(k):
            copy.start()
        if k == 0:
            loads[6].wait()
        inner_part(k)
        if k == 0:
            loads[7].wait()
            loads[8].wait()
            comp = iota((ECOMP, ENB), 0)
            for q in range(ECOMP):
                both = (off[q] + off[:, q, :]) * (0.5 * INV)
                own = (diag[...] - CENTER) * INV
                stiff[q] = jnp.where(comp == q, own, both)
        parts[2 * k] = local_product(k, k)
        if k > 0:
            parts[2 * k - 1] = local_product(k - 1, k)
        pushed = jnp.zeros((ECOMP, ENB), F32)
        for q in range(ECOMP):
            pushed = pushed + stiff[q] * wbuf[k, ea, pl.ds(q, 1), :]
        for copy in w_copies(k):
            copy.wait_recv()
        added = terms_for_cells(k) * INV
        wait_halos(k)
        outer_part(k, added)
        for copy in t_copies(k):
            copy.wait_recv()
        terms = tsend[k, ea]
        for d in range(OWNERS - 1):
            terms = terms + trecv[k, d]
        wbuf[k + 1, ea, 0:ECOMP, :] = pushed + terms[0:ECOMP] * INV
        if k + 1 < ITERS:
            for copy in w_copies(k + 1):
                copy.start()
    parts[2 * ITERS - 1] = local_product(ITERS - 1, ITERS)

    at = iota((8, 128), 1)
    tile = jnp.zeros((8, 128), F32)
    for m in range(MOMENTS):
        tile = jnp.where(at == m, jnp.sum(parts[m], axis=1, keepdims=True), tile)
    total = jnp.sum(tile, axis=0, keepdims=True)
    stages = (
        ("gx", red_gx, gx_send, gx_recv),
        ("gy", red_gy, gy_send, gy_recv),
        ("ea", red_ea, ea_send, ea_recv),
    )
    reductions = []
    for a, buf, send_sem, recv_sem in stages:
        mine = buf.at[me[a]]
        mine[...] = total
        copies = [
            remote(mine, mine, send_sem.at[d - 1], recv_sem.at[d - 1], a, d)
            for d in range(1, sizes[a])
        ]
        for copy in copies:
            copy.start()
        for copy in copies:
            copy.wait_recv()
        total = jnp.sum(buf[...], axis=0)
        reductions.extend(copies)

    flat = iota((1, 128), 1)
    mu = [
        jnp.broadcast_to(
            jnp.sum(jnp.where(flat == m, total, 0.0), axis=1, keepdims=True), (1, 128)
        )
        for m in range(MOMENTS)
    ]

    def form(left, right):
        out = None
        for i, p in enumerate(left):
            for j, q in enumerate(right):
                term = p * q * mu[i + j]
                out = term if out is None else out + term
        return out

    zero = jnp.zeros((1, 128), F32)
    sol, res, way = [zero] * ITERS, [zero + 1.0] + [zero] * ITERS, [zero + 1.0]
    norm = mu[0]
    for it in range(ITERS):
        image = [zero] * (it + 2)
        for j, p in enumerate(way):
            image[j] = image[j] + CENTER * p
            image[j + 1] = image[j + 1] + SPREAD * p
        alpha = norm / form(way, image)
        for j, p in enumerate(way):
            sol[j] = sol[j] + alpha * p
        for j, p in enumerate(image):
            res[j] = res[j] - alpha * p
        if it + 1 < ITERS:
            norm_next = form(res[: it + 2], res[: it + 2])
            ratio = norm_next / norm
            way = [res[j] + (ratio * way[j] if j < len(way) else 0.0) for j in range(it + 2)]
            norm = norm_next

    for i in range(COMP):
        for x in range(CX):
            b = [v[k, i, x] for k in range(ITERS + 1)]
            sol_v[i, x] = sum(sol[k] * b[k] for k in range(ITERS))
            res_v[i, x] = sum(res[k] * b[k] for k in range(ITERS + 1))
    spread = [
        (jnp.concatenate([sol[k]] * 2, axis=1) if k < ITERS else None,
         jnp.concatenate([res[k]] * 2, axis=1))
        for k in range(ITERS + 1)
    ]
    b = [wbuf[k, ea, 0:ECOMP, :] for k in range(ITERS + 1)]
    sol_w[...] = sum(spread[k][0] * b[k] for k in range(ITERS))
    res_w[...] = sum(spread[k][1] * b[k] for k in range(ITERS + 1))

    for k in range(ITERS):
        end_halos(k)
        for copy in w_copies(k):
            copy.wait_send()
        for copy in t_copies(k):
            copy.wait_send()
    for copy in reductions:
        copy.wait_send()


def body(sizes, *args):
    v_in, w_in = args[0], args[1]
    vmem, dma = pltpu.VMEM, pltpu.SemaphoreType.DMA
    steps = ITERS
    return pl.pallas_call(
        functools.partial(kernel, sizes),
        name="krylov",
        out_shape=(
            jax.ShapeDtypeStruct(v_in.shape, F32),
            jax.ShapeDtypeStruct(v_in.shape, F32),
            jax.ShapeDtypeStruct(w_in.shape, F32),
            jax.ShapeDtypeStruct(w_in.shape, F32),
        ),
        in_specs=[pl.BlockSpec(memory_space=pl.ANY)] * len(args),
        out_specs=[pl.BlockSpec(memory_space=pltpu.VMEM)] * 4,
        scratch_shapes=[
            vmem((steps + 1, COMP, CX, CY, CZ), F32),
            vmem((ECOMP, ENB), F32),
            vmem((CX, CY, CZ), F32),
            vmem((ECOMP, ENB), F32),
            vmem((ECOMP, ECOMP, ENB), F32),
            vmem((COMP, ECOMP, SLOTS), F32),
            vmem((1, OWNERS, CAP), jnp.int32),
            vmem((1, OWNERS, CAP), jnp.int32),
            vmem((1, OWNERS, CAP), jnp.int32),
            vmem((COMP, CX, CY, CZ), F32),
            vmem((steps + 1, OWNERS, EPAD, ENB), F32),
            vmem((COMP, EPAD, SLOTS), F32),
            vmem((ECOMP, ECOMP, ENB), F32),
            vmem((2 * CZ, SLOTS), BF16),
            vmem((ROWS, SLOTS), BF16),
            vmem((OWNERS, ENB, CAP), BF16),
            vmem((2, COMP, CX, CY, SLOTS), BF16),
            vmem((steps, OWNERS, EPAD, ENB), F32),
            vmem((steps, OWNERS - 1, EPAD, ENB), F32),
            vmem((steps, 2, COMP, CY, CZ), F32),
            vmem((steps, 2, 16, CZ), F32),
            vmem((steps, 2, CY, CZ), F32),
            vmem((steps, 2, 16, CZ), F32),
            vmem((steps, 2, CY, CZ), F32),
            vmem((sizes["gx"], 1, 128), F32),
            vmem((sizes["gy"], 1, 128), F32),
            vmem((sizes["ea"], 1, 128), F32),
            dma((len(args),)),
            dma((steps, 6)),
            dma((steps, 6)),
            dma((steps, OWNERS - 1)),
            dma((steps, OWNERS - 1)),
            dma((steps, OWNERS - 1)),
            dma((steps, OWNERS - 1)),
            dma((sizes["gx"] - 1,)),
            dma((sizes["gx"] - 1,)),
            dma((sizes["gy"] - 1,)),
            dma((sizes["gy"] - 1,)),
            dma((sizes["ea"] - 1,)),
            dma((sizes["ea"] - 1,)),
        ],
        compiler_params=pltpu.CompilerParams(collective_id=0, has_side_effects=True),
    )(*args)


def solution(mesh):
    sizes = {a: mesh.shape[a] for a in AXES}
    return jax.shard_map(
        functools.partial(body, sizes),
        mesh=mesh,
        in_specs=(
            P(None, "gx", "gy", "ea"),
            P(None, GX_GY_EA),
            P("gx", "gy", "ea"),
            P(None, GX_GY_EA),
            P(None, None, GX_GY_EA),
            P(None, None, GX_GY_EA),
            P(GX_GY_EA, None, None),
            P(GX_GY_EA, None, None),
            P(GX_GY_EA, None, None),
        ),
        out_specs=(
            P(None, "gx", "gy", "ea"),
            P(None, "gx", "gy", "ea"),
            P(None, GX_GY_EA),
            P(None, GX_GY_EA),
        ),
        check_vma=False,
    )
```

```python
import functools

import jax
import jax.numpy as jnp
from jax import lax
from jax.experimental import pallas as pl
from jax.experimental.pallas import tpu as pltpu
from jax.sharding import PartitionSpec as P

ITERS = 3
COMP = 3
CX = 4
CY = 16
CZ = 128
ROWS = CX * CY
FACES = COMP * CX
ECOMP = 15
EPAD = 16
ENB = 256
OWNERS = 4
CAP = 128
SLOTS = OWNERS * CAP
MOMENTS = 6
VMEM_LIMIT = 16 << 20

CENTER = 12.0
SPREAD = 8.0
INV = 1.0 / SPREAD

F32 = jnp.float32
BF16 = jnp.bfloat16
GX_GY_EA = ("gx", "gy", "ea")
AXES = ("gx", "gy", "ea")


def two_parts(x):
    high = x.astype(BF16)
    low = (x - high.astype(F32)).astype(BF16)
    return high, low


def dot_nn(a, b):
    return lax.dot_general(a, b, (((1,), (0,)), ((), ())), preferred_element_type=F32)


def dot_nt(a, b):
    return lax.dot_general(a, b, (((1,), (1,)), ((), ())), preferred_element_type=F32)


def iota(shape, dim):
    return lax.broadcasted_iota(jnp.int32, shape, dim)


def kernel(
    sizes,
    v_in,
    w_in,
    shift_in,
    diag_in,
    off_in,
    coup_in,
    kind_in,
    cell_in,
    node_in,
    v_out,
    w_out,
    moments,
    v,
    w,
    w_first,
    shift,
    diag,
    off,
    coup,
    kind,
    cell,
    node,
    acc,
    weights,
    stiff,
    gather_hot,
    scatter_hot,
    row_hot,
    row_mask,
    node_hot,
    spread_rows,
    wrecv,
    tsend,
    trecv,
    hx,
    hy,
    hz,
    sy,
    sz,
    red_line,
    red_plane,
    in_sem,
    out_sem,
    halo_send,
    halo_recv,
    w_send,
    w_recv,
    t_send,
    t_recv,
    line_send,
    line_recv,
    plane_send,
    plane_recv,
):
    scope = jax.named_scope
    me = {a: lax.axis_index(a) for a in AXES}
    ea = me["ea"]

    def other(axis, d):
        return lax.rem(me[axis] + d, sizes[axis])

    with scope("issue"):
        loads = {
            name: pltpu.make_async_copy(src, dst, in_sem.at[n])
            for n, (name, src, dst) in enumerate(
                (
                    ("cell", cell_in, cell),
                    ("node", node_in, node),
                    ("v", v_in, v.at[0]),
                    ("w", w_in, w_first),
                    ("kind", kind_in, kind),
                    ("coup", coup_in, coup),
                    ("shift", shift_in, shift),
                    ("diag", diag_in, diag),
                    ("off", off_in, off),
                )
            )
        }
        for load in loads.values():
            load.start()

    line = [{"gx": d} for d in range(1, sizes["gx"])]
    plane = [
        {"gy": dy, "ea": dx}
        for dy in range(sizes["gy"])
        for dx in range(sizes["ea"])
        if dy or dx
    ]
    with scope("signals"):
        barrier = pltpu.get_barrier_semaphore()
        for shifts in line + plane:
            pl.semaphore_signal(
                barrier,
                inc=1,
                device_id={a: other(a, d) for a, d in shifts.items()},
                device_id_type=pl.DeviceIdType.MESH,
            )

    low_edge = [me[a] == 0 for a in AXES]
    high_edge = [me[a] == sizes[a] - 1 for a in AXES]
    halos = (hx, hy, hz)
    with scope("edges"):
        for n in range(3):

            @pl.when(low_edge[n])
            def _():
                halos[n][:, 0] = jnp.zeros_like(halos[n][:, 0])

            @pl.when(high_edge[n])
            def _():
                halos[n][:, 1] = jnp.zeros_like(halos[n][:, 1])

    def remote(src, dst, send_sem, recv_sem, shifts):
        return pltpu.make_async_remote_copy(
            src_ref=src,
            dst_ref=dst,
            send_sem=send_sem,
            recv_sem=recv_sem,
            device_id={a: other(a, d) for a, d in shifts.items()},
            device_id_type=pl.DeviceIdType.MESH,
        )

    def halo_copies(k, n):
        sources = (
            (v.at[k, :, CX - 1], v.at[k, :, 0]),
            (sy.at[k, 0], sy.at[k, 1]),
            (sz.at[k, 0], sz.at[k, 1]),
        )
        a = AXES[n]
        return [
            remote(
                sources[n][side],
                halos[n].at[k, side],
                halo_send.at[2 * n + side],
                halo_recv.at[k, 2 * n + side],
                {a: d},
            )
            for side, d in ((0, 1), (1, sizes[a] - 1))
        ]

    def on_halos(k, n, there, act):
        for copy, edge in zip(halo_copies(k, n), there[n]):

            @pl.when(jnp.logical_not(edge))
            def _():
                act(copy)

    going = list(zip(high_edge, low_edge))
    coming = list(zip(low_edge, high_edge))

    def w_copy(k, d):
        return remote(
            w.at[k], wrecv.at[k, d - 1], w_send, w_recv.at[k, d % 2], {"ea": d}
        )

    def t_copy(k, d):
        return remote(
            tsend.at[k, d],
            trecv.at[k, d - 1],
            t_send,
            t_recv.at[k],
            {"ea": d},
        )

    def wait_bytes(ref, sem):
        pltpu.make_async_copy(ref, ref, sem).wait()

    def wait_w(k, distances):
        at = pl.ds(1, 1) if distances == (2,) else pl.ds(0, len(distances))
        wait_bytes(wrecv.at[k, at], w_recv.at[k, distances[0] % 2])

    lane = iota((CY, CZ), 1)
    row = iota((CY, CZ), 0)

    def pack_faces(k):
        last = jnp.zeros((CY, CZ), F32)
        first = jnp.zeros((CY, CZ), F32)
        for g in range(FACES):
            i, x = divmod(g, CX)
            tile = v[k, i, x]
            sy[k, 0, pl.ds(g, 1), :] = v[k, i, x, pl.ds(CY - 1, 1), :]
            sy[k, 1, pl.ds(g, 1), :] = v[k, i, x, pl.ds(0, 1), :]
            last = jnp.where(lane == g, pltpu.roll(tile, g + 1, 1), last)
            first = jnp.where(lane == g, pltpu.roll(tile, g, 1) if g else tile, first)
        sz[k, 0] = last
        sz[k, 1] = first

    def terms_for_nodes(k):
        both_parts = jnp.concatenate(two_parts(v[k].reshape(COMP * ROWS, CZ)), axis=1)
        owners = [other("ea", d) for d in range(OWNERS)]
        order = (2, 1, 3, 0)
        spread = {d: dot_nn(both_parts, gather_hot[owners[d]]) for d in order}
        term = {}
        for d in order:
            here = row_mask[owners[d]]
            term[d] = jnp.zeros((EPAD, CAP), F32)
            for i in range(COMP):
                rows = spread[d][i * ROWS : (i + 1) * ROWS]
                picked = jnp.sum(rows * here, axis=0, keepdims=True)
                term[d] = term[d] + weights[owners[d], i] * picked
        both = {
            d: dot_nt(jnp.concatenate(two_parts(term[d]), axis=0), node_hot[owners[d]])
            for d in order
        }
        for d in order:
            tsend[k, d] = both[d][:EPAD] + both[d][EPAD:]

    def terms_for_cells(k, distances):
        owners = {d: other("ea", OWNERS - d) for d in distances}
        both = {}
        for d in distances:
            values = w[k] if d == 0 else wrecv[k, d - 1]
            both[d] = dot_nn(jnp.concatenate(two_parts(values), axis=0), node_hot[owners[d]])
        for d in distances:
            value = both[d][:EPAD] + both[d][EPAD:]
            hot = row_hot[owners[d]]
            for i in range(COMP):
                total = jnp.sum(weights[owners[d], i] * value, axis=0, keepdims=True)
                for part, piece in enumerate(two_parts(jnp.broadcast_to(total, (CY, CAP)))):
                    for x in range(CX):
                        spread_rows[d, i, x, :, part * CAP : (part + 1) * CAP] = (
                            hot[x * CY : (x + 1) * CY] * piece
                        )
        added = sum(
            dot_nt(spread_rows[d].reshape(COMP * ROWS, 2 * CAP), scatter_hot[owners[d]])
            for d in distances
        )
        return added.reshape(COMP, CX, CY, CZ)

    def inner_part(k):
        for i in range(COMP):
            for x in range(CX):
                tile = v[k, i, x]
                beside = jnp.where(row > 0, pltpu.roll(tile, 1, 0), 0.0)
                beside += jnp.where(row < CY - 1, pltpu.roll(tile, CY - 1, 0), 0.0)
                beside += jnp.where(lane > 0, pltpu.roll(tile, 1, 1), 0.0)
                beside += jnp.where(lane < CZ - 1, pltpu.roll(tile, CZ - 1, 1), 0.0)
                if x > 0:
                    beside += v[k, i, x - 1]
                if x < CX - 1:
                    beside += v[k, i, x + 1]
                acc[i, x] = ((shift[x] + (6.0 - CENTER)) * tile - beside) * INV

    def outer_part(k, target):
        low_z, high_z = hz[k, 0], hz[k, 1]
        for i in range(COMP):
            for x in range(CX):
                g = i * CX + x
                beside = jnp.where(row == 0, hy[k, 0, pl.ds(g, 1), :], 0.0)
                beside += jnp.where(row == CY - 1, hy[k, 1, pl.ds(g, 1), :], 0.0)
                beside += jnp.where(
                    lane == 0, pltpu.roll(low_z, CZ - g, 1) if g else low_z, 0.0
                )
                beside += jnp.where(lane == CZ - 1, pltpu.roll(high_z, CZ - 1 - g, 1), 0.0)
                if x == 0:
                    beside += hx[k, 0, i]
                if x == CX - 1:
                    beside += hx[k, 1, i]
                target[i, x] = acc[i, x] - beside * INV

    def fold_v(left, right):
        return jnp.sum((left * right).reshape(FACES * CY // 8, 8, CZ), axis=0)

    def fold_w(prod):
        return prod[0:8, 0:128] + prod[0:8, 128:256] + prod[8:16, 0:128] + prod[8:16, 128:256]

    def local_product(j, k):
        return fold_v(v[j], v[k]) + fold_w(w[j] * w[k])

    with scope("tables_wait"):
        loads["cell"].wait()
        loads["node"].wait()
    with scope("tables"):
        for o in range(OWNERS):
            cells = cell[0, o : o + 1, :]
            hot = (iota((CZ, CAP), 0) == jnp.bitwise_and(cells, CZ - 1)).astype(F32).astype(BF16)
            gather_hot[o, 0:CZ] = hot
            gather_hot[o, CZ : 2 * CZ] = hot
            scatter_hot[o, :, 0:CAP] = hot
            scatter_hot[o, :, CAP : 2 * CAP] = hot
            mask = (iota((ROWS, CAP), 0) == lax.shift_right_logical(cells, 7)).astype(F32)
            row_mask[o] = mask
            row_hot[o] = mask.astype(BF16)
            node_hot[o] = (
                (iota((ENB, CAP), 0) == node[0, o : o + 1, :]).astype(F32).astype(BF16)
            )

    with scope("vw_wait"):
        loads["v"].wait()
        loads["w"].wait()
    with scope("pack_0"):
        for k in range(ITERS + 1):
            w[k, 8:16, :] = jnp.zeros((8, ENB), F32)
        w[0, 0:ECOMP, :] = w_first[...]
        pack_faces(0)
    with scope("weights"):
        loads["kind"].wait()
        loads["coup"].wait()
        needed = jnp.where(iota((ECOMP, CAP), 0) < 3, 1, 2)
        for o in range(OWNERS):
            live = kind[0, o : o + 1, :] >= needed
            for i in range(COMP):
                weights[o, i, 8:16] = jnp.zeros((8, CAP), F32)
                weights[o, i, 0:ECOMP] = jnp.where(
                    live, coup[i, :, o * CAP : (o + 1) * CAP] * INV, 0.0
                )
    with scope("nodes_0"):
        terms_for_nodes(0)
    with scope("barrier_wait"):
        pl.semaphore_wait(barrier, len(line) + len(plane))

    parts = [None] * MOMENTS
    for k in range(ITERS):
        final = k == ITERS - 1
        if k > 0:
            with scope(f"nodes_{k}"):
                pack_faces(k)
                terms_for_nodes(k)
        with scope(f"send_{k}"):
            for d in (2, 1, 3):
                if k == 0:
                    w_copy(0, d).start()
                t_copy(k, d).start()
            for n in range(3):
                on_halos(k, n, going, lambda copy: copy.start())
        with scope(f"inner_{k}"):
            if k == 0:
                loads["shift"].wait()
            inner_part(k)
        if k == 0:
            with scope("stiff"):
                loads["diag"].wait()
                loads["off"].wait()
                comp = iota((ECOMP, ENB), 0)
                for q in range(ECOMP):
                    both = (off[q] + off[:, q, :]) * (0.5 * INV)
                    own = (diag[...] - CENTER) * INV
                    stiff[q] = jnp.where(comp == q, own, both)
        with scope(f"pushed_{k}"):
            parts[2 * k] = local_product(k, k)
            if k > 0:
                parts[2 * k - 1] = local_product(k - 1, k)
            pushed = tsend[k, 0, 0:ECOMP]
            for q in range(ECOMP):
                pushed = pushed + stiff[q] * w[k, pl.ds(q, 1), :]
        if not final:
            with scope(f"cells_{k}"):
                acc[...] += terms_for_cells(k, (0,))
            for distances in ((1, 3), (2,)):
                with scope(f"w_wait_{k}#d={distances[0]}"):
                    wait_w(k, distances)
                with scope(f"cells_{k}#d={distances[0]}"):
                    acc[...] += terms_for_cells(k, distances)
        with scope(f"t_wait_{k}"):
            wait_bytes(trecv.at[k], t_recv.at[k])
        with scope(f"w_next_{k}"):
            came = trecv[k, 0, 0:ECOMP] + trecv[k, 1, 0:ECOMP] + trecv[k, 2, 0:ECOMP]
            pushed = pushed + came
            w[k + 1, 0:ECOMP, :] = pushed
            if not final:
                for d in (2, 1, 3):
                    w_copy(k + 1, d).start()
        with scope(f"halo_wait_{k}"):
            for n in range(3):
                on_halos(k, n, coming, lambda copy: copy.wait_recv())
        with scope(f"outer_{k}"):
            outer_part(k, acc if final else v.at[k + 1])

    with scope("moments"):
        last = ITERS - 1
        twice = tsend[last, 0] + trecv[last, 0] + trecv[last, 1] + trecv[last, 2]
        parts[2 * last + 1] = fold_v(v[last], acc[...]) + fold_w(
            w[last] * (w[last + 1] + twice)
        )
        at = iota((8, 128), 1)
        tile = jnp.zeros((8, 128), F32)
        for m in range(MOMENTS):
            tile = jnp.where(at == m, jnp.sum(parts[m], axis=1, keepdims=True), tile)
        total = jnp.sum(tile, axis=0, keepdims=True)

    def send_total(buf, at, send_sem, recv_sem, group):
        mine = buf.at[at]
        mine[...] = total
        copies = [
            remote(mine, mine, send_sem, recv_sem, shifts)
            for shifts in group
        ]
        for copy in copies:
            copy.start()
        return buf.at[pl.ds(0, len(group))]

    with scope("line_send"):
        on_line = send_total(red_line, me["gx"], line_send, line_recv, line)
    with scope("cells_last"):
        wait_w(last, (1, 3))
        wait_w(last, (2,))
        v[last + 1] = acc[...] + terms_for_cells(last, (0, 1, 3, 2))
    with scope("out_send"):
        out = [
            pltpu.make_async_copy(v, v_out, out_sem.at[0]),
            pltpu.make_async_copy(w, w_out, out_sem.at[1]),
        ]
        for copy in out:
            copy.start()
    with scope("line_wait"):
        wait_bytes(on_line, line_recv)
        total = jnp.sum(red_line[...], axis=0)
    with scope("plane_send"):
        on_plane = send_total(
            red_plane, me["gy"] * sizes["ea"] + ea, plane_send, plane_recv, plane
        )
    with scope("ends"):
        for n in range(3):
            for side, edge in enumerate(going[n]):

                @pl.when(jnp.logical_not(edge))
                def _():
                    wait_bytes(halos[n].at[:, side], halo_send.at[2 * n + side])

        wait_bytes(wrecv, w_send)
        wait_bytes(trecv, t_send)
        wait_bytes(on_line, line_send)
        wait_bytes(v, out_sem.at[0])
        wait_bytes(w, out_sem.at[1])
    with scope("plane_wait"):
        wait_bytes(on_plane, plane_recv)
        moments[...] = jnp.sum(red_plane[...], axis=0)
    with scope("plane_end"):
        wait_bytes(on_plane, plane_send)


def combine(v, w_all, moments, sol_v, res_v, sol_w, res_w):
    total = moments[...]
    flat = iota((1, 128), 1)
    mu = [
        jnp.broadcast_to(
            jnp.sum(jnp.where(flat == m, total, 0.0), axis=1, keepdims=True), (1, 128)
        )
        for m in range(MOMENTS)
    ]

    def form(left, right):
        out = None
        for i, p in enumerate(left):
            for j, q in enumerate(right):
                term = p * q * mu[i + j]
                out = term if out is None else out + term
        return out

    zero = jnp.zeros((1, 128), F32)
    sol, res, way = [zero] * ITERS, [zero + 1.0] + [zero] * ITERS, [zero + 1.0]
    norm = mu[0]
    for it in range(ITERS):
        image = [zero] * (it + 2)
        for j, p in enumerate(way):
            image[j] = image[j] + CENTER * p
            image[j + 1] = image[j + 1] + SPREAD * p
        alpha = norm / form(way, image)
        for j, p in enumerate(way):
            sol[j] = sol[j] + alpha * p
        for j, p in enumerate(image):
            res[j] = res[j] - alpha * p
        if it + 1 < ITERS:
            norm_next = form(res[: it + 2], res[: it + 2])
            ratio = norm_next / norm
            way = [res[j] + (ratio * way[j] if j < len(way) else 0.0) for j in range(it + 2)]
            norm = norm_next

    for i in range(COMP):
        for x in range(CX):
            b = [v[k, i, x] for k in range(ITERS + 1)]
            sol_v[i, x] = sum(sol[k] * b[k] for k in range(ITERS))
            res_v[i, x] = sum(res[k] * b[k] for k in range(ITERS + 1))
    spread = [
        (jnp.concatenate([sol[k]] * 2, axis=1) if k < ITERS else None,
         jnp.concatenate([res[k]] * 2, axis=1))
        for k in range(ITERS + 1)
    ]
    b = [w_all[k, 0:ECOMP, :] for k in range(ITERS + 1)]
    sol_w[...] = sum(spread[k][0] * b[k] for k in range(ITERS))
    res_w[...] = sum(spread[k][1] * b[k] for k in range(ITERS + 1))


def body(sizes, *args):
    v_in, w_in = args[0], args[1]
    vmem, dma = pltpu.VMEM, pltpu.SemaphoreType.DMA
    steps = ITERS
    basis = pl.pallas_call(
        functools.partial(kernel, sizes),
        name="krylov",
        out_shape=(
            vmem((steps + 1, COMP, CX, CY, CZ), F32),
            vmem((steps + 1, EPAD, ENB), F32),
            vmem((1, 128), F32),
        ),
        in_specs=[pl.BlockSpec(memory_space=pl.ANY)] * len(args),
        out_specs=[pl.BlockSpec(memory_space=pl.ANY)] * 2
        + [pl.BlockSpec(memory_space=pltpu.VMEM)],
        scratch_shapes=[
            vmem((steps + 1, COMP, CX, CY, CZ), F32),
            vmem((steps + 1, EPAD, ENB), F32),
            vmem((ECOMP, ENB), F32),
            vmem((CX, CY, CZ), F32),
            vmem((ECOMP, ENB), F32),
            vmem((ECOMP, ECOMP, ENB), F32),
            vmem((COMP, ECOMP, SLOTS), F32),
            vmem((1, OWNERS, CAP), jnp.int32),
            vmem((1, OWNERS, CAP), jnp.int32),
            vmem((1, OWNERS, CAP), jnp.int32),
            vmem((COMP, CX, CY, CZ), F32),
            vmem((OWNERS, COMP, EPAD, CAP), F32),
            vmem((ECOMP, ECOMP, ENB), F32),
            vmem((OWNERS, 2 * CZ, CAP), BF16),
            vmem((OWNERS, CZ, 2 * CAP), BF16),
            vmem((OWNERS, ROWS, CAP), BF16),
            vmem((OWNERS, ROWS, CAP), F32),
            vmem((OWNERS, ENB, CAP), BF16),
            vmem((OWNERS, COMP, CX, CY, 2 * CAP), BF16),
            vmem((steps, OWNERS - 1, EPAD, ENB), F32),
            vmem((steps, OWNERS, EPAD, ENB), F32),
            vmem((steps, OWNERS - 1, EPAD, ENB), F32),
            vmem((steps, 2, COMP, CY, CZ), F32),
            vmem((steps, 2, 16, CZ), F32),
            vmem((steps, 2, CY, CZ), F32),
            vmem((steps, 2, 16, CZ), F32),
            vmem((steps, 2, CY, CZ), F32),
            vmem((sizes["gx"], 1, 128), F32),
            vmem((sizes["gy"] * sizes["ea"], 1, 128), F32),
            dma((len(args),)),
            dma((2,)),
            dma((6,)),
            dma((steps, 6)),
            dma,
            dma((steps, 2)),
            dma,
            dma((steps,)),
            dma,
            dma,
            dma,
            dma,
        ],
        compiler_params=pltpu.CompilerParams(collective_id=0, has_side_effects=True),
    )(*args)
    return pl.pallas_call(
        combine,
        name="combine",
        out_shape=(
            jax.ShapeDtypeStruct(v_in.shape, F32),
            jax.ShapeDtypeStruct(v_in.shape, F32),
            jax.ShapeDtypeStruct(w_in.shape, F32),
            jax.ShapeDtypeStruct(w_in.shape, F32),
        ),
        in_specs=[pl.BlockSpec(memory_space=pltpu.VMEM)] * 3,
        out_specs=[pl.BlockSpec(memory_space=pltpu.VMEM)] * 4,
        compiler_params=pltpu.CompilerParams(vmem_limit_bytes=VMEM_LIMIT),
    )(*(pltpu.with_memory_space_constraint(b, pltpu.VMEM) for b in basis))


def solution(mesh):
    sizes = {a: mesh.shape[a] for a in AXES}
    return jax.shard_map(
        functools.partial(body, sizes),
        mesh=mesh,
        in_specs=(
            P(None, "gx", "gy", "ea"),
            P(None, GX_GY_EA),
            P("gx", "gy", "ea"),
            P(None, GX_GY_EA),
            P(None, None, GX_GY_EA),
            P(None, None, GX_GY_EA),
            P(GX_GY_EA, None, None),
            P(GX_GY_EA, None, None),
            P(GX_GY_EA, None, None),
        ),
        out_specs=(
            P(None, "gx", "gy", "ea"),
            P(None, "gx", "gy", "ea"),
            P(None, GX_GY_EA),
            P(None, GX_GY_EA),
        ),
        check_vma=False,
    )
```

```python
import functools

import jax
import jax.numpy as jnp
from jax import lax
from jax.experimental import pallas as pl
from jax.experimental.pallas import tpu as pltpu
from jax.sharding import PartitionSpec as P

ITERS = 3
COMP = 3
CX = 4
CY = 16
CZ = 128
ROWS = CX * CY
FACES = COMP * CX
ECOMP = 15
EPAD = 16
ENB = 256
OWNERS = 4
CAP = 128
SLOTS = OWNERS * CAP
MOMENTS = 6
VMEM_LIMIT = 16 << 20
TOKENS = 4

CENTER = 12.0
SPREAD = 8.0
INV = 1.0 / SPREAD

F32 = jnp.float32
BF16 = jnp.bfloat16
GX_GY_EA = ("gx", "gy", "ea")
AXES = ("gx", "gy", "ea")


def two_parts(x):
    high = x.astype(BF16)
    low = (x - high.astype(F32)).astype(BF16)
    return high, low


def dot_nn(a, b):
    return lax.dot_general(a, b, (((1,), (0,)), ((), ())), preferred_element_type=F32)


def dot_nt(a, b):
    return lax.dot_general(a, b, (((1,), (1,)), ((), ())), preferred_element_type=F32)


def iota(shape, dim):
    return lax.broadcasted_iota(jnp.int32, shape, dim)


def kernel(
    sizes,
    v_in,
    w_in,
    shift_in,
    diag_in,
    off_in,
    coup_in,
    kind_in,
    cell_in,
    node_in,
    v_out,
    w_out,
    moments,
    v,
    w,
    w_first,
    shift,
    diag,
    off,
    coup,
    kind,
    cell,
    node,
    acc,
    weights,
    stiff,
    gather_hot,
    scatter_hot,
    row_hot,
    row_mask,
    node_hot,
    spread_rows,
    wrecv,
    tsend,
    trecv,
    hx,
    hy,
    hz,
    sy,
    sz,
    red_line,
    red_plane,
    tokens,
    in_sem,
    out_sem,
    halo_send,
    halo_recv,
    w_send,
    w_recv,
    t_send,
    t_recv,
    line_send,
    line_recv,
    plane_send,
    plane_recv,
):
    scope = jax.named_scope
    me = {a: lax.axis_index(a) for a in AXES}
    ea = me["ea"]

    def other(axis, d):
        return lax.rem(me[axis] + d, sizes[axis])

    with scope("issue"):
        loads = {
            name: pltpu.make_async_copy(src, dst, in_sem.at[n])
            for n, (name, src, dst) in enumerate(
                (
                    ("cell", cell_in, cell),
                    ("node", node_in, node),
                    ("v", v_in, v.at[0]),
                    ("w", w_in, w_first),
                    ("kind", kind_in, kind),
                    ("coup", coup_in, coup),
                    ("shift", shift_in, shift),
                    ("diag", diag_in, diag),
                    ("off", off_in, off),
                )
            )
        }
        for load in loads.values():
            load.start()

    line = [{"gx": d} for d in range(1, sizes["gx"])]
    plane = [
        {"gy": dy, "ea": dx}
        for dy in range(sizes["gy"])
        for dx in range(sizes["ea"])
        if dy or dx
    ]
    def near(axis, reach):
        n = sizes[axis]
        steps = sorted({d % n for r in range(1, reach + 1) for d in (r, n - r)} - {0})
        return [{axis: d} for d in steps]

    neighbours = near("gx", 2) + near("gy", 1)
    first = neighbours + near("ea", OWNERS // 2)

    def signal(sem, shifts):
        pl.semaphore_signal(
            sem,
            inc=1,
            device_id={a: other(a, d) for a, d in shifts.items()},
            device_id_type=pl.DeviceIdType.MESH,
        )

    def send_token(t):
        for shifts in neighbours:
            signal(tokens.at[t], shifts)

    def wait_token(t):
        pl.semaphore_wait(tokens.at[t], len(neighbours))

    with scope("signals"):
        barrier = pltpu.get_barrier_semaphore()
        for shifts in first:
            signal(barrier, shifts)

    low_edge = [me[a] == 0 for a in AXES]
    high_edge = [me[a] == sizes[a] - 1 for a in AXES]
    halos = (hx, hy, hz)
    with scope("edges"):
        for n in range(3):

            @pl.when(low_edge[n])
            def _():
                halos[n][:, 0] = jnp.zeros_like(halos[n][:, 0])

            @pl.when(high_edge[n])
            def _():
                halos[n][:, 1] = jnp.zeros_like(halos[n][:, 1])

    def remote(src, dst, send_sem, recv_sem, shifts):
        return pltpu.make_async_remote_copy(
            src_ref=src,
            dst_ref=dst,
            send_sem=send_sem,
            recv_sem=recv_sem,
            device_id={a: other(a, d) for a, d in shifts.items()},
            device_id_type=pl.DeviceIdType.MESH,
        )

    def halo_copies(k, n):
        sources = (
            (v.at[k, :, CX - 1], v.at[k, :, 0]),
            (sy.at[k, 0], sy.at[k, 1]),
            (sz.at[k, 0], sz.at[k, 1]),
        )
        a = AXES[n]
        return [
            remote(
                sources[n][side],
                halos[n].at[k, side],
                halo_send.at[2 * n + side],
                halo_recv.at[k, 2 * n + side],
                {a: d},
            )
            for side, d in ((0, 1), (1, sizes[a] - 1))
        ]

    def on_halos(k, n, there, act):
        for copy, edge in zip(halo_copies(k, n), there[n]):

            @pl.when(jnp.logical_not(edge))
            def _():
                act(copy)

    going = list(zip(high_edge, low_edge))
    coming = list(zip(low_edge, high_edge))

    def w_copy(k, d):
        return remote(
            w.at[k], wrecv.at[k, d - 1], w_send, w_recv.at[k, d % 2], {"ea": d}
        )

    def t_copy(k, d):
        return remote(
            tsend.at[k, d],
            trecv.at[k, d - 1],
            t_send,
            t_recv.at[k],
            {"ea": d},
        )

    def wait_bytes(ref, sem):
        pltpu.make_async_copy(ref, ref, sem).wait()

    def wait_w(k, distances):
        at = pl.ds(1, 1) if distances == (2,) else pl.ds(0, len(distances))
        wait_bytes(wrecv.at[k, at], w_recv.at[k, distances[0] % 2])

    lane = iota((CY, CZ), 1)
    row = iota((CY, CZ), 0)

    def pack_faces(k):
        last = jnp.zeros((CY, CZ), F32)
        first = jnp.zeros((CY, CZ), F32)
        for g in range(FACES):
            i, x = divmod(g, CX)
            tile = v[k, i, x]
            sy[k, 0, pl.ds(g, 1), :] = v[k, i, x, pl.ds(CY - 1, 1), :]
            sy[k, 1, pl.ds(g, 1), :] = v[k, i, x, pl.ds(0, 1), :]
            last = jnp.where(lane == g, pltpu.roll(tile, g + 1, 1), last)
            first = jnp.where(lane == g, pltpu.roll(tile, g, 1) if g else tile, first)
        sz[k, 0] = last
        sz[k, 1] = first

    def terms_for_nodes(k):
        both_parts = jnp.concatenate(two_parts(v[k].reshape(COMP * ROWS, CZ)), axis=1)
        owners = [other("ea", d) for d in range(OWNERS)]
        order = (2, 1, 3, 0)
        spread = {d: dot_nn(both_parts, gather_hot[owners[d]]) for d in order}
        term = {}
        for d in order:
            here = row_mask[owners[d]]
            term[d] = jnp.zeros((EPAD, CAP), F32)
            for i in range(COMP):
                rows = spread[d][i * ROWS : (i + 1) * ROWS]
                picked = jnp.sum(rows * here, axis=0, keepdims=True)
                term[d] = term[d] + weights[owners[d], i] * picked
        both = {
            d: dot_nt(jnp.concatenate(two_parts(term[d]), axis=0), node_hot[owners[d]])
            for d in order
        }
        for d in order:
            tsend[k, d] = both[d][:EPAD] + both[d][EPAD:]

    def terms_for_cells(k, distances):
        owners = {d: other("ea", OWNERS - d) for d in distances}
        both = {}
        for d in distances:
            values = w[k] if d == 0 else wrecv[k, d - 1]
            both[d] = dot_nn(jnp.concatenate(two_parts(values), axis=0), node_hot[owners[d]])
        for d in distances:
            value = both[d][:EPAD] + both[d][EPAD:]
            hot = row_hot[owners[d]]
            for i in range(COMP):
                total = jnp.sum(weights[owners[d], i] * value, axis=0, keepdims=True)
                for part, piece in enumerate(two_parts(jnp.broadcast_to(total, (CY, CAP)))):
                    for x in range(CX):
                        spread_rows[d, i, x, :, part * CAP : (part + 1) * CAP] = (
                            hot[x * CY : (x + 1) * CY] * piece
                        )
        added = sum(
            dot_nt(spread_rows[d].reshape(COMP * ROWS, 2 * CAP), scatter_hot[owners[d]])
            for d in distances
        )
        return added.reshape(COMP, CX, CY, CZ)

    def inner_part(k):
        for i in range(COMP):
            for x in range(CX):
                tile = v[k, i, x]
                beside = jnp.where(row > 0, pltpu.roll(tile, 1, 0), 0.0)
                beside += jnp.where(row < CY - 1, pltpu.roll(tile, CY - 1, 0), 0.0)
                beside += jnp.where(lane > 0, pltpu.roll(tile, 1, 1), 0.0)
                beside += jnp.where(lane < CZ - 1, pltpu.roll(tile, CZ - 1, 1), 0.0)
                if x > 0:
                    beside += v[k, i, x - 1]
                if x < CX - 1:
                    beside += v[k, i, x + 1]
                acc[i, x] = ((shift[x] + (6.0 - CENTER)) * tile - beside) * INV

    def outer_part(k, target):
        low_z, high_z = hz[k, 0], hz[k, 1]
        for i in range(COMP):
            for x in range(CX):
                g = i * CX + x
                beside = jnp.where(row == 0, hy[k, 0, pl.ds(g, 1), :], 0.0)
                beside += jnp.where(row == CY - 1, hy[k, 1, pl.ds(g, 1), :], 0.0)
                beside += jnp.where(
                    lane == 0, pltpu.roll(low_z, CZ - g, 1) if g else low_z, 0.0
                )
                beside += jnp.where(lane == CZ - 1, pltpu.roll(high_z, CZ - 1 - g, 1), 0.0)
                if x == 0:
                    beside += hx[k, 0, i]
                if x == CX - 1:
                    beside += hx[k, 1, i]
                target[i, x] = acc[i, x] - beside * INV

    def fold_v(left, right):
        return jnp.sum((left * right).reshape(FACES * CY // 8, 8, CZ), axis=0)

    def fold_w(prod):
        return prod[0:8, 0:128] + prod[0:8, 128:256] + prod[8:16, 0:128] + prod[8:16, 128:256]

    def local_product(j, k):
        return fold_v(v[j], v[k]) + fold_w(w[j] * w[k])

    with scope("tables_wait"):
        loads["cell"].wait()
        loads["node"].wait()
    with scope("tables"):
        for o in range(OWNERS):
            cells = cell[0, o : o + 1, :]
            hot = (iota((CZ, CAP), 0) == jnp.bitwise_and(cells, CZ - 1)).astype(F32).astype(BF16)
            gather_hot[o, 0:CZ] = hot
            gather_hot[o, CZ : 2 * CZ] = hot
            scatter_hot[o, :, 0:CAP] = hot
            scatter_hot[o, :, CAP : 2 * CAP] = hot
            mask = (iota((ROWS, CAP), 0) == lax.shift_right_logical(cells, 7)).astype(F32)
            row_mask[o] = mask
            row_hot[o] = mask.astype(BF16)
            node_hot[o] = (
                (iota((ENB, CAP), 0) == node[0, o : o + 1, :]).astype(F32).astype(BF16)
            )

    with scope("vw_wait"):
        loads["v"].wait()
        loads["w"].wait()
    with scope("pack_0"):
        for k in range(ITERS + 1):
            w[k, 8:16, :] = jnp.zeros((8, ENB), F32)
        w[0, 0:ECOMP, :] = w_first[...]
        pack_faces(0)
    with scope("weights"):
        loads["kind"].wait()
        loads["coup"].wait()
        needed = jnp.where(iota((ECOMP, CAP), 0) < 3, 1, 2)
        for o in range(OWNERS):
            live = kind[0, o : o + 1, :] >= needed
            for i in range(COMP):
                weights[o, i, 8:16] = jnp.zeros((8, CAP), F32)
                weights[o, i, 0:ECOMP] = jnp.where(
                    live, coup[i, :, o * CAP : (o + 1) * CAP] * INV, 0.0
                )
    with scope("nodes_0"):
        terms_for_nodes(0)
    with scope("barrier_wait"):
        pl.semaphore_wait(barrier, len(first))

    def send_halos(k):
        for n in (2, 1, 0):
            on_halos(k, n, going, lambda copy: copy.start())

    def wait_halos(k):
        for n in range(3):
            on_halos(k, n, coming, lambda copy: copy.wait_recv())

    def send_terms(k):
        for d in (2, 1, 3):
            t_copy(k, d).start()

    def send_w(k):
        for d in (2, 1, 3):
            w_copy(k, d).start()

    def stiff_times(k):
        out = tsend[k, 0, 0:ECOMP]
        for q in range(ECOMP):
            out = out + stiff[q] * w[k, pl.ds(q, 1), :]
        return out

    def next_w(k, pushed):
        wait_bytes(trecv.at[k], t_recv.at[k])
        came = trecv[k, 0, 0:ECOMP] + trecv[k, 1, 0:ECOMP] + trecv[k, 2, 0:ECOMP]
        w[k + 1, 0:ECOMP, :] = pushed + came

    def next_v(k):
        with scope(f"w_wait_{k}"):
            wait_w(k, (1, 3))
        with scope(f"cells_{k}"):
            acc[...] += terms_for_cells(k, (1, 3))
        with scope(f"w_wait_{k}#d=2"):
            wait_w(k, (2,))
        with scope(f"cells_{k}#d=2"):
            acc[...] += terms_for_cells(k, (2,))
        with scope(f"halo_wait_{k}"):
            wait_halos(k)
        with scope(f"outer_{k}"):
            outer_part(k, v.at[k + 1])

    parts = [None] * MOMENTS
    last = ITERS - 1

    with scope("send_0"):
        send_halos(0)
        send_terms(0)
        send_w(0)
        send_token(0)
    with scope("inner_0"):
        loads["shift"].wait()
        inner_part(0)
    with scope("stiff"):
        loads["diag"].wait()
        loads["off"].wait()
        comp = iota((ECOMP, ENB), 0)
        for q in range(ECOMP):
            both = (off[q] + off[:, q, :]) * (0.5 * INV)
            own = (diag[...] - CENTER) * INV
            stiff[q] = jnp.where(comp == q, own, both)
    with scope("pushed_0"):
        pushed = stiff_times(0)
        parts[0] = local_product(0, 0)
        acc[...] += terms_for_cells(0, (0,))
    with scope("w_next_0"):
        next_w(0, pushed)
        send_w(1)
    next_v(0)

    with scope("pack_1"):
        pack_faces(1)
        send_halos(1)
    with scope("token_1"):
        wait_token(0)
        send_token(1)
    with scope("nodes_1"):
        terms_for_nodes(1)
        send_terms(1)
    with scope("inner_1"):
        inner_part(1)
        parts[1] = local_product(0, 1)
        parts[2] = local_product(1, 1)
        acc[...] += terms_for_cells(1, (0,))
        pushed = stiff_times(1)
    next_v(1)

    with scope("nodes_2"):
        pack_faces(2)
        terms_for_nodes(2)
        send_halos(2)
        send_terms(2)
    with scope("token_2"):
        wait_token(1)
        send_token(2)
    with scope("w_next_1"):
        next_w(1, pushed)
        send_w(2)
    with scope("inner_2"):
        inner_part(2)
        parts[3] = local_product(1, 2)
        parts[4] = local_product(2, 2)
        pushed = stiff_times(2)
    with scope("token_3"):
        wait_token(2)
        send_token(3)
    with scope("halo_wait_2"):
        wait_halos(2)
    with scope("outer_2"):
        outer_part(2, acc)
    with scope("w_next_2"):
        next_w(2, pushed)

    with scope("moments"):
        twice = tsend[last, 0] + trecv[last, 0] + trecv[last, 1] + trecv[last, 2]
        parts[2 * last + 1] = fold_v(v[last], acc[...]) + fold_w(
            w[last] * (w[last + 1] + twice)
        )
        at = iota((8, 128), 1)
        tile = jnp.zeros((8, 128), F32)
        for m in range(MOMENTS):
            tile = jnp.where(at == m, jnp.sum(parts[m], axis=1, keepdims=True), tile)
        total = jnp.sum(tile, axis=0, keepdims=True)

    def send_total(buf, at, send_sem, recv_sem, group):
        mine = buf.at[at]
        mine[...] = total
        copies = [
            remote(mine, mine, send_sem, recv_sem, shifts)
            for shifts in group
        ]
        for copy in copies:
            copy.start()
        return buf.at[pl.ds(0, len(group))]

    with scope("token_end"):
        wait_token(TOKENS - 1)
    with scope("line_send"):
        on_line = send_total(red_line, me["gx"], line_send, line_recv, line)
    with scope("cells_last"):
        wait_w(last, (1, 3))
        wait_w(last, (2,))
        v[last + 1] = acc[...] + terms_for_cells(last, (0, 1, 3, 2))
    with scope("out_send"):
        out = [
            pltpu.make_async_copy(v, v_out, out_sem.at[0]),
            pltpu.make_async_copy(w, w_out, out_sem.at[1]),
        ]
        for copy in out:
            copy.start()
    with scope("line_wait"):
        wait_bytes(on_line, line_recv)
        total = jnp.sum(red_line[...], axis=0)
    with scope("plane_send"):
        on_plane = send_total(
            red_plane, me["gy"] * sizes["ea"] + ea, plane_send, plane_recv, plane
        )
    with scope("ends"):
        for n in range(3):
            for side, edge in enumerate(going[n]):

                @pl.when(jnp.logical_not(edge))
                def _():
                    wait_bytes(halos[n].at[:, side], halo_send.at[2 * n + side])

        wait_bytes(wrecv, w_send)
        wait_bytes(trecv, t_send)
        wait_bytes(on_line, line_send)
        wait_bytes(v, out_sem.at[0])
        wait_bytes(w, out_sem.at[1])
    with scope("plane_wait"):
        wait_bytes(on_plane, plane_recv)
        moments[...] = jnp.sum(red_plane[...], axis=0)
    with scope("plane_end"):
        wait_bytes(on_plane, plane_send)


def combine(v, w_all, moments, sol_v, res_v, sol_w, res_w):
    total = moments[...]
    flat = iota((1, 128), 1)
    mu = [
        jnp.broadcast_to(
            jnp.sum(jnp.where(flat == m, total, 0.0), axis=1, keepdims=True), (1, 128)
        )
        for m in range(MOMENTS)
    ]

    def form(left, right):
        out = None
        for i, p in enumerate(left):
            for j, q in enumerate(right):
                term = p * q * mu[i + j]
                out = term if out is None else out + term
        return out

    zero = jnp.zeros((1, 128), F32)
    sol, res, way = [zero] * ITERS, [zero + 1.0] + [zero] * ITERS, [zero + 1.0]
    norm = mu[0]
    for it in range(ITERS):
        image = [zero] * (it + 2)
        for j, p in enumerate(way):
            image[j] = image[j] + CENTER * p
            image[j + 1] = image[j + 1] + SPREAD * p
        alpha = norm / form(way, image)
        for j, p in enumerate(way):
            sol[j] = sol[j] + alpha * p
        for j, p in enumerate(image):
            res[j] = res[j] - alpha * p
        if it + 1 < ITERS:
            norm_next = form(res[: it + 2], res[: it + 2])
            ratio = norm_next / norm
            way = [res[j] + (ratio * way[j] if j < len(way) else 0.0) for j in range(it + 2)]
            norm = norm_next

    for i in range(COMP):
        for x in range(CX):
            b = [v[k, i, x] for k in range(ITERS + 1)]
            sol_v[i, x] = sum(sol[k] * b[k] for k in range(ITERS))
            res_v[i, x] = sum(res[k] * b[k] for k in range(ITERS + 1))
    spread = [
        (jnp.concatenate([sol[k]] * 2, axis=1) if k < ITERS else None,
         jnp.concatenate([res[k]] * 2, axis=1))
        for k in range(ITERS + 1)
    ]
    b = [w_all[k, 0:ECOMP, :] for k in range(ITERS + 1)]
    sol_w[...] = sum(spread[k][0] * b[k] for k in range(ITERS))
    res_w[...] = sum(spread[k][1] * b[k] for k in range(ITERS + 1))


def body(sizes, *args):
    v_in, w_in = args[0], args[1]
    vmem, dma = pltpu.VMEM, pltpu.SemaphoreType.DMA
    steps = ITERS
    basis = pl.pallas_call(
        functools.partial(kernel, sizes),
        name="krylov",
        out_shape=(
            vmem((steps + 1, COMP, CX, CY, CZ), F32),
            vmem((steps + 1, EPAD, ENB), F32),
            vmem((1, 128), F32),
        ),
        in_specs=[pl.BlockSpec(memory_space=pl.ANY)] * len(args),
        out_specs=[pl.BlockSpec(memory_space=pl.ANY)] * 2
        + [pl.BlockSpec(memory_space=pltpu.VMEM)],
        scratch_shapes=[
            vmem((steps + 1, COMP, CX, CY, CZ), F32),
            vmem((steps + 1, EPAD, ENB), F32),
            vmem((ECOMP, ENB), F32),
            vmem((CX, CY, CZ), F32),
            vmem((ECOMP, ENB), F32),
            vmem((ECOMP, ECOMP, ENB), F32),
            vmem((COMP, ECOMP, SLOTS), F32),
            vmem((1, OWNERS, CAP), jnp.int32),
            vmem((1, OWNERS, CAP), jnp.int32),
            vmem((1, OWNERS, CAP), jnp.int32),
            vmem((COMP, CX, CY, CZ), F32),
            vmem((OWNERS, COMP, EPAD, CAP), F32),
            vmem((ECOMP, ECOMP, ENB), F32),
            vmem((OWNERS, 2 * CZ, CAP), BF16),
            vmem((OWNERS, CZ, 2 * CAP), BF16),
            vmem((OWNERS, ROWS, CAP), BF16),
            vmem((OWNERS, ROWS, CAP), F32),
            vmem((OWNERS, ENB, CAP), BF16),
            vmem((OWNERS, COMP, CX, CY, 2 * CAP), BF16),
            vmem((steps, OWNERS - 1, EPAD, ENB), F32),
            vmem((steps, OWNERS, EPAD, ENB), F32),
            vmem((steps, OWNERS - 1, EPAD, ENB), F32),
            vmem((steps, 2, COMP, CY, CZ), F32),
            vmem((steps, 2, 16, CZ), F32),
            vmem((steps, 2, CY, CZ), F32),
            vmem((steps, 2, 16, CZ), F32),
            vmem((steps, 2, CY, CZ), F32),
            vmem((sizes["gx"], 1, 128), F32),
            vmem((sizes["gy"] * sizes["ea"], 1, 128), F32),
            pltpu.SemaphoreType.REGULAR((TOKENS,)),
            dma((len(args),)),
            dma((2,)),
            dma((6,)),
            dma((steps, 6)),
            dma,
            dma((steps, 2)),
            dma,
            dma((steps,)),
            dma,
            dma,
            dma,
            dma,
        ],
        compiler_params=pltpu.CompilerParams(collective_id=0, has_side_effects=True),
    )(*args)
    return pl.pallas_call(
        combine,
        name="combine",
        out_shape=(
            jax.ShapeDtypeStruct(v_in.shape, F32),
            jax.ShapeDtypeStruct(v_in.shape, F32),
            jax.ShapeDtypeStruct(w_in.shape, F32),
            jax.ShapeDtypeStruct(w_in.shape, F32),
        ),
        in_specs=[pl.BlockSpec(memory_space=pltpu.VMEM)] * 3,
        out_specs=[pl.BlockSpec(memory_space=pltpu.VMEM)] * 4,
        compiler_params=pltpu.CompilerParams(vmem_limit_bytes=VMEM_LIMIT),
    )(*(pltpu.with_memory_space_constraint(b, pltpu.VMEM) for b in basis))


def solution(mesh):
    sizes = {a: mesh.shape[a] for a in AXES}
    return jax.shard_map(
        functools.partial(body, sizes),
        mesh=mesh,
        in_specs=(
            P(None, "gx", "gy", "ea"),
            P(None, GX_GY_EA),
            P("gx", "gy", "ea"),
            P(None, GX_GY_EA),
            P(None, None, GX_GY_EA),
            P(None, None, GX_GY_EA),
            P(GX_GY_EA, None, None),
            P(GX_GY_EA, None, None),
            P(GX_GY_EA, None, None),
        ),
        out_specs=(
            P(None, "gx", "gy", "ea"),
            P(None, "gx", "gy", "ea"),
            P(None, GX_GY_EA),
            P(None, GX_GY_EA),
        ),
        check_vma=False,
    )
```

```python
import functools

import jax
import jax.numpy as jnp
from jax import lax
from jax.experimental import pallas as pl
from jax.experimental.pallas import tpu as pltpu
from jax.sharding import PartitionSpec as P

ITERS = 3
COMP = 3
CX = 4
CY = 16
CZ = 128
ROWS = CX * CY
FACES = COMP * CX
ECOMP = 15
EPAD = 16
ENB = 256
OWNERS = 4
CAP = 128
SLOTS = OWNERS * CAP
MOMENTS = 6
VMEM_LIMIT = 16 << 20
TOKENS = 4

CENTER = 12.0
SPREAD = 8.0
INV = 1.0 / SPREAD

F32 = jnp.float32
BF16 = jnp.bfloat16
GX_GY_EA = ("gx", "gy", "ea")
AXES = ("gx", "gy", "ea")


def two_parts(x):
    high = x.astype(BF16)
    low = (x - high.astype(F32)).astype(BF16)
    return high, low


def dot_nn(a, b):
    return lax.dot_general(a, b, (((1,), (0,)), ((), ())), preferred_element_type=F32)


def dot_nt(a, b):
    return lax.dot_general(a, b, (((1,), (1,)), ((), ())), preferred_element_type=F32)


def iota(shape, dim):
    return lax.broadcasted_iota(jnp.int32, shape, dim)


def kernel(
    sizes,
    v_in,
    w_in,
    shift_in,
    diag_in,
    off_in,
    coup_in,
    kind_in,
    cell_in,
    node_in,
    v_out,
    w_out,
    moments,
    v,
    w,
    w_first,
    shift,
    diag,
    off,
    coup,
    slots,
    node_rows,
    their_nodes,
    their_hot,
    acc,
    weights,
    stiff,
    gather_hot,
    scatter_hot,
    row_hot,
    row_mask,
    node_hot,
    spread_rows,
    wsend,
    wrecv,
    wfirst,
    tsend,
    trecv,
    came,
    hx,
    hy,
    hz,
    sy,
    sz,
    red_line,
    red_plane,
    tokens,
    in_sem,
    sent,
    node_recv,
    halo_recv,
    w_recv,
    t_recv,
    line_recv,
    plane_recv,
):
    scope = jax.named_scope
    me = {a: lax.axis_index(a) for a in AXES}
    ea = me["ea"]

    def other(axis, d):
        return lax.rem(me[axis] + d, sizes[axis])

    with scope("issue"):
        loads = {
            name: pltpu.make_async_copy(src, dst, in_sem.at[n])
            for name, n, src, dst in (
                ("v", 1, v_in, v.at[0]),
                ("cell", 0, cell_in, slots.at[0]),
                ("node", 0, node_in, slots.at[1]),
                ("kind", 0, kind_in, slots.at[2]),
                ("w", 2, w_in, w_first),
                ("coup", 3, coup_in, coup),
                ("shift", 4, shift_in, shift),
                ("diag", 5, diag_in, diag),
                ("off", 6, off_in, off),
            )
        }
        for load in loads.values():
            load.start()

    def hops(shifts):
        return sum(min(d, sizes[a] - d) for a, d in shifts.items())

    line = [{"gx": d} for d in range(1, sizes["gx"])]
    plane = [
        {"gy": dy, "ea": dx}
        for dy in range(sizes["gy"])
        for dx in range(sizes["ea"])
        if dy or dx
    ]
    line.sort(key=hops, reverse=True)
    plane.sort(key=hops, reverse=True)
    def near(axis, reach):
        n = sizes[axis]
        steps = sorted({d % n for r in range(1, reach + 1) for d in (r, n - r)} - {0})
        return [{axis: d} for d in steps]

    neighbours = near("gx", 2) + near("gy", 1)
    first = neighbours + near("ea", OWNERS // 2)

    def signal(sem, shifts):
        pl.semaphore_signal(
            sem,
            inc=1,
            device_id={a: other(a, d) for a, d in shifts.items()},
            device_id_type=pl.DeviceIdType.MESH,
        )

    def send_token(t):
        for shifts in neighbours:
            signal(tokens.at[t], shifts)

    def wait_token(t):
        pl.semaphore_wait(tokens.at[t], len(neighbours))

    with scope("signals"):
        barrier = pltpu.get_barrier_semaphore()
        for shifts in first:
            signal(barrier, shifts)

    low_edge = [me[a] == 0 for a in AXES]
    high_edge = [me[a] == sizes[a] - 1 for a in AXES]
    halos = (hx, hy, hz)
    with scope("edges"):
        for n in range(3):

            @pl.when(low_edge[n])
            def _():
                halos[n][:, 0] = jnp.zeros_like(halos[n][:, 0])

            @pl.when(high_edge[n])
            def _():
                halos[n][:, 1] = jnp.zeros_like(halos[n][:, 1])

    def remote(src, dst, send_sem, recv_sem, shifts):
        return pltpu.make_async_remote_copy(
            src_ref=src,
            dst_ref=dst,
            send_sem=send_sem,
            recv_sem=recv_sem,
            device_id={a: other(a, d) for a, d in shifts.items()},
            device_id_type=pl.DeviceIdType.MESH,
        )

    def wait_bytes(ref, sem):
        pltpu.make_async_copy(ref, ref, sem).wait()

    def halo_copies(k, n):
        sources = (
            (v.at[k, :, CX - 1], v.at[k, :, 0]),
            (sy.at[k, 0], sy.at[k, 1]),
            (sz.at[k, 0], sz.at[k, 1]),
        )
        a = AXES[n]
        return [
            remote(
                sources[n][side],
                halos[n].at[k, side],
                sent,
                halo_recv.at[k % 2, 2 * n + side],
                {a: d},
            )
            for side, d in ((0, 1), (1, sizes[a] - 1))
        ]

    def on_halos(k, n, there, act):
        for copy, edge in zip(halo_copies(k, n), there[n]):

            @pl.when(jnp.logical_not(edge))
            def _():
                act(copy)

    going = list(zip(high_edge, low_edge))
    coming = list(zip(low_edge, high_edge))

    def w_copy(k, d):
        src, dst = (w.at[0], wfirst.at[d - 1]) if k == 0 else (wsend.at[k, d - 1], wrecv.at[k, d - 1])
        return remote(src, dst, sent, w_recv.at[k % 2], {"ea": d})

    def t_copy(k, d):
        return remote(tsend.at[k, d - 1], trecv.at[k, d - 1], sent, t_recv.at[k % 2], {"ea": d})

    def node_copy(d):
        return remote(
            node_rows.at[other("ea", d)], their_nodes.at[d - 1], sent, node_recv, {"ea": d}
        )

    lane = iota((CY, CZ), 1)
    row = iota((CY, CZ), 0)

    half = iota((8, CZ), 1)

    def turned(tile, by):
        return pltpu.roll(tile, by % CZ, 1) if by % CZ else tile

    def pack_faces(k):
        last = jnp.zeros((8, CZ), F32)
        first = jnp.zeros((8, CZ), F32)
        for g in range(FACES):
            i, x = divmod(g, CX)
            sy[k, 0, pl.ds(g, 1), :] = v[k, i, x, pl.ds(CY - 1, 1), :]
            sy[k, 1, pl.ds(g, 1), :] = v[k, i, x, pl.ds(0, 1), :]
            for top in (0, 1):
                tile = v[k, i, x, pl.ds(8 * top, 8), :]
                at = g + FACES * top
                last = jnp.where(half == at, turned(tile, at + 1), last)
                first = jnp.where(half == at, turned(tile, at), first)
        sz[k, 0] = last
        sz[k, 1] = first

    def unpacked(faces, g, to):
        return jnp.concatenate(
            [turned(faces, to - g - FACES * top) for top in (0, 1)], axis=0
        )

    def terms_for_nodes(k):
        both_parts = jnp.concatenate(two_parts(v[k].reshape(COMP * ROWS, CZ)), axis=1)
        owners = [other("ea", d) for d in range(OWNERS)]
        order = (2, 1, 3, 0)
        spread = {d: dot_nn(both_parts, gather_hot[owners[d]]) for d in order}
        term = {}
        for d in order:
            here = row_mask[owners[d]]
            term[d] = jnp.zeros((EPAD, CAP), F32)
            for i in range(COMP):
                rows = spread[d][i * ROWS : (i + 1) * ROWS]
                picked = jnp.sum(rows * here, axis=0, keepdims=True)
                term[d] = term[d] + weights[owners[d], i] * picked
        for d in order[:3]:
            tsend[k, d - 1] = term[d]
        return term[0]

    def own_terms(term):
        both = dot_nt(jnp.concatenate(two_parts(term), axis=0), node_hot[ea])
        return both[:EPAD] + both[EPAD:]

    def values_at(values, hot):
        both = dot_nn(jnp.concatenate(two_parts(values), axis=0), hot)
        return both[:EPAD] + both[EPAD:]

    def terms_for_cells(k, distances):
        owners = {d: other("ea", OWNERS - d) for d in distances}
        value = {}
        for d in distances:
            if d == 0:
                value[d] = values_at(w[k], node_hot[ea])
            elif k == 0:
                value[d] = values_at(wfirst[d - 1], node_hot[owners[d]])
            else:
                value[d] = wrecv[k, d - 1]
        for d in distances:
            hot = row_hot[owners[d]]
            for i in range(COMP):
                total = jnp.sum(weights[owners[d], i] * value[d], axis=0, keepdims=True)
                for part, piece in enumerate(two_parts(jnp.broadcast_to(total, (CY, CAP)))):
                    for x in range(CX):
                        spread_rows[d, i, x, :, part * CAP : (part + 1) * CAP] = (
                            hot[x * CY : (x + 1) * CY] * piece
                        )
        added = sum(
            dot_nt(spread_rows[d].reshape(COMP * ROWS, 2 * CAP), scatter_hot[owners[d]])
            for d in distances
        )
        return added.reshape(COMP, CX, CY, CZ)

    def inner_part(k):
        for i in range(COMP):
            for x in range(CX):
                tile = v[k, i, x]
                beside = jnp.where(row > 0, pltpu.roll(tile, 1, 0), 0.0)
                beside += jnp.where(row < CY - 1, pltpu.roll(tile, CY - 1, 0), 0.0)
                beside += jnp.where(lane > 0, pltpu.roll(tile, 1, 1), 0.0)
                beside += jnp.where(lane < CZ - 1, pltpu.roll(tile, CZ - 1, 1), 0.0)
                if x > 0:
                    beside += v[k, i, x - 1]
                if x < CX - 1:
                    beside += v[k, i, x + 1]
                acc[i, x] = ((shift[x] + (6.0 - CENTER)) * tile - beside) * INV

    def outer_part(k, target):
        low_z, high_z = hz[k, 0], hz[k, 1]
        for i in range(COMP):
            for x in range(CX):
                g = i * CX + x
                beside = jnp.where(row == 0, hy[k, 0, pl.ds(g, 1), :], 0.0)
                beside += jnp.where(row == CY - 1, hy[k, 1, pl.ds(g, 1), :], 0.0)
                beside += jnp.where(lane == 0, unpacked(low_z, g, 0), 0.0)
                beside += jnp.where(lane == CZ - 1, unpacked(high_z, g, CZ - 1), 0.0)
                if x == 0:
                    beside += hx[k, 0, i]
                if x == CX - 1:
                    beside += hx[k, 1, i]
                target[i, x] = acc[i, x] - beside * INV

    def fold_v(left, right):
        return jnp.sum((left * right).reshape(FACES * CY // 8, 8, CZ), axis=0)

    def fold_w(prod):
        return prod[0:8, 0:128] + prod[0:8, 128:256] + prod[8:16, 0:128] + prod[8:16, 128:256]

    def local_product(j, k):
        return fold_v(v[j], v[k]) + fold_w(w[j] * w[k])

    with scope("tables_wait"):
        wait_bytes(slots, in_sem.at[0])
    with scope("tables"):
        for o in range(OWNERS):
            cells = slots[0, 0, o : o + 1, :]
            nodes = slots[1, 0, o : o + 1, :]
            node_rows[o] = nodes
            hot = (iota((CZ, CAP), 0) == jnp.bitwise_and(cells, CZ - 1)).astype(F32).astype(BF16)
            gather_hot[o, 0:CZ] = hot
            gather_hot[o, CZ : 2 * CZ] = hot
            scatter_hot[o, :, 0:CAP] = hot
            scatter_hot[o, :, CAP : 2 * CAP] = hot
            mask = (iota((ROWS, CAP), 0) == lax.shift_right_logical(cells, 7)).astype(F32)
            row_mask[o] = mask
            row_hot[o] = mask.astype(BF16)
            node_hot[o] = (
                (iota((ENB, CAP), 0) == nodes).astype(F32).astype(BF16)
            )

    with scope("vw_wait"):
        loads["v"].wait()
        loads["w"].wait()
    with scope("pack_0"):
        for k in range(ITERS + 1):
            w[k, 8:16, :] = jnp.zeros((8, ENB), F32)
        w[0, 0:ECOMP, :] = w_first[...]
        pack_faces(0)
    with scope("weights"):
        loads["coup"].wait()
        needed = jnp.where(iota((ECOMP, CAP), 0) < 3, 1, 2)
        for o in range(OWNERS):
            live = slots[2, 0, o : o + 1, :] >= needed
            for i in range(COMP):
                weights[o, i, 8:16] = jnp.zeros((8, CAP), F32)
                weights[o, i, 0:ECOMP] = jnp.where(
                    live, coup[i, :, o * CAP : (o + 1) * CAP] * INV, 0.0
                )
    with scope("nodes_0"):
        own = terms_for_nodes(0)
    with scope("barrier_wait"):
        pl.semaphore_wait(barrier, len(first))

    def send_halos(k):
        for n in (2, 1, 0):
            on_halos(k, n, going, lambda copy: copy.start())

    def wait_halos(k):
        for n in range(3):
            on_halos(k, n, coming, lambda copy: copy.wait_recv())

    def send_terms(k):
        for d in (2, 1, 3):
            t_copy(k, d).start()

    def send_w(k):
        if k > 0:
            values = values_at(w[k], their_hot[...])
            for d in (2, 1, 3):
                wsend[k, OWNERS - d - 1] = values[:, (d - 1) * CAP : d * CAP]
        for d in (2, 1, 3):
            w_copy(k, d).start()

    def stiff_times(k):
        out = own_terms(own)[0:ECOMP]
        for q in range(ECOMP):
            out = out + stiff[q] * w[k, pl.ds(q, 1), :]
        return out

    def next_w(k, pushed):
        wait_bytes(trecv.at[k], t_recv.at[k % 2])
        pieces = [two_parts(trecv[k, d]) for d in range(OWNERS - 1)]
        rows = [jnp.concatenate([p[n] for p in pieces], axis=1) for n in (0, 1)]
        both = dot_nt(jnp.concatenate(rows, axis=0), their_hot[...])
        came[...] = both[:EPAD] + both[EPAD:]
        w[k + 1, 0:ECOMP, :] = pushed + came[0:ECOMP]

    def wait_w(k):
        wait_bytes(wfirst if k == 0 else wrecv.at[k], w_recv.at[k % 2])

    def next_v(k):
        with scope(f"w_wait_{k}"):
            wait_w(k)
        with scope(f"cells_{k}"):
            acc[...] += terms_for_cells(k, (1, 3, 2))
        if k == 1:
            with scope("token_3"):
                wait_token(2)
                send_token(3)
        with scope(f"halo_wait_{k}"):
            wait_halos(k)
        with scope(f"outer_{k}"):
            outer_part(k, v.at[k + 1])

    parts = [None] * MOMENTS
    last = ITERS - 1

    with scope("send_0"):
        for d in (2, 1, 3):
            node_copy(d).start()
        send_halos(0)
        send_terms(0)
        send_w(0)
        send_token(0)
    with scope("inner_0"):
        loads["shift"].wait()
        inner_part(0)
    with scope("stiff"):
        loads["diag"].wait()
        loads["off"].wait()
        comp = iota((ECOMP, ENB), 0)
        for q in range(ECOMP):
            both = (off[q] + off[:, q, :]) * (0.5 * INV)
            stiff[q] = jnp.where(comp == q, (diag[...] - CENTER) * INV, both)
    with scope("pushed_0"):
        pushed = stiff_times(0)
        parts[0] = local_product(0, 0)
        acc[...] += terms_for_cells(0, (0,))
    with scope("their_nodes"):
        wait_bytes(their_nodes, node_recv)
        for d in range(OWNERS - 1):
            their_hot[:, d * CAP : (d + 1) * CAP] = (
                (iota((ENB, CAP), 0) == their_nodes[d]).astype(F32).astype(BF16)
            )
    with scope("w_next_0"):
        next_w(0, pushed)
        send_w(1)
    with scope("token_1"):
        wait_token(0)
        send_token(1)
    next_v(0)

    with scope("pack_1"):
        pack_faces(1)
        send_halos(1)
    with scope("nodes_1"):
        own = terms_for_nodes(1)
        send_terms(1)
    with scope("inner_1"):
        inner_part(1)
        parts[1] = local_product(0, 1)
        parts[2] = local_product(1, 1)
        acc[...] += terms_for_cells(1, (0,))
        pushed = stiff_times(1)
    with scope("token_2"):
        wait_token(1)
        send_token(2)
    next_v(1)

    with scope("nodes_2"):
        pack_faces(2)
        own = terms_for_nodes(2)
        send_halos(2)
        send_terms(2)
    with scope("w_next_1"):
        next_w(1, pushed)
        send_w(2)
    with scope("inner_2"):
        inner_part(2)
        parts[3] = local_product(1, 2)
        parts[4] = local_product(2, 2)
        own_node_terms = own_terms(own)
        pushed = stiff_times(2)
    with scope("halo_wait_2"):
        wait_halos(2)
    with scope("outer_2"):
        outer_part(2, acc)
    with scope("w_next_2"):
        next_w(2, pushed)

    with scope("moments"):
        twice = own_node_terms + came[...]
        parts[2 * last + 1] = fold_v(v[last], acc[...]) + fold_w(
            w[last] * (w[last + 1] + twice)
        )
        at = iota((8, 128), 1)
        tile = jnp.zeros((8, 128), F32)
        for m in range(MOMENTS):
            tile = jnp.where(at == m, jnp.sum(parts[m], axis=1, keepdims=True), tile)
        total = jnp.sum(tile, axis=0, keepdims=True)

    def send_total(buf, at, recv_sem, group):
        mine = buf.at[at]
        mine[...] = total
        copies = [
            remote(mine, mine, sent, recv_sem, shifts)
            for shifts in group
        ]
        for copy in copies:
            copy.start()
        return buf.at[pl.ds(0, len(group))]

    with scope("token_end"):
        wait_token(TOKENS - 1)
    with scope("line_send"):
        on_line = send_total(red_line, me["gx"], line_recv, line)
    with scope("cells_last"):
        wait_w(last)
        v[last + 1] = acc[...] + terms_for_cells(last, (0, 1, 3, 2))
    with scope("out_send"):
        out = [
            pltpu.make_async_copy(v, v_out, sent),
            pltpu.make_async_copy(w, w_out, sent),
        ]
        for copy in out:
            copy.start()
    with scope("line_wait"):
        wait_bytes(on_line, line_recv)
        total = jnp.sum(red_line[...], axis=0)
    with scope("plane_send"):
        on_plane = send_total(
            red_plane, me["gy"] * sizes["ea"] + ea, plane_recv, plane
        )
    with scope("plane_wait"):
        wait_bytes(on_plane, plane_recv)
        moments[...] = jnp.sum(red_plane[...], axis=0)
    with scope("ends"):
        for n in range(3):
            for side, edge in enumerate(going[n]):

                @pl.when(jnp.logical_not(edge))
                def _():
                    wait_bytes(halos[n].at[:, side], sent)

        for ref in (their_nodes, wfirst, wrecv.at[pl.ds(1, ITERS - 1)], trecv, on_line, on_plane, v, w):
            wait_bytes(ref, sent)


def combine(v, w_all, moments, sol_v, res_v, sol_w, res_w):
    total = moments[...]
    flat = iota((1, 128), 1)
    mu = [
        jnp.broadcast_to(
            jnp.sum(jnp.where(flat == m, total, 0.0), axis=1, keepdims=True), (1, 128)
        )
        for m in range(MOMENTS)
    ]

    def form(left, right):
        out = None
        for i, p in enumerate(left):
            for j, q in enumerate(right):
                term = p * q * mu[i + j]
                out = term if out is None else out + term
        return out

    zero = jnp.zeros((1, 128), F32)
    sol, res, way = [zero] * ITERS, [zero + 1.0] + [zero] * ITERS, [zero + 1.0]
    norm = mu[0]
    for it in range(ITERS):
        image = [zero] * (it + 2)
        for j, p in enumerate(way):
            image[j] = image[j] + CENTER * p
            image[j + 1] = image[j + 1] + SPREAD * p
        alpha = norm / form(way, image)
        for j, p in enumerate(way):
            sol[j] = sol[j] + alpha * p
        for j, p in enumerate(image):
            res[j] = res[j] - alpha * p
        if it + 1 < ITERS:
            norm_next = form(res[: it + 2], res[: it + 2])
            ratio = norm_next / norm
            way = [res[j] + (ratio * way[j] if j < len(way) else 0.0) for j in range(it + 2)]
            norm = norm_next

    for i in range(COMP):
        for x in range(CX):
            b = [v[k, i, x] for k in range(ITERS + 1)]
            sol_v[i, x] = sum(sol[k] * b[k] for k in range(ITERS))
            res_v[i, x] = sum(res[k] * b[k] for k in range(ITERS + 1))
    spread = [
        (jnp.concatenate([sol[k]] * 2, axis=1) if k < ITERS else None,
         jnp.concatenate([res[k]] * 2, axis=1))
        for k in range(ITERS + 1)
    ]
    b = [w_all[k, 0:ECOMP, :] for k in range(ITERS + 1)]
    sol_w[...] = sum(spread[k][0] * b[k] for k in range(ITERS))
    res_w[...] = sum(spread[k][1] * b[k] for k in range(ITERS + 1))


def body(sizes, *args):
    v_in, w_in = args[0], args[1]
    vmem, dma = pltpu.VMEM, pltpu.SemaphoreType.DMA
    steps = ITERS
    basis = pl.pallas_call(
        functools.partial(kernel, sizes),
        name="krylov",
        out_shape=(
            vmem((steps + 1, COMP, CX, CY, CZ), F32),
            vmem((steps + 1, EPAD, ENB), F32),
            vmem((1, 128), F32),
        ),
        in_specs=[pl.BlockSpec(memory_space=pl.ANY)] * len(args),
        out_specs=[pl.BlockSpec(memory_space=pl.ANY)] * 2
        + [pl.BlockSpec(memory_space=pltpu.VMEM)],
        scratch_shapes=[
            vmem((steps + 1, COMP, CX, CY, CZ), F32),
            vmem((steps + 1, EPAD, ENB), F32),
            vmem((ECOMP, ENB), F32),
            vmem((CX, CY, CZ), F32),
            vmem((ECOMP, ENB), F32),
            vmem((ECOMP, ECOMP, ENB), F32),
            vmem((COMP, ECOMP, SLOTS), F32),
            vmem((3, 1, OWNERS, CAP), jnp.int32),
            vmem((OWNERS, 1, CAP), jnp.int32),
            vmem((OWNERS - 1, 1, CAP), jnp.int32),
            vmem((ENB, (OWNERS - 1) * CAP), BF16),
            vmem((COMP, CX, CY, CZ), F32),
            vmem((OWNERS, COMP, EPAD, CAP), F32),
            vmem((ECOMP, ECOMP, ENB), F32),
            vmem((OWNERS, 2 * CZ, CAP), BF16),
            vmem((OWNERS, CZ, 2 * CAP), BF16),
            vmem((OWNERS, ROWS, CAP), BF16),
            vmem((OWNERS, ROWS, CAP), F32),
            vmem((OWNERS, ENB, CAP), BF16),
            vmem((OWNERS, COMP, CX, CY, 2 * CAP), BF16),
            vmem((steps, OWNERS - 1, EPAD, CAP), F32),
            vmem((steps, OWNERS - 1, EPAD, CAP), F32),
            vmem((OWNERS - 1, EPAD, ENB), F32),
            vmem((steps, OWNERS - 1, EPAD, CAP), F32),
            vmem((steps, OWNERS - 1, EPAD, CAP), F32),
            vmem((EPAD, ENB), F32),
            vmem((steps, 2, COMP, CY, CZ), F32),
            vmem((steps, 2, 16, CZ), F32),
            vmem((steps, 2, 8, CZ), F32),
            vmem((steps, 2, 16, CZ), F32),
            vmem((steps, 2, 8, CZ), F32),
            vmem((sizes["gx"], 1, 128), F32),
            vmem((sizes["gy"] * sizes["ea"], 1, 128), F32),
            pltpu.SemaphoreType.REGULAR((TOKENS,)),
            dma((7,)),
            dma,
            dma,
            dma((2, 6)),
            dma((2,)),
            dma((2,)),
            dma,
            dma,
        ],
        compiler_params=pltpu.CompilerParams(collective_id=0, has_side_effects=True),
    )(*args)
    return pl.pallas_call(
        combine,
        name="combine",
        out_shape=(
            jax.ShapeDtypeStruct(v_in.shape, F32),
            jax.ShapeDtypeStruct(v_in.shape, F32),
            jax.ShapeDtypeStruct(w_in.shape, F32),
            jax.ShapeDtypeStruct(w_in.shape, F32),
        ),
        in_specs=[pl.BlockSpec(memory_space=pltpu.VMEM)] * 3,
        out_specs=[pl.BlockSpec(memory_space=pltpu.VMEM)] * 4,
        compiler_params=pltpu.CompilerParams(vmem_limit_bytes=VMEM_LIMIT),
    )(*(pltpu.with_memory_space_constraint(b, pltpu.VMEM) for b in basis))


def solution(mesh):
    sizes = {a: mesh.shape[a] for a in AXES}
    return jax.shard_map(
        functools.partial(body, sizes),
        mesh=mesh,
        in_specs=(
            P(None, "gx", "gy", "ea"),
            P(None, GX_GY_EA),
            P("gx", "gy", "ea"),
            P(None, GX_GY_EA),
            P(None, None, GX_GY_EA),
            P(None, None, GX_GY_EA),
            P(GX_GY_EA, None, None),
            P(GX_GY_EA, None, None),
            P(GX_GY_EA, None, None),
        ),
        out_specs=(
            P(None, "gx", "gy", "ea"),
            P(None, "gx", "gy", "ea"),
            P(None, GX_GY_EA),
            P(None, GX_GY_EA),
        ),
        check_vma=False,
    )
```

```python
import functools

import jax
import jax.numpy as jnp
from jax import lax
from jax.experimental import pallas as pl
from jax.experimental.pallas import tpu as pltpu
from jax.sharding import PartitionSpec as P

ITERS = 3
COMP = 3
CX = 4
CY = 16
CZ = 128
ROWS = CX * CY
FACES = COMP * CX
ECOMP = 15
EPAD = 16
ENB = 256
OWNERS = 4
CAP = 128
SLOTS = OWNERS * CAP
MOMENTS = 6
VMEM_LIMIT = 16 << 20
TOKENS = 3

CENTER = 12.0
SPREAD = 8.0
INV = 1.0 / SPREAD

F32 = jnp.float32
BF16 = jnp.bfloat16
GX_GY_EA = ("gx", "gy", "ea")
AXES = ("gx", "gy", "ea")


def two_parts(x):
    high = x.astype(BF16)
    low = (x - high.astype(F32)).astype(BF16)
    return high, low


def dot_nn(a, b):
    return lax.dot_general(a, b, (((1,), (0,)), ((), ())), preferred_element_type=F32)


def dot_nt(a, b):
    return lax.dot_general(a, b, (((1,), (1,)), ((), ())), preferred_element_type=F32)


def iota(shape, dim):
    return lax.broadcasted_iota(jnp.int32, shape, dim)


def kernel(
    sizes,
    v_in,
    w_in,
    shift_in,
    diag_in,
    off_in,
    coup_in,
    kind_in,
    cell_in,
    node_in,
    v_out,
    w_out,
    moments,
    v,
    w,
    w_first,
    shift,
    diag,
    off,
    coup,
    slots,
    node_rows,
    their_nodes,
    their_hot,
    acc,
    weights,
    stiff,
    gather_hot,
    scatter_hot,
    row_hot,
    row_mask,
    node_hot,
    spread_rows,
    wsend,
    wrecv,
    wfirst,
    tsend,
    trecv,
    came,
    hx,
    hy,
    hz,
    sy,
    sz,
    red_line,
    red_plane,
    tokens,
    in_sem,
    sent,
    node_recv,
    halo_recv,
    w_recv,
    t_recv,
    line_recv,
    plane_recv,
):
    scope = jax.named_scope
    me = {a: lax.axis_index(a) for a in AXES}
    ea = me["ea"]

    def other(axis, d):
        return lax.rem(me[axis] + d, sizes[axis])

    with scope("issue"):
        loads = {
            name: pltpu.make_async_copy(src, dst, in_sem.at[n])
            for name, n, src, dst in (
                ("v", 1, v_in, v.at[0]),
                ("cell", 0, cell_in, slots.at[0]),
                ("node", 0, node_in, slots.at[1]),
                ("kind", 0, kind_in, slots.at[2]),
                ("w", 2, w_in, w_first),
                ("coup", 3, coup_in, coup),
                ("shift", 4, shift_in, shift),
                ("diag", 5, diag_in, diag),
                ("off", 6, off_in, off),
            )
        }
        for load in loads.values():
            load.start()

    def hops(shifts):
        return sum(min(d, sizes[a] - d) for a, d in shifts.items())

    line = [{"gx": d} for d in range(1, sizes["gx"])]
    plane = [
        {"gy": dy, "ea": dx}
        for dy in range(sizes["gy"])
        for dx in range(sizes["ea"])
        if dy or dx
    ]
    line.sort(key=hops, reverse=True)
    plane.sort(key=hops, reverse=True)
    def near(axis, *reach):
        n = sizes[axis]
        return [{axis: d} for d in sorted({d % n for r in reach for d in (r, n - r)} - {0})]

    first = near("gx", 1) + near("gy", 1) + near("ea", 1, 2)
    rounds = [near("gx", r) + near("gy", r) for r in (1, 2, 4)]

    def signal(sem, shifts):
        pl.semaphore_signal(
            sem,
            inc=1,
            device_id={a: other(a, d) for a, d in shifts.items()},
            device_id_type=pl.DeviceIdType.MESH,
        )

    def send_token(t):
        for shifts in rounds[t]:
            signal(tokens.at[t], shifts)

    def wait_token(t):
        pl.semaphore_wait(tokens.at[t], len(rounds[t]))

    with scope("signals"):
        barrier = pltpu.get_barrier_semaphore()
        for shifts in first:
            signal(barrier, shifts)

    low_edge = [me[a] == 0 for a in AXES]
    high_edge = [me[a] == sizes[a] - 1 for a in AXES]
    halos = (hx, hy, hz)
    with scope("edges"):
        for n in range(3):

            @pl.when(low_edge[n])
            def _():
                halos[n][:, 0] = jnp.zeros_like(halos[n][:, 0])

            @pl.when(high_edge[n])
            def _():
                halos[n][:, 1] = jnp.zeros_like(halos[n][:, 1])

    def remote(src, dst, send_sem, recv_sem, shifts):
        return pltpu.make_async_remote_copy(
            src_ref=src,
            dst_ref=dst,
            send_sem=send_sem,
            recv_sem=recv_sem,
            device_id={a: other(a, d) for a, d in shifts.items()},
            device_id_type=pl.DeviceIdType.MESH,
        )

    def wait_bytes(ref, sem):
        pltpu.make_async_copy(ref, ref, sem).wait()

    def halo_copies(k, n):
        sources = (
            (v.at[k, :, CX - 1], v.at[k, :, 0]),
            (sy.at[k, 0], sy.at[k, 1]),
            (sz.at[k, 0], sz.at[k, 1]),
        )
        a = AXES[n]
        return [
            remote(
                sources[n][side],
                halos[n].at[k, side],
                sent,
                halo_recv.at[k % 2, n],
                {a: d},
            )
            for side, d in ((0, 1), (1, sizes[a] - 1))
        ]

    def on_halos(k, n, there, act):
        for copy, edge in zip(halo_copies(k, n), there[n]):

            @pl.when(jnp.logical_not(edge))
            def _():
                act(copy)

    going = list(zip(high_edge, low_edge))

    def w_copy(k, d):
        src, dst = (w.at[0], wfirst.at[d - 1]) if k == 0 else (wsend.at[k, d - 1], wrecv.at[k, d - 1])
        return remote(src, dst, sent, w_recv.at[k % 2], {"ea": d})

    def t_copy(k, d):
        src = tsend.at[k, other("ea", d)]
        return remote(src, trecv.at[k, d - 1], sent, t_recv.at[k % 2], {"ea": d})

    def node_copy(d):
        return remote(
            node_rows.at[other("ea", d)], their_nodes.at[d - 1], sent, node_recv, {"ea": d}
        )

    lane = iota((CY, CZ), 1)
    row = iota((CY, CZ), 0)

    half = iota((8, CZ), 1)

    def turned(tile, by):
        return pltpu.roll(tile, by % CZ, 1) if by % CZ else tile

    def pack_faces(k):
        last = jnp.zeros((8, CZ), F32)
        first = jnp.zeros((8, CZ), F32)
        for g in range(FACES):
            i, x = divmod(g, CX)
            sy[k, 0, pl.ds(g, 1), :] = v[k, i, x, pl.ds(CY - 1, 1), :]
            sy[k, 1, pl.ds(g, 1), :] = v[k, i, x, pl.ds(0, 1), :]
            for top in (0, 1):
                tile = v[k, i, x, pl.ds(8 * top, 8), :]
                at = g + FACES * top
                last = jnp.where(half == at, turned(tile, at + 1), last)
                first = jnp.where(half == at, turned(tile, at), first)
        sz[k, 0] = last
        sz[k, 1] = first

    def unpacked(faces, g, to):
        return jnp.concatenate(
            [turned(faces, to - g - FACES * top) for top in (0, 1)], axis=0
        )

    def terms_for_nodes(k):
        both_parts = jnp.concatenate(two_parts(v[k].reshape(COMP * ROWS, CZ)), axis=1)
        spread = [dot_nn(both_parts, gather_hot[n]) for n in range(OWNERS // 2)]
        for o in range(OWNERS):
            cols = slice(o % 2 * CAP, (o % 2 + 1) * CAP)
            term = jnp.zeros((EPAD, CAP), F32)
            for i in range(COMP):
                rows = spread[o // 2][i * ROWS : (i + 1) * ROWS, cols]
                picked = jnp.sum(rows * row_mask[o], axis=0, keepdims=True)
                term = term + weights[o, i] * picked
            tsend[k, o] = term
        return tsend[k, ea]

    def own_terms(term):
        both = dot_nt(jnp.concatenate(two_parts(term), axis=0), node_hot[ea])
        return both[:EPAD] + both[EPAD:]

    def values_at(values, hot):
        both = dot_nn(jnp.concatenate(two_parts(values), axis=0), hot)
        return both[:EPAD] + both[EPAD:]

    def terms_for_cells(k, distances):
        owners = {d: other("ea", OWNERS - d) for d in distances}
        value = {}
        for d in distances:
            if d == 0:
                value[d] = values_at(w[k], node_hot[ea])
            elif k == 0:
                value[d] = values_at(wfirst[d - 1], node_hot[owners[d]])
            else:
                value[d] = wrecv[k, d - 1]
        for d in distances:
            hot = row_hot[owners[d]]
            for i in range(COMP):
                total = jnp.sum(weights[owners[d], i] * value[d], axis=0, keepdims=True)
                for part, piece in enumerate(two_parts(jnp.broadcast_to(total, (CY, CAP)))):
                    for x in range(CX):
                        spread_rows[d, i, x, :, part * CAP : (part + 1) * CAP] = (
                            hot[x * CY : (x + 1) * CY] * piece
                        )
        added = sum(
            dot_nt(spread_rows[d].reshape(COMP * ROWS, 2 * CAP), scatter_hot[owners[d]])
            for d in distances
        )
        return added.reshape(COMP, CX, CY, CZ)

    def inner_part(k):
        for i in range(COMP):
            for x in range(CX):
                tile = v[k, i, x]
                beside = jnp.where(row > 0, pltpu.roll(tile, 1, 0), 0.0)
                beside += jnp.where(row < CY - 1, pltpu.roll(tile, CY - 1, 0), 0.0)
                beside += jnp.where(lane > 0, pltpu.roll(tile, 1, 1), 0.0)
                beside += jnp.where(lane < CZ - 1, pltpu.roll(tile, CZ - 1, 1), 0.0)
                if x > 0:
                    beside += v[k, i, x - 1]
                if x < CX - 1:
                    beside += v[k, i, x + 1]
                acc[i, x] = ((shift[x] + (6.0 - CENTER)) * tile - beside) * INV

    def outer_part(k, target):
        low_z, high_z = hz[k, 0], hz[k, 1]
        for i in range(COMP):
            for x in range(CX):
                g = i * CX + x
                beside = jnp.where(row == 0, hy[k, 0, pl.ds(g, 1), :], 0.0)
                beside += jnp.where(row == CY - 1, hy[k, 1, pl.ds(g, 1), :], 0.0)
                beside += jnp.where(lane == 0, unpacked(low_z, g, 0), 0.0)
                beside += jnp.where(lane == CZ - 1, unpacked(high_z, g, CZ - 1), 0.0)
                if x == 0:
                    beside += hx[k, 0, i]
                if x == CX - 1:
                    beside += hx[k, 1, i]
                target[i, x] = acc[i, x] - beside * INV

    def fold_v(left, right):
        return jnp.sum((left * right).reshape(FACES * CY // 8, 8, CZ), axis=0)

    def fold_w(prod):
        return prod[0:8, 0:128] + prod[0:8, 128:256] + prod[8:16, 0:128] + prod[8:16, 128:256]

    def local_product(j, k):
        return fold_v(v[j], v[k]) + fold_w(w[j] * w[k])

    with scope("tables_wait"):
        wait_bytes(slots, in_sem.at[0])
    with scope("tables"):
        for o in range(OWNERS):
            cells = slots[0, 0, o : o + 1, :]
            nodes = slots[1, 0, o : o + 1, :]
            node_rows[o] = nodes
            hot = (iota((CZ, CAP), 0) == jnp.bitwise_and(cells, CZ - 1)).astype(F32).astype(BF16)
            cols = slice(o % 2 * CAP, (o % 2 + 1) * CAP)
            gather_hot[o // 2, 0:CZ, cols] = hot
            gather_hot[o // 2, CZ : 2 * CZ, cols] = hot
            scatter_hot[o, :, 0:CAP] = hot
            scatter_hot[o, :, CAP : 2 * CAP] = hot
            mask = (iota((ROWS, CAP), 0) == lax.shift_right_logical(cells, 7)).astype(F32)
            row_mask[o] = mask
            row_hot[o] = mask.astype(BF16)
            node_hot[o] = (
                (iota((ENB, CAP), 0) == nodes).astype(F32).astype(BF16)
            )

    with scope("vw_wait"):
        loads["v"].wait()
        loads["w"].wait()
    with scope("pack_0"):
        for k in range(ITERS + 1):
            w[k, 8:16, :] = jnp.zeros((8, ENB), F32)
        w[0, 0:ECOMP, :] = w_first[...]
        pack_faces(0)
    with scope("weights"):
        loads["coup"].wait()
        needed = jnp.where(iota((ECOMP, CAP), 0) < 3, 1, 2)
        for o in range(OWNERS):
            live = slots[2, 0, o : o + 1, :] >= needed
            for i in range(COMP):
                weights[o, i, 8:16] = jnp.zeros((8, CAP), F32)
                weights[o, i, 0:ECOMP] = jnp.where(
                    live, coup[i, :, o * CAP : (o + 1) * CAP] * INV, 0.0
                )
    with scope("nodes_0"):
        own = terms_for_nodes(0)
    with scope("barrier_wait"):
        pl.semaphore_wait(barrier, len(first))

    def send_halos(k):
        for n in (2, 1, 0):
            on_halos(k, n, going, lambda copy: copy.start())

    def wait_halos(k):
        for n in range(3):
            sem = halo_recv.at[k % 2, n]
            low, high = low_edge[n], high_edge[n]

            @pl.when(jnp.logical_not(jnp.logical_or(low, high)))
            def _():
                wait_bytes(halos[n].at[k], sem)

            @pl.when(low)
            def _():
                wait_bytes(halos[n].at[k, 1], sem)

            @pl.when(high)
            def _():
                wait_bytes(halos[n].at[k, 0], sem)

    def send_terms(k):
        for d in (2, 1, 3):
            t_copy(k, d).start()

    def send_w(k):
        if k > 0:
            values = values_at(w[k], their_hot[...])
            for d in (2, 1, 3):
                wsend[k, OWNERS - d - 1] = values[:, (d - 1) * CAP : d * CAP]
        for d in (2, 1, 3):
            w_copy(k, d).start()

    def stiff_times(k):
        out = own_terms(own)[0:ECOMP]
        for q in range(ECOMP):
            out = out + stiff[q] * w[k, pl.ds(q, 1), :]
        return out

    def next_w(k, pushed):
        wait_bytes(trecv.at[k], t_recv.at[k % 2])
        pieces = [two_parts(trecv[k, d]) for d in range(OWNERS - 1)]
        rows = [jnp.concatenate([p[n] for p in pieces], axis=1) for n in (0, 1)]
        both = dot_nt(jnp.concatenate(rows, axis=0), their_hot[...])
        came[...] = both[:EPAD] + both[EPAD:]
        w[k + 1, 0:ECOMP, :] = pushed + came[0:ECOMP]

    def wait_w(k):
        wait_bytes(wfirst if k == 0 else wrecv.at[k], w_recv.at[k % 2])

    def next_v(k):
        with scope(f"w_wait_{k}"):
            wait_w(k)
        with scope(f"cells_{k}"):
            acc[...] += terms_for_cells(k, (1, 3, 2))
        if k == 1:
            with scope("token_2"):
                wait_token(1)
                send_token(2)
        with scope(f"halo_wait_{k}"):
            wait_halos(k)
        with scope(f"outer_{k}"):
            outer_part(k, v.at[k + 1])

    parts = [None] * (MOMENTS - 1)
    last = ITERS - 1

    with scope("send_0"):
        for d in (2, 1, 3):
            node_copy(d).start()
        send_halos(0)
        send_terms(0)
        send_w(0)
        send_token(0)
    with scope("inner_0"):
        loads["shift"].wait()
        inner_part(0)
    with scope("stiff"):
        loads["diag"].wait()
        loads["off"].wait()
        comp = iota((ECOMP, ENB), 0)
        for q in range(ECOMP):
            both = (off[q] + off[:, q, :]) * (0.5 * INV)
            stiff[q] = jnp.where(comp == q, (diag[...] - CENTER) * INV, both)
    with scope("pushed_0"):
        pushed = stiff_times(0)
        parts[0] = local_product(0, 0)
        acc[...] += terms_for_cells(0, (0,))
    with scope("their_nodes"):
        wait_bytes(their_nodes, node_recv)
        for d in range(OWNERS - 1):
            their_hot[:, d * CAP : (d + 1) * CAP] = (
                (iota((ENB, CAP), 0) == their_nodes[d]).astype(F32).astype(BF16)
            )
    with scope("w_next_0"):
        next_w(0, pushed)
        send_w(1)
    with scope("token_1"):
        wait_token(0)
        send_token(1)
    next_v(0)

    with scope("pack_1"):
        pack_faces(1)
        send_halos(1)
    with scope("nodes_1"):
        own = terms_for_nodes(1)
        send_terms(1)
    with scope("inner_1"):
        inner_part(1)
        parts[1] = local_product(0, 1)
        parts[2] = local_product(1, 1)
        acc[...] += terms_for_cells(1, (0,))
        pushed = stiff_times(1)
    next_v(1)

    with scope("nodes_2"):
        pack_faces(2)
        own = terms_for_nodes(2)
        send_halos(2)
        send_terms(2)
    with scope("w_next_1"):
        next_w(1, pushed)
        send_w(2)
    with scope("inner_2"):
        inner_part(2)
        parts[3] = local_product(1, 2)
        parts[4] = local_product(2, 2)
        own_node_terms = own_terms(own)
        pushed = stiff_times(2)
        at = iota((8, 128), 1)
        tile = jnp.zeros((8, 128), F32)
        for m in range(MOMENTS - 1):
            tile = jnp.where(at == m, jnp.sum(parts[m], axis=1, keepdims=True), tile)
    with scope("halo_wait_2"):
        wait_halos(2)
    with scope("outer_2"):
        outer_part(2, acc)
        final = fold_v(v[last], acc[...])
    with scope("w_next_2"):
        next_w(2, pushed)

    with scope("moments"):
        twice = own_node_terms + came[...]
        final = final + fold_w(w[last] * (w[last + 1] + twice))
        tile = jnp.where(at == MOMENTS - 1, jnp.sum(final, axis=1, keepdims=True), tile)
        total = jnp.sum(tile, axis=0, keepdims=True)

    def send_total(buf, at, recv_sem, group):
        mine = buf.at[at]
        mine[...] = total
        copies = [
            remote(mine, mine, sent, recv_sem, shifts)
            for shifts in group
        ]
        for copy in copies:
            copy.start()
        return buf.at[pl.ds(0, len(group))]

    with scope("token_end"):
        wait_token(TOKENS - 1)
    with scope("line_send"):
        on_line = send_total(red_line, me["gx"], line_recv, line)
    with scope("cells_last"):
        wait_w(last)
        v[last + 1] = acc[...] + terms_for_cells(last, (0, 1, 3, 2))
    with scope("out_send"):
        out = [
            pltpu.make_async_copy(v, v_out, sent),
            pltpu.make_async_copy(w, w_out, sent),
        ]
        for copy in out:
            copy.start()
    with scope("line_wait"):
        wait_bytes(on_line, line_recv)
        total = jnp.sum(red_line[...], axis=0)
    with scope("plane_send"):
        on_plane = send_total(
            red_plane, me["gy"] * sizes["ea"] + ea, plane_recv, plane
        )
    with scope("plane_wait"):
        wait_bytes(on_plane, plane_recv)
        moments[...] = jnp.sum(red_plane[...], axis=0)
    with scope("ends"):
        for n in range(3):
            for side, edge in enumerate(going[n]):

                @pl.when(jnp.logical_not(edge))
                def _():
                    wait_bytes(halos[n].at[:, side], sent)

        for ref in (their_nodes, wfirst, wrecv.at[pl.ds(1, ITERS - 1)], trecv, on_line, on_plane, v, w):
            wait_bytes(ref, sent)


def combine(v, w_all, moments, sol_v, res_v, sol_w, res_w):
    total = moments[...]
    flat = iota((1, 128), 1)
    mu = [
        jnp.broadcast_to(
            jnp.sum(jnp.where(flat == m, total, 0.0), axis=1, keepdims=True), (1, 128)
        )
        for m in range(MOMENTS)
    ]

    def form(left, right):
        out = None
        for i, p in enumerate(left):
            for j, q in enumerate(right):
                term = p * q * mu[i + j]
                out = term if out is None else out + term
        return out

    zero = jnp.zeros((1, 128), F32)
    sol, res, way = [zero] * ITERS, [zero + 1.0] + [zero] * ITERS, [zero + 1.0]
    norm = mu[0]
    for it in range(ITERS):
        image = [zero] * (it + 2)
        for j, p in enumerate(way):
            image[j] = image[j] + CENTER * p
            image[j + 1] = image[j + 1] + SPREAD * p
        alpha = norm / form(way, image)
        for j, p in enumerate(way):
            sol[j] = sol[j] + alpha * p
        for j, p in enumerate(image):
            res[j] = res[j] - alpha * p
        if it + 1 < ITERS:
            norm_next = form(res[: it + 2], res[: it + 2])
            ratio = norm_next / norm
            way = [res[j] + (ratio * way[j] if j < len(way) else 0.0) for j in range(it + 2)]
            norm = norm_next

    for i in range(COMP):
        for x in range(CX):
            b = [v[k, i, x] for k in range(ITERS + 1)]
            sol_v[i, x] = sum(sol[k] * b[k] for k in range(ITERS))
            res_v[i, x] = sum(res[k] * b[k] for k in range(ITERS + 1))
    spread = [
        (jnp.concatenate([sol[k]] * 2, axis=1) if k < ITERS else None,
         jnp.concatenate([res[k]] * 2, axis=1))
        for k in range(ITERS + 1)
    ]
    b = [w_all[k, 0:ECOMP, :] for k in range(ITERS + 1)]
    sol_w[...] = sum(spread[k][0] * b[k] for k in range(ITERS))
    res_w[...] = sum(spread[k][1] * b[k] for k in range(ITERS + 1))


def body(sizes, *args):
    v_in, w_in = args[0], args[1]
    vmem, dma = pltpu.VMEM, pltpu.SemaphoreType.DMA
    steps = ITERS
    basis = pl.pallas_call(
        functools.partial(kernel, sizes),
        name="krylov",
        out_shape=(
            vmem((steps + 1, COMP, CX, CY, CZ), F32),
            vmem((steps + 1, EPAD, ENB), F32),
            vmem((1, 128), F32),
        ),
        in_specs=[pl.BlockSpec(memory_space=pl.ANY)] * len(args),
        out_specs=[pl.BlockSpec(memory_space=pl.ANY)] * 2
        + [pl.BlockSpec(memory_space=pltpu.VMEM)],
        scratch_shapes=[
            vmem((steps + 1, COMP, CX, CY, CZ), F32),
            vmem((steps + 1, EPAD, ENB), F32),
            vmem((ECOMP, ENB), F32),
            vmem((CX, CY, CZ), F32),
            vmem((ECOMP, ENB), F32),
            vmem((ECOMP, ECOMP, ENB), F32),
            vmem((COMP, ECOMP, SLOTS), F32),
            vmem((3, 1, OWNERS, CAP), jnp.int32),
            vmem((OWNERS, 1, CAP), jnp.int32),
            vmem((OWNERS - 1, 1, CAP), jnp.int32),
            vmem((ENB, (OWNERS - 1) * CAP), BF16),
            vmem((COMP, CX, CY, CZ), F32),
            vmem((OWNERS, COMP, EPAD, CAP), F32),
            vmem((ECOMP, ECOMP, ENB), F32),
            vmem((OWNERS // 2, 2 * CZ, 2 * CAP), BF16),
            vmem((OWNERS, CZ, 2 * CAP), BF16),
            vmem((OWNERS, ROWS, CAP), BF16),
            vmem((OWNERS, ROWS, CAP), F32),
            vmem((OWNERS, ENB, CAP), BF16),
            vmem((OWNERS, COMP, CX, CY, 2 * CAP), BF16),
            vmem((steps, OWNERS - 1, EPAD, CAP), F32),
            vmem((steps, OWNERS - 1, EPAD, CAP), F32),
            vmem((OWNERS - 1, EPAD, ENB), F32),
            vmem((steps, OWNERS, EPAD, CAP), F32),
            vmem((steps, OWNERS - 1, EPAD, CAP), F32),
            vmem((EPAD, ENB), F32),
            vmem((steps, 2, COMP, CY, CZ), F32),
            vmem((steps, 2, 16, CZ), F32),
            vmem((steps, 2, 8, CZ), F32),
            vmem((steps, 2, 16, CZ), F32),
            vmem((steps, 2, 8, CZ), F32),
            vmem((sizes["gx"], 1, 128), F32),
            vmem((sizes["gy"] * sizes["ea"], 1, 128), F32),
            pltpu.SemaphoreType.REGULAR((TOKENS,)),
            dma((7,)),
            dma,
            dma,
            dma((2, 3)),
            dma((2,)),
            dma((2,)),
            dma,
            dma,
        ],
        compiler_params=pltpu.CompilerParams(collective_id=0, has_side_effects=True),
    )(*args)
    return pl.pallas_call(
        combine,
        name="combine",
        out_shape=(
            jax.ShapeDtypeStruct(v_in.shape, F32),
            jax.ShapeDtypeStruct(v_in.shape, F32),
            jax.ShapeDtypeStruct(w_in.shape, F32),
            jax.ShapeDtypeStruct(w_in.shape, F32),
        ),
        in_specs=[pl.BlockSpec(memory_space=pltpu.VMEM)] * 3,
        out_specs=[pl.BlockSpec(memory_space=pltpu.VMEM)] * 4,
        compiler_params=pltpu.CompilerParams(vmem_limit_bytes=VMEM_LIMIT),
    )(*(pltpu.with_memory_space_constraint(b, pltpu.VMEM) for b in basis))


def solution(mesh):
    sizes = {a: mesh.shape[a] for a in AXES}
    return jax.shard_map(
        functools.partial(body, sizes),
        mesh=mesh,
        in_specs=(
            P(None, "gx", "gy", "ea"),
            P(None, GX_GY_EA),
            P("gx", "gy", "ea"),
            P(None, GX_GY_EA),
            P(None, None, GX_GY_EA),
            P(None, None, GX_GY_EA),
            P(GX_GY_EA, None, None),
            P(GX_GY_EA, None, None),
            P(GX_GY_EA, None, None),
        ),
        out_specs=(
            P(None, "gx", "gy", "ea"),
            P(None, "gx", "gy", "ea"),
            P(None, GX_GY_EA),
            P(None, GX_GY_EA),
        ),
        check_vma=False,
    )
```

```python
import functools

import jax
import jax.numpy as jnp
from jax import lax
from jax.experimental import pallas as pl
from jax.experimental.pallas import tpu as pltpu
from jax.sharding import PartitionSpec as P

ITERS = 3
COMP = 3
CX = 4
CY = 16
CZ = 128
ROWS = CX * CY
FACES = COMP * CX
ECOMP = 15
EPAD = 16
ENB = 256
OWNERS = 4
CAP = 128
SLOTS = OWNERS * CAP
MOMENTS = 6
VMEM_LIMIT = 16 << 20
TOKENS = 3

CENTER = 12.0
SPREAD = 8.0
INV = 1.0 / SPREAD

F32 = jnp.float32
BF16 = jnp.bfloat16
GX_GY_EA = ("gx", "gy", "ea")
AXES = ("gx", "gy", "ea")


def two_parts(x):
    high = x.astype(BF16)
    low = (x - high.astype(F32)).astype(BF16)
    return high, low


def dot_nn(a, b):
    return lax.dot_general(a, b, (((1,), (0,)), ((), ())), preferred_element_type=F32)


def dot_nt(a, b):
    return lax.dot_general(a, b, (((1,), (1,)), ((), ())), preferred_element_type=F32)


def iota(shape, dim):
    return lax.broadcasted_iota(jnp.int32, shape, dim)


def kernel(
    sizes,
    v_in,
    w_in,
    shift_in,
    diag_in,
    off_in,
    coup_in,
    kind_in,
    cell_in,
    node_in,
    v_out,
    w_out,
    moments,
    v,
    w,
    w_first,
    shift,
    diag,
    off,
    coup,
    slots,
    node_rows,
    their_nodes,
    their_hot,
    acc,
    weights,
    stiff,
    gather_hot,
    scatter_hot,
    row_hot,
    row_mask,
    node_hot,
    spread_rows,
    wsend,
    wrecv,
    wfirst,
    tsend,
    trecv,
    came,
    hx,
    hy,
    hz,
    sy,
    sz,
    red_line,
    red_plane,
    tokens,
    in_sem,
    sent,
    node_recv,
    halo_recv,
    w_recv,
    t_recv,
    line_recv,
    plane_recv,
):
    scope = jax.named_scope
    me = {a: lax.axis_index(a) for a in AXES}
    ea = me["ea"]

    def other(axis, d):
        return lax.rem(me[axis] + d, sizes[axis])

    with scope("issue"):
        loads = {
            name: pltpu.make_async_copy(src, dst, in_sem.at[n])
            for name, n, src, dst in (
                ("v", 1, v_in, v.at[0]),
                ("cell", 0, cell_in, slots.at[0]),
                ("node", 0, node_in, slots.at[1]),
                ("kind", 0, kind_in, slots.at[2]),
                ("w", 2, w_in, w_first),
                ("coup", 3, coup_in, coup),
                ("shift", 4, shift_in, shift),
                ("diag", 5, diag_in, diag),
                ("off", 6, off_in, off),
            )
        }
        for load in loads.values():
            load.start()

    def hops(shifts):
        return sum(min(d, sizes[a] - d) for a, d in shifts.items())

    line = [{"gx": d} for d in range(1, sizes["gx"])]
    plane = [
        {"gy": dy, "ea": dx}
        for dy in range(sizes["gy"])
        for dx in range(sizes["ea"])
        if dy or dx
    ]
    line.sort(key=hops)
    plane.sort(key=hops, reverse=True)
    def near(axis, *reach):
        n = sizes[axis]
        return [{axis: d} for d in sorted({d % n for r in reach for d in (r, n - r)} - {0})]

    first = near("gx", 1) + near("gy", 1) + near("ea", 1, 2)
    rounds = [near("gx", r) + near("gy", r) for r in (1, 2, 4)]

    def signal(sem, shifts):
        pl.semaphore_signal(
            sem,
            inc=1,
            device_id={a: other(a, d) for a, d in shifts.items()},
            device_id_type=pl.DeviceIdType.MESH,
        )

    def send_token(t):
        for shifts in rounds[t]:
            signal(tokens.at[t], shifts)

    def wait_token(t):
        pl.semaphore_wait(tokens.at[t], len(rounds[t]))

    with scope("signals"):
        barrier = pltpu.get_barrier_semaphore()
        for shifts in first:
            signal(barrier, shifts)

    low_edge = [me[a] == 0 for a in AXES]
    high_edge = [me[a] == sizes[a] - 1 for a in AXES]
    halos = (hx, hy, hz)
    with scope("edges"):
        for n in range(3):

            @pl.when(low_edge[n])
            def _():
                halos[n][:, 0] = jnp.zeros_like(halos[n][:, 0])

            @pl.when(high_edge[n])
            def _():
                halos[n][:, 1] = jnp.zeros_like(halos[n][:, 1])

    def remote(src, dst, send_sem, recv_sem, shifts):
        return pltpu.make_async_remote_copy(
            src_ref=src,
            dst_ref=dst,
            send_sem=send_sem,
            recv_sem=recv_sem,
            device_id={a: other(a, d) for a, d in shifts.items()},
            device_id_type=pl.DeviceIdType.MESH,
        )

    def wait_bytes(ref, sem):
        pltpu.make_async_copy(ref, ref, sem).wait()

    def halo_copies(k, n):
        sources = (
            (v.at[k, :, CX - 1], v.at[k, :, 0]),
            (sy.at[k, 0], sy.at[k, 1]),
            (sz.at[k, 0], sz.at[k, 1]),
        )
        a = AXES[n]
        return [
            remote(
                sources[n][side],
                halos[n].at[k, side],
                sent,
                halo_recv.at[k % 2, n],
                {a: d},
            )
            for side, d in ((0, 1), (1, sizes[a] - 1))
        ]

    def on_halos(k, n, there, act):
        for copy, edge in zip(halo_copies(k, n), there[n]):

            @pl.when(jnp.logical_not(edge))
            def _():
                act(copy)

    going = list(zip(high_edge, low_edge))

    def w_copy(k, d):
        src, dst = (w.at[0], wfirst.at[d - 1]) if k == 0 else (wsend.at[k, d - 1], wrecv.at[k, d - 1])
        return remote(src, dst, sent, w_recv.at[k % 2], {"ea": d})

    def t_copy(k, d):
        src = tsend.at[k, other("ea", d)]
        return remote(src, trecv.at[k, d - 1], sent, t_recv.at[k % 2], {"ea": d})

    def node_copy(d):
        return remote(
            node_rows.at[other("ea", d)], their_nodes.at[d - 1], sent, node_recv, {"ea": d}
        )

    lane = iota((CY, CZ), 1)
    row = iota((CY, CZ), 0)

    half = iota((8, CZ), 1)

    def turned(tile, by):
        return pltpu.roll(tile, by % CZ, 1) if by % CZ else tile

    def pack_rows(k):
        for g in range(FACES):
            i, x = divmod(g, CX)
            sy[k, 0, pl.ds(g, 1), :] = v[k, i, x, pl.ds(CY - 1, 1), :]
            sy[k, 1, pl.ds(g, 1), :] = v[k, i, x, pl.ds(0, 1), :]

    def pack_lanes(k):
        last = jnp.zeros((8, CZ), F32)
        first = jnp.zeros((8, CZ), F32)
        for g in range(FACES):
            i, x = divmod(g, CX)
            for top in (0, 1):
                tile = v[k, i, x, pl.ds(8 * top, 8), :]
                at = g + FACES * top
                last = jnp.where(half == at, turned(tile, at + 1), last)
                first = jnp.where(half == at, turned(tile, at), first)
        sz[k, 0] = last
        sz[k, 1] = first

    def unpacked(faces, g, to):
        return jnp.concatenate(
            [turned(faces, to - g - FACES * top) for top in (0, 1)], axis=0
        )

    def terms_for_nodes(k):
        both_parts = jnp.concatenate(two_parts(v[k].reshape(COMP * ROWS, CZ)), axis=1)
        spread = [dot_nn(both_parts, gather_hot[n]) for n in range(OWNERS // 2)]
        for o in range(OWNERS):
            cols = slice(o % 2 * CAP, (o % 2 + 1) * CAP)
            term = jnp.zeros((EPAD, CAP), F32)
            for i in range(COMP):
                rows = spread[o // 2][i * ROWS : (i + 1) * ROWS, cols]
                picked = jnp.sum(rows * row_mask[o], axis=0, keepdims=True)
                term = term + weights[o, i] * picked
            tsend[k, o] = term
        return tsend[k, ea]

    def own_terms(term):
        both = dot_nt(jnp.concatenate(two_parts(term), axis=0), node_hot[ea])
        return both[:EPAD] + both[EPAD:]

    def values_at(values, hot):
        both = dot_nn(jnp.concatenate(two_parts(values), axis=0), hot)
        return both[:EPAD] + both[EPAD:]

    def terms_for_cells(k, distances):
        owners = {d: other("ea", OWNERS - d) for d in distances}
        value = {}
        for d in distances:
            if d == 0:
                value[d] = values_at(w[k], node_hot[ea])
            elif k == 0:
                value[d] = values_at(wfirst[d - 1], node_hot[owners[d]])
            else:
                value[d] = wrecv[k, d - 1]
        for d in distances:
            hot = row_hot[owners[d]]
            for i in range(COMP):
                total = jnp.sum(weights[owners[d], i] * value[d], axis=0, keepdims=True)
                for part, piece in enumerate(two_parts(jnp.broadcast_to(total, (CY, CAP)))):
                    for x in range(CX):
                        spread_rows[d, i, x, :, part * CAP : (part + 1) * CAP] = (
                            hot[x * CY : (x + 1) * CY] * piece
                        )
        added = sum(
            dot_nt(spread_rows[d].reshape(COMP * ROWS, 2 * CAP), scatter_hot[owners[d]])
            for d in distances
        )
        return added.reshape(COMP, CX, CY, CZ)

    def inner_part(k):
        for i in range(COMP):
            for x in range(CX):
                tile = v[k, i, x]
                beside = jnp.where(row > 0, pltpu.roll(tile, 1, 0), 0.0)
                beside += jnp.where(row < CY - 1, pltpu.roll(tile, CY - 1, 0), 0.0)
                beside += jnp.where(lane > 0, pltpu.roll(tile, 1, 1), 0.0)
                beside += jnp.where(lane < CZ - 1, pltpu.roll(tile, CZ - 1, 1), 0.0)
                if x > 0:
                    beside += v[k, i, x - 1]
                if x < CX - 1:
                    beside += v[k, i, x + 1]
                acc[i, x] = ((shift[x] + (6.0 - CENTER)) * tile - beside) * INV

    def outer_part(k, target):
        low_z, high_z = hz[k, 0], hz[k, 1]
        for i in range(COMP):
            for x in range(CX):
                g = i * CX + x
                beside = jnp.where(row == 0, hy[k, 0, pl.ds(g, 1), :], 0.0)
                beside += jnp.where(row == CY - 1, hy[k, 1, pl.ds(g, 1), :], 0.0)
                beside += jnp.where(lane == 0, unpacked(low_z, g, 0), 0.0)
                beside += jnp.where(lane == CZ - 1, unpacked(high_z, g, CZ - 1), 0.0)
                if x == 0:
                    beside += hx[k, 0, i]
                if x == CX - 1:
                    beside += hx[k, 1, i]
                target[i, x] = acc[i, x] - beside * INV

    def fold_v(left, right):
        return jnp.sum((left * right).reshape(FACES * CY // 8, 8, CZ), axis=0)

    def fold_w(prod):
        return prod[0:8, 0:128] + prod[0:8, 128:256] + prod[8:16, 0:128] + prod[8:16, 128:256]

    def local_product(j, k):
        return fold_v(v[j], v[k]) + fold_w(w[j] * w[k])

    with scope("tables_wait"):
        wait_bytes(slots, in_sem.at[0])
    with scope("tables"):
        for o in range(OWNERS):
            cells = slots[0, 0, o : o + 1, :]
            nodes = slots[1, 0, o : o + 1, :]
            node_rows[o] = nodes
            hot = (iota((CZ, CAP), 0) == jnp.bitwise_and(cells, CZ - 1)).astype(F32).astype(BF16)
            cols = slice(o % 2 * CAP, (o % 2 + 1) * CAP)
            gather_hot[o // 2, 0:CZ, cols] = hot
            gather_hot[o // 2, CZ : 2 * CZ, cols] = hot
            scatter_hot[o, :, 0:CAP] = hot
            scatter_hot[o, :, CAP : 2 * CAP] = hot
            mask = (iota((ROWS, CAP), 0) == lax.shift_right_logical(cells, 7)).astype(F32)
            row_mask[o] = mask
            row_hot[o] = mask.astype(BF16)
            node_hot[o] = (
                (iota((ENB, CAP), 0) == nodes).astype(F32).astype(BF16)
            )

    with scope("vw_wait"):
        loads["v"].wait()
        loads["w"].wait()
    with scope("pack_0"):
        for k in range(ITERS + 1):
            w[k, 8:16, :] = jnp.zeros((8, ENB), F32)
        w[0, 0:ECOMP, :] = w_first[...]
        pack_rows(0)
        pack_lanes(0)
    with scope("weights"):
        loads["coup"].wait()
        needed = jnp.where(iota((ECOMP, CAP), 0) < 3, 1, 2)
        for o in range(OWNERS):
            live = slots[2, 0, o : o + 1, :] >= needed
            for i in range(COMP):
                weights[o, i, 8:16] = jnp.zeros((8, CAP), F32)
                weights[o, i, 0:ECOMP] = jnp.where(
                    live, coup[i, :, o * CAP : (o + 1) * CAP] * INV, 0.0
                )
    with scope("nodes_0"):
        own = terms_for_nodes(0)
    with scope("barrier_wait"):
        pl.semaphore_wait(barrier, len(first))

    def send_halos(k, axes=(2, 1, 0)):
        for n in axes:
            on_halos(k, n, going, lambda copy: copy.start())

    def wait_halos(k):
        for n in range(3):
            sem = halo_recv.at[k % 2, n]
            low, high = low_edge[n], high_edge[n]

            @pl.when(jnp.logical_not(jnp.logical_or(low, high)))
            def _():
                wait_bytes(halos[n].at[k], sem)

            @pl.when(low)
            def _():
                wait_bytes(halos[n].at[k, 1], sem)

            @pl.when(high)
            def _():
                wait_bytes(halos[n].at[k, 0], sem)

    def send_terms(k):
        for d in (2, 1, 3):
            t_copy(k, d).start()

    def send_w(k):
        if k > 0:
            values = values_at(w[k], their_hot[...])
            for d in (2, 1, 3):
                wsend[k, OWNERS - d - 1] = values[:, (d - 1) * CAP : d * CAP]
        for d in (2, 1, 3):
            w_copy(k, d).start()

    def stiff_times(k):
        out = own_terms(own)[0:ECOMP]
        for q in range(ECOMP):
            out = out + stiff[q] * w[k, pl.ds(q, 1), :]
        return out

    def next_w(k, pushed):
        wait_bytes(trecv.at[k], t_recv.at[k % 2])
        pieces = [two_parts(trecv[k, d]) for d in range(OWNERS - 1)]
        rows = [jnp.concatenate([p[n] for p in pieces], axis=1) for n in (0, 1)]
        both = dot_nt(jnp.concatenate(rows, axis=0), their_hot[...])
        came[...] = both[:EPAD] + both[EPAD:]
        w[k + 1, 0:ECOMP, :] = pushed + came[0:ECOMP]

    def wait_w(k):
        wait_bytes(wfirst if k == 0 else wrecv.at[k], w_recv.at[k % 2])

    def next_v(k):
        with scope(f"w_wait_{k}"):
            wait_w(k)
        with scope(f"cells_{k}"):
            acc[...] += terms_for_cells(k, (1, 3, 2))
        if k == 1:
            with scope("token_2"):
                wait_token(1)
                send_token(2)
        with scope(f"halo_wait_{k}"):
            wait_halos(k)
        with scope(f"outer_{k}"):
            outer_part(k, v.at[k + 1])

    parts = [None] * (MOMENTS - 1)
    last = ITERS - 1

    with scope("send_0"):
        for d in (2, 1, 3):
            node_copy(d).start()
        send_halos(0)
        send_terms(0)
        send_w(0)
        send_token(0)
    with scope("inner_0"):
        loads["shift"].wait()
        inner_part(0)
    with scope("stiff"):
        loads["diag"].wait()
        loads["off"].wait()
        comp = iota((ECOMP, ENB), 0)
        for q in range(ECOMP):
            both = (off[q] + off[:, q, :]) * (0.5 * INV)
            stiff[q] = jnp.where(comp == q, (diag[...] - CENTER) * INV, both)
    with scope("pushed_0"):
        pushed = stiff_times(0)
        parts[0] = local_product(0, 0)
        acc[...] += terms_for_cells(0, (0,))
    with scope("their_nodes"):
        wait_bytes(their_nodes, node_recv)
        for d in range(OWNERS - 1):
            their_hot[:, d * CAP : (d + 1) * CAP] = (
                (iota((ENB, CAP), 0) == their_nodes[d]).astype(F32).astype(BF16)
            )
    with scope("w_next_0"):
        next_w(0, pushed)
        send_w(1)
    with scope("token_1"):
        wait_token(0)
        send_token(1)
    next_v(0)

    with scope("pack_1"):
        pack_rows(1)
        send_halos(1, (1, 0))
        pack_lanes(1)
        send_halos(1, (2,))
    with scope("nodes_1"):
        own = terms_for_nodes(1)
        send_terms(1)
    with scope("inner_1"):
        inner_part(1)
        parts[1] = local_product(0, 1)
        parts[2] = local_product(1, 1)
        acc[...] += terms_for_cells(1, (0,))
        pushed = stiff_times(1)
    next_v(1)

    with scope("nodes_2"):
        pack_rows(2)
        pack_lanes(2)
        own = terms_for_nodes(2)
        send_halos(2)
        send_terms(2)
    with scope("w_next_1"):
        next_w(1, pushed)
        send_w(2)
    with scope("inner_2"):
        inner_part(2)
        parts[3] = local_product(1, 2)
        parts[4] = local_product(2, 2)
        own_node_terms = own_terms(own)
        pushed = stiff_times(2)
        at = iota((8, 128), 1)
        tile = jnp.zeros((8, 128), F32)
        for m in range(MOMENTS - 1):
            tile = jnp.where(at == m, jnp.sum(parts[m], axis=1, keepdims=True), tile)
    with scope("halo_wait_2"):
        wait_halos(2)
    with scope("outer_2"):
        outer_part(2, acc)
        final = fold_v(v[last], acc[...])
    with scope("w_next_2"):
        next_w(2, pushed)

    with scope("moments"):
        twice = own_node_terms + came[...]
        final = final + fold_w(w[last] * (w[last + 1] + twice))
        tile = jnp.where(at == MOMENTS - 1, jnp.sum(final, axis=1, keepdims=True), tile)
        total = jnp.sum(tile, axis=0, keepdims=True)

    def send_total(buf, at, recv_sem, group):
        mine = buf.at[at]
        mine[...] = total
        copies = [
            remote(mine, mine, sent, recv_sem, shifts)
            for shifts in group
        ]
        for copy in copies:
            copy.start()
        return buf.at[pl.ds(0, len(group))]

    with scope("token_end"):
        wait_token(TOKENS - 1)
    with scope("line_send"):
        on_line = send_total(red_line, me["gx"], line_recv, line)
    with scope("cells_last"):
        wait_w(last)
        v[last + 1] = acc[...] + terms_for_cells(last, (0, 1, 3, 2))
    with scope("out_send"):
        out = [
            pltpu.make_async_copy(v, v_out, sent),
            pltpu.make_async_copy(w, w_out, sent),
        ]
        for copy in out:
            copy.start()
    with scope("line_wait"):
        wait_bytes(on_line, line_recv)
        total = jnp.sum(red_line[...], axis=0)
    with scope("plane_send"):
        on_plane = send_total(
            red_plane, me["gy"] * sizes["ea"] + ea, plane_recv, plane
        )
    with scope("plane_wait"):
        wait_bytes(on_plane, plane_recv)
        moments[...] = jnp.sum(red_plane[...], axis=0)
    with scope("ends"):
        for n in range(3):
            for side, edge in enumerate(going[n]):

                @pl.when(jnp.logical_not(edge))
                def _():
                    wait_bytes(halos[n].at[:, side], sent)

        for ref in (their_nodes, wfirst, wrecv.at[pl.ds(1, ITERS - 1)], trecv, on_line, on_plane, v, w):
            wait_bytes(ref, sent)


def combine(v, w_all, moments, sol_v, res_v, sol_w, res_w):
    total = moments[...]
    flat = iota((1, 128), 1)
    mu = [
        jnp.broadcast_to(
            jnp.sum(jnp.where(flat == m, total, 0.0), axis=1, keepdims=True), (1, 128)
        )
        for m in range(MOMENTS)
    ]

    def form(left, right):
        out = None
        for i, p in enumerate(left):
            for j, q in enumerate(right):
                term = p * q * mu[i + j]
                out = term if out is None else out + term
        return out

    zero = jnp.zeros((1, 128), F32)
    sol, res, way = [zero] * ITERS, [zero + 1.0] + [zero] * ITERS, [zero + 1.0]
    norm = mu[0]
    for it in range(ITERS):
        image = [zero] * (it + 2)
        for j, p in enumerate(way):
            image[j] = image[j] + CENTER * p
            image[j + 1] = image[j + 1] + SPREAD * p
        alpha = norm / form(way, image)
        for j, p in enumerate(way):
            sol[j] = sol[j] + alpha * p
        for j, p in enumerate(image):
            res[j] = res[j] - alpha * p
        if it + 1 < ITERS:
            norm_next = form(res[: it + 2], res[: it + 2])
            ratio = norm_next / norm
            way = [res[j] + (ratio * way[j] if j < len(way) else 0.0) for j in range(it + 2)]
            norm = norm_next

    for i in range(COMP):
        for x in range(CX):
            b = [v[k, i, x] for k in range(ITERS + 1)]
            sol_v[i, x] = sum(sol[k] * b[k] for k in range(ITERS))
            res_v[i, x] = sum(res[k] * b[k] for k in range(ITERS + 1))
    spread = [
        (jnp.concatenate([sol[k]] * 2, axis=1) if k < ITERS else None,
         jnp.concatenate([res[k]] * 2, axis=1))
        for k in range(ITERS + 1)
    ]
    b = [w_all[k, 0:ECOMP, :] for k in range(ITERS + 1)]
    sol_w[...] = sum(spread[k][0] * b[k] for k in range(ITERS))
    res_w[...] = sum(spread[k][1] * b[k] for k in range(ITERS + 1))


def body(sizes, *args):
    v_in, w_in = args[0], args[1]
    vmem, dma = pltpu.VMEM, pltpu.SemaphoreType.DMA
    steps = ITERS
    basis = pl.pallas_call(
        functools.partial(kernel, sizes),
        name="krylov",
        out_shape=(
            vmem((steps + 1, COMP, CX, CY, CZ), F32),
            vmem((steps + 1, EPAD, ENB), F32),
            vmem((1, 128), F32),
        ),
        in_specs=[pl.BlockSpec(memory_space=pl.ANY)] * len(args),
        out_specs=[pl.BlockSpec(memory_space=pl.ANY)] * 2
        + [pl.BlockSpec(memory_space=pltpu.VMEM)],
        scratch_shapes=[
            vmem((steps + 1, COMP, CX, CY, CZ), F32),
            vmem((steps + 1, EPAD, ENB), F32),
            vmem((ECOMP, ENB), F32),
            vmem((CX, CY, CZ), F32),
            vmem((ECOMP, ENB), F32),
            vmem((ECOMP, ECOMP, ENB), F32),
            vmem((COMP, ECOMP, SLOTS), F32),
            vmem((3, 1, OWNERS, CAP), jnp.int32),
            vmem((OWNERS, 1, CAP), jnp.int32),
            vmem((OWNERS - 1, 1, CAP), jnp.int32),
            vmem((ENB, (OWNERS - 1) * CAP), BF16),
            vmem((COMP, CX, CY, CZ), F32),
            vmem((OWNERS, COMP, EPAD, CAP), F32),
            vmem((ECOMP, ECOMP, ENB), F32),
            vmem((OWNERS // 2, 2 * CZ, 2 * CAP), BF16),
            vmem((OWNERS, CZ, 2 * CAP), BF16),
            vmem((OWNERS, ROWS, CAP), BF16),
            vmem((OWNERS, ROWS, CAP), F32),
            vmem((OWNERS, ENB, CAP), BF16),
            vmem((OWNERS, COMP, CX, CY, 2 * CAP), BF16),
            vmem((steps, OWNERS - 1, EPAD, CAP), F32),
            vmem((steps, OWNERS - 1, EPAD, CAP), F32),
            vmem((OWNERS - 1, EPAD, ENB), F32),
            vmem((steps, OWNERS, EPAD, CAP), F32),
            vmem((steps, OWNERS - 1, EPAD, CAP), F32),
            vmem((EPAD, ENB), F32),
            vmem((steps, 2, COMP, CY, CZ), F32),
            vmem((steps, 2, 16, CZ), F32),
            vmem((steps, 2, 8, CZ), F32),
            vmem((steps, 2, 16, CZ), F32),
            vmem((steps, 2, 8, CZ), F32),
            vmem((sizes["gx"], 1, 128), F32),
            vmem((sizes["gy"] * sizes["ea"], 1, 128), F32),
            pltpu.SemaphoreType.REGULAR((TOKENS,)),
            dma((7,)),
            dma,
            dma,
            dma((2, 3)),
            dma((2,)),
            dma((2,)),
            dma,
            dma,
        ],
        compiler_params=pltpu.CompilerParams(collective_id=0, has_side_effects=True),
    )(*args)
    return pl.pallas_call(
        combine,
        name="combine",
        out_shape=(
            jax.ShapeDtypeStruct(v_in.shape, F32),
            jax.ShapeDtypeStruct(v_in.shape, F32),
            jax.ShapeDtypeStruct(w_in.shape, F32),
            jax.ShapeDtypeStruct(w_in.shape, F32),
        ),
        in_specs=[pl.BlockSpec(memory_space=pltpu.VMEM)] * 3,
        out_specs=[pl.BlockSpec(memory_space=pltpu.VMEM)] * 4,
        compiler_params=pltpu.CompilerParams(vmem_limit_bytes=VMEM_LIMIT),
    )(*(pltpu.with_memory_space_constraint(b, pltpu.VMEM) for b in basis))


def solution(mesh):
    sizes = {a: mesh.shape[a] for a in AXES}
    return jax.shard_map(
        functools.partial(body, sizes),
        mesh=mesh,
        in_specs=(
            P(None, "gx", "gy", "ea"),
            P(None, GX_GY_EA),
            P("gx", "gy", "ea"),
            P(None, GX_GY_EA),
            P(None, None, GX_GY_EA),
            P(None, None, GX_GY_EA),
            P(GX_GY_EA, None, None),
            P(GX_GY_EA, None, None),
            P(GX_GY_EA, None, None),
        ),
        out_specs=(
            P(None, "gx", "gy", "ea"),
            P(None, "gx", "gy", "ea"),
            P(None, GX_GY_EA),
            P(None, GX_GY_EA),
        ),
        check_vma=False,
    )
```

```python
import functools

import jax
import jax.numpy as jnp
from jax import lax
from jax.experimental import pallas as pl
from jax.experimental.pallas import tpu as pltpu
from jax.sharding import PartitionSpec as P

ITERS = 3
COMP = 3
CX = 4
CY = 16
CZ = 128
ROWS = CX * CY
FACES = COMP * CX
ECOMP = 15
EPAD = 16
ENB = 256
OWNERS = 4
CAP = 128
SLOTS = OWNERS * CAP
MOMENTS = 6
VMEM_LIMIT = 16 << 20
TOKENS = 3

CENTER = 12.0
SPREAD = 8.0
INV = 1.0 / SPREAD

F32 = jnp.float32
BF16 = jnp.bfloat16
GX_GY_EA = ("gx", "gy", "ea")
AXES = ("gx", "gy", "ea")


def two_parts(x):
    high = x.astype(BF16)
    low = (x - high.astype(F32)).astype(BF16)
    return high, low


def dot_nn(a, b):
    return lax.dot_general(a, b, (((1,), (0,)), ((), ())), preferred_element_type=F32)


def dot_nt(a, b):
    return lax.dot_general(a, b, (((1,), (1,)), ((), ())), preferred_element_type=F32)


def iota(shape, dim):
    return lax.broadcasted_iota(jnp.int32, shape, dim)


def kernel(
    sizes,
    v_in,
    w_in,
    shift_in,
    diag_in,
    off_in,
    coup_in,
    kind_in,
    cell_in,
    node_in,
    v_out,
    w_out,
    moments,
    v,
    w,
    w_first,
    shift,
    diag,
    off,
    coup,
    slots,
    node_rows,
    their_nodes,
    their_hot,
    acc,
    weights,
    stiff,
    gather_hot,
    scatter_hot,
    row_hot,
    row_mask,
    node_hot,
    spread_rows,
    wsend,
    wrecv,
    wfirst,
    tsend,
    trecv,
    came,
    hx,
    hy,
    hz,
    sy,
    sz,
    red_line,
    red_plane,
    tokens,
    in_sem,
    sent,
    node_recv,
    halo_recv,
    w_recv,
    t_recv,
    line_recv,
    plane_recv,
):
    scope = jax.named_scope
    me = {a: lax.axis_index(a) for a in AXES}
    ea = me["ea"]

    def other(axis, d):
        return lax.rem(me[axis] + d, sizes[axis])

    with scope("issue"):
        loads = {
            name: pltpu.make_async_copy(src, dst, in_sem.at[n])
            for name, n, src, dst in (
                ("v", 1, v_in, v.at[0]),
                ("cell", 0, cell_in, slots.at[0]),
                ("node", 0, node_in, slots.at[1]),
                ("kind", 0, kind_in, slots.at[2]),
                ("w", 2, w_in, w_first),
                ("coup", 3, coup_in, coup),
                ("shift", 4, shift_in, shift),
                ("diag", 5, diag_in, diag),
                ("off", 6, off_in, off),
            )
        }
        for load in loads.values():
            load.start()

    def hops(shifts):
        return sum(min(d, sizes[a] - d) for a, d in shifts.items())

    line = [{"gx": d} for d in range(1, sizes["gx"])]
    plane = [
        {"gy": dy, "ea": dx}
        for dy in range(sizes["gy"])
        for dx in range(sizes["ea"])
        if dy or dx
    ]
    line.sort(key=hops)
    plane.sort(key=hops, reverse=True)
    def near(axis, *reach):
        n = sizes[axis]
        return [{axis: d} for d in sorted({d % n for r in reach for d in (r, n - r)} - {0})]

    first = near("ea", 2) + near("ea", 1) + near("gy", 1) + near("gx", 1)
    rounds = [near("gx", r) + near("gy", r) for r in (1, 2, 4)]

    def signal(sem, shifts):
        pl.semaphore_signal(
            sem,
            inc=1,
            device_id={a: other(a, d) for a, d in shifts.items()},
            device_id_type=pl.DeviceIdType.MESH,
        )

    def send_token(t):
        for shifts in rounds[t]:
            signal(tokens.at[t], shifts)

    def wait_token(t):
        pl.semaphore_wait(tokens.at[t], len(rounds[t]))

    with scope("signals"):
        barrier = pltpu.get_barrier_semaphore()
        for shifts in first:
            signal(barrier, shifts)

    low_edge = [me[a] == 0 for a in AXES]
    high_edge = [me[a] == sizes[a] - 1 for a in AXES]
    halos = (hx, hy, hz)
    with scope("edges"):
        for n in range(3):

            @pl.when(low_edge[n])
            def _():
                halos[n][:, 0] = jnp.zeros_like(halos[n][:, 0])

            @pl.when(high_edge[n])
            def _():
                halos[n][:, 1] = jnp.zeros_like(halos[n][:, 1])

    def remote(src, dst, send_sem, recv_sem, shifts):
        return pltpu.make_async_remote_copy(
            src_ref=src,
            dst_ref=dst,
            send_sem=send_sem,
            recv_sem=recv_sem,
            device_id={a: other(a, d) for a, d in shifts.items()},
            device_id_type=pl.DeviceIdType.MESH,
        )

    def wait_bytes(ref, sem):
        pltpu.make_async_copy(ref, ref, sem).wait()

    def halo_copies(k, n):
        sources = (
            (v.at[k, :, CX - 1], v.at[k, :, 0]),
            (sy.at[k, 0], sy.at[k, 1]),
            (sz.at[k, 0], sz.at[k, 1]),
        )
        a = AXES[n]
        return [
            remote(
                sources[n][side],
                halos[n].at[k, side],
                sent,
                halo_recv.at[k % 2, n],
                {a: d},
            )
            for side, d in ((0, 1), (1, sizes[a] - 1))
        ]

    def on_halos(k, n, there, act):
        for copy, edge in zip(halo_copies(k, n), there[n]):

            @pl.when(jnp.logical_not(edge))
            def _():
                act(copy)

    going = list(zip(high_edge, low_edge))

    def w_copy(k, d):
        src, dst = (w.at[0], wfirst.at[d - 1]) if k == 0 else (wsend.at[k, d - 1], wrecv.at[k, d - 1])
        return remote(src, dst, sent, w_recv.at[k % 2], {"ea": d})

    def t_copy(k, d):
        src = tsend.at[k, other("ea", d)]
        return remote(src, trecv.at[k, d - 1], sent, t_recv.at[k % 2], {"ea": d})

    def node_copy(d):
        return remote(
            node_rows.at[other("ea", d)], their_nodes.at[d - 1], sent, node_recv, {"ea": d}
        )

    lane = iota((CY, CZ), 1)
    row = iota((CY, CZ), 0)

    half = iota((8, CZ), 1)

    def turned(tile, by):
        return pltpu.roll(tile, by % CZ, 1) if by % CZ else tile

    def pack_rows(k):
        for g in range(FACES):
            i, x = divmod(g, CX)
            sy[k, 0, pl.ds(g, 1), :] = v[k, i, x, pl.ds(CY - 1, 1), :]
            sy[k, 1, pl.ds(g, 1), :] = v[k, i, x, pl.ds(0, 1), :]

    def pack_lanes(k):
        last = jnp.zeros((8, CZ), F32)
        first = jnp.zeros((8, CZ), F32)
        for g in range(FACES):
            i, x = divmod(g, CX)
            for top in (0, 1):
                tile = v[k, i, x, pl.ds(8 * top, 8), :]
                at = g + FACES * top
                last = jnp.where(half == at, turned(tile, at + 1), last)
                first = jnp.where(half == at, turned(tile, at), first)
        sz[k, 0] = last
        sz[k, 1] = first

    def unpacked(faces, g, to):
        return jnp.concatenate(
            [turned(faces, to - g - FACES * top) for top in (0, 1)], axis=0
        )

    def terms_for_nodes(k):
        both_parts = jnp.concatenate(two_parts(v[k].reshape(COMP * ROWS, CZ)), axis=1)
        spread = [dot_nn(both_parts, gather_hot[n]) for n in range(OWNERS // 2)]
        for o in range(OWNERS):
            cols = slice(o % 2 * CAP, (o % 2 + 1) * CAP)
            term = jnp.zeros((EPAD, CAP), F32)
            for i in range(COMP):
                rows = spread[o // 2][i * ROWS : (i + 1) * ROWS, cols]
                picked = jnp.sum(rows * row_mask[o], axis=0, keepdims=True)
                term = term + weights[o, i] * picked
            tsend[k, o] = term
        return tsend[k, ea]

    def own_terms(term):
        both = dot_nt(jnp.concatenate(two_parts(term), axis=0), node_hot[ea])
        return both[:EPAD] + both[EPAD:]

    def values_at(values, hot):
        both = dot_nn(jnp.concatenate(two_parts(values), axis=0), hot)
        return both[:EPAD] + both[EPAD:]

    def terms_for_cells(k, distances):
        owners = {d: other("ea", OWNERS - d) for d in distances}
        value = {}
        for d in distances:
            if d == 0:
                value[d] = values_at(w[k], node_hot[ea])
            elif k == 0:
                value[d] = values_at(wfirst[d - 1], node_hot[owners[d]])
            else:
                value[d] = wrecv[k, d - 1]
        for d in distances:
            hot = row_hot[owners[d]]
            for i in range(COMP):
                total = jnp.sum(weights[owners[d], i] * value[d], axis=0, keepdims=True)
                for part, piece in enumerate(two_parts(jnp.broadcast_to(total, (CY, CAP)))):
                    for x in range(CX):
                        spread_rows[d, i, x, :, part * CAP : (part + 1) * CAP] = (
                            hot[x * CY : (x + 1) * CY] * piece
                        )
        added = sum(
            dot_nt(spread_rows[d].reshape(COMP * ROWS, 2 * CAP), scatter_hot[owners[d]])
            for d in distances
        )
        return added.reshape(COMP, CX, CY, CZ)

    def inner_part(k):
        for i in range(COMP):
            for x in range(CX):
                tile = v[k, i, x]
                beside = jnp.where(row > 0, pltpu.roll(tile, 1, 0), 0.0)
                beside += jnp.where(row < CY - 1, pltpu.roll(tile, CY - 1, 0), 0.0)
                beside += jnp.where(lane > 0, pltpu.roll(tile, 1, 1), 0.0)
                beside += jnp.where(lane < CZ - 1, pltpu.roll(tile, CZ - 1, 1), 0.0)
                if x > 0:
                    beside += v[k, i, x - 1]
                if x < CX - 1:
                    beside += v[k, i, x + 1]
                acc[i, x] = ((shift[x] + (6.0 - CENTER)) * tile - beside) * INV

    def outer_part(k, target):
        low_z, high_z = hz[k, 0], hz[k, 1]
        for i in range(COMP):
            for x in range(CX):
                g = i * CX + x
                beside = jnp.where(row == 0, hy[k, 0, pl.ds(g, 1), :], 0.0)
                beside += jnp.where(row == CY - 1, hy[k, 1, pl.ds(g, 1), :], 0.0)
                beside += jnp.where(lane == 0, unpacked(low_z, g, 0), 0.0)
                beside += jnp.where(lane == CZ - 1, unpacked(high_z, g, CZ - 1), 0.0)
                if x == 0:
                    beside += hx[k, 0, i]
                if x == CX - 1:
                    beside += hx[k, 1, i]
                target[i, x] = acc[i, x] - beside * INV

    def fold_v(left, right):
        return jnp.sum((left * right).reshape(FACES * CY // 8, 8, CZ), axis=0)

    def fold_w(prod):
        return prod[0:8, 0:128] + prod[0:8, 128:256] + prod[8:16, 0:128] + prod[8:16, 128:256]

    def local_product(j, k):
        return fold_v(v[j], v[k]) + fold_w(w[j] * w[k])

    with scope("tables_wait"):
        wait_bytes(slots, in_sem.at[0])
    with scope("tables"):
        for o in range(OWNERS):
            cells = slots[0, 0, o : o + 1, :]
            nodes = slots[1, 0, o : o + 1, :]
            node_rows[o] = nodes
            hot = (iota((CZ, CAP), 0) == jnp.bitwise_and(cells, CZ - 1)).astype(F32).astype(BF16)
            cols = slice(o % 2 * CAP, (o % 2 + 1) * CAP)
            gather_hot[o // 2, 0:CZ, cols] = hot
            gather_hot[o // 2, CZ : 2 * CZ, cols] = hot
            scatter_hot[o, :, 0:CAP] = hot
            scatter_hot[o, :, CAP : 2 * CAP] = hot
            mask = (iota((ROWS, CAP), 0) == lax.shift_right_logical(cells, 7)).astype(F32)
            row_mask[o] = mask
            row_hot[o] = mask.astype(BF16)
            node_hot[o] = (
                (iota((ENB, CAP), 0) == nodes).astype(F32).astype(BF16)
            )

    with scope("vw_wait"):
        loads["v"].wait()
        loads["w"].wait()
    with scope("pack_0"):
        for k in range(ITERS + 1):
            w[k, 8:16, :] = jnp.zeros((8, ENB), F32)
        w[0, 0:ECOMP, :] = w_first[...]
        pack_rows(0)
        pack_lanes(0)
    with scope("weights"):
        loads["coup"].wait()
        needed = jnp.where(iota((ECOMP, CAP), 0) < 3, 1, 2)
        for o in range(OWNERS):
            live = slots[2, 0, o : o + 1, :] >= needed
            for i in range(COMP):
                weights[o, i, 8:16] = jnp.zeros((8, CAP), F32)
                weights[o, i, 0:ECOMP] = jnp.where(
                    live, coup[i, :, o * CAP : (o + 1) * CAP] * INV, 0.0
                )
    with scope("nodes_0"):
        own = terms_for_nodes(0)
    with scope("barrier_wait"):
        pl.semaphore_wait(barrier, len(first))

    def send_halos(k, axes=(2, 1, 0)):
        for n in axes:
            on_halos(k, n, going, lambda copy: copy.start())

    def wait_halos(k):
        for n in range(3):
            sem = halo_recv.at[k % 2, n]
            low, high = low_edge[n], high_edge[n]

            @pl.when(jnp.logical_not(jnp.logical_or(low, high)))
            def _():
                wait_bytes(halos[n].at[k], sem)

            @pl.when(low)
            def _():
                wait_bytes(halos[n].at[k, 1], sem)

            @pl.when(high)
            def _():
                wait_bytes(halos[n].at[k, 0], sem)

    def send_terms(k):
        for d in (2, 1, 3):
            t_copy(k, d).start()

    def send_w(k):
        if k > 0:
            values = values_at(w[k], their_hot[...])
            for d in (2, 1, 3):
                wsend[k, OWNERS - d - 1] = values[:, (d - 1) * CAP : d * CAP]
        for d in (2, 1, 3):
            w_copy(k, d).start()

    def stiff_times(k):
        out = own_terms(own)[0:ECOMP]
        for q in range(ECOMP):
            out = out + stiff[q] * w[k, pl.ds(q, 1), :]
        return out

    def next_w(k, pushed):
        wait_bytes(trecv.at[k], t_recv.at[k % 2])
        pieces = [two_parts(trecv[k, d]) for d in range(OWNERS - 1)]
        rows = [jnp.concatenate([p[n] for p in pieces], axis=1) for n in (0, 1)]
        both = dot_nt(jnp.concatenate(rows, axis=0), their_hot[...])
        came[...] = both[:EPAD] + both[EPAD:]
        w[k + 1, 0:ECOMP, :] = pushed + came[0:ECOMP]

    def wait_w(k):
        wait_bytes(wfirst if k == 0 else wrecv.at[k], w_recv.at[k % 2])

    def next_v(k):
        with scope(f"w_wait_{k}"):
            wait_w(k)
        with scope(f"cells_{k}"):
            acc[...] += terms_for_cells(k, (1, 3, 2))
        if k == 1:
            with scope("token_2"):
                wait_token(1)
                send_token(2)
        with scope(f"halo_wait_{k}"):
            wait_halos(k)
        with scope(f"outer_{k}"):
            outer_part(k, v.at[k + 1])

    parts = [None] * (MOMENTS - 1)
    last = ITERS - 1

    with scope("send_0"):
        for d in (2, 1, 3):
            node_copy(d).start()
        send_halos(0)
        send_terms(0)
        send_w(0)
        send_token(0)
    with scope("inner_0"):
        loads["shift"].wait()
        inner_part(0)
    with scope("stiff"):
        loads["diag"].wait()
        loads["off"].wait()
        comp = iota((ECOMP, ENB), 0)
        for q in range(ECOMP):
            both = (off[q] + off[:, q, :]) * (0.5 * INV)
            stiff[q] = jnp.where(comp == q, (diag[...] - CENTER) * INV, both)
    with scope("pushed_0"):
        pushed = stiff_times(0)
        parts[0] = local_product(0, 0)
        acc[...] += terms_for_cells(0, (0,))
    with scope("their_nodes"):
        wait_bytes(their_nodes, node_recv)
        for d in range(OWNERS - 1):
            their_hot[:, d * CAP : (d + 1) * CAP] = (
                (iota((ENB, CAP), 0) == their_nodes[d]).astype(F32).astype(BF16)
            )
    with scope("w_next_0"):
        next_w(0, pushed)
        send_w(1)
    with scope("token_1"):
        wait_token(0)
        send_token(1)
    next_v(0)

    with scope("pack_1"):
        pack_rows(1)
        send_halos(1, (1, 0))
        pack_lanes(1)
        send_halos(1, (2,))
    with scope("nodes_1"):
        own = terms_for_nodes(1)
        send_terms(1)
    with scope("inner_1"):
        inner_part(1)
        parts[1] = local_product(0, 1)
        parts[2] = local_product(1, 1)
        acc[...] += terms_for_cells(1, (0,))
        pushed = stiff_times(1)
    next_v(1)

    with scope("nodes_2"):
        pack_rows(2)
        pack_lanes(2)
        own = terms_for_nodes(2)
        send_halos(2)
        send_terms(2)
    with scope("w_next_1"):
        next_w(1, pushed)
        send_w(2)
    with scope("inner_2"):
        inner_part(2)
        parts[3] = local_product(1, 2)
        parts[4] = local_product(2, 2)
        own_node_terms = own_terms(own)
        pushed = stiff_times(2)
        at = iota((8, 128), 1)
        tile = jnp.zeros((8, 128), F32)
        for m in range(MOMENTS - 1):
            tile = jnp.where(at == m, jnp.sum(parts[m], axis=1, keepdims=True), tile)
    with scope("halo_wait_2"):
        wait_halos(2)
    with scope("outer_2"):
        outer_part(2, acc)
        final = fold_v(v[last], acc[...])
    with scope("w_next_2"):
        next_w(2, pushed)

    with scope("moments"):
        twice = own_node_terms + came[...]
        final = final + fold_w(w[last] * (w[last + 1] + twice))
        tile = jnp.where(at == MOMENTS - 1, jnp.sum(final, axis=1, keepdims=True), tile)
        total = jnp.sum(tile, axis=0, keepdims=True)

    def send_total(buf, at, recv_sem, group):
        mine = buf.at[at]
        mine[...] = total
        copies = [
            remote(mine, mine, sent, recv_sem, shifts)
            for shifts in group
        ]
        for copy in copies:
            copy.start()
        return buf.at[pl.ds(0, len(group))]

    with scope("token_end"):
        wait_token(TOKENS - 1)
    with scope("line_send"):
        on_line = send_total(red_line, me["gx"], line_recv, line)
    with scope("cells_last"):
        wait_w(last)
        v[last + 1] = acc[...] + terms_for_cells(last, (0, 1, 3, 2))
    with scope("out_send"):
        out = [
            pltpu.make_async_copy(v, v_out, sent),
            pltpu.make_async_copy(w, w_out, sent),
        ]
        for copy in out:
            copy.start()
    with scope("line_wait"):
        wait_bytes(on_line, line_recv)
        total = jnp.sum(red_line[...], axis=0)
    with scope("plane_send"):
        on_plane = send_total(
            red_plane, me["gy"] * sizes["ea"] + ea, plane_recv, plane
        )
    with scope("plane_wait"):
        wait_bytes(on_plane, plane_recv)
        moments[...] = jnp.sum(red_plane[...], axis=0)
    with scope("ends"):
        for n in range(3):
            for side, edge in enumerate(going[n]):

                @pl.when(jnp.logical_not(edge))
                def _():
                    wait_bytes(halos[n].at[:, side], sent)

        for ref in (their_nodes, wfirst, wrecv.at[pl.ds(1, ITERS - 1)], trecv, on_line, on_plane, v, w):
            wait_bytes(ref, sent)


def combine(v, w_all, moments, sol_v, res_v, sol_w, res_w):
    total = moments[...]
    flat = iota((1, 128), 1)
    mu = [
        jnp.broadcast_to(
            jnp.sum(jnp.where(flat == m, total, 0.0), axis=1, keepdims=True), (1, 128)
        )
        for m in range(MOMENTS)
    ]

    def form(left, right):
        out = None
        for i, p in enumerate(left):
            for j, q in enumerate(right):
                term = p * q * mu[i + j]
                out = term if out is None else out + term
        return out

    zero = jnp.zeros((1, 128), F32)
    sol, res, way = [zero] * ITERS, [zero + 1.0] + [zero] * ITERS, [zero + 1.0]
    norm = mu[0]
    for it in range(ITERS):
        image = [zero] * (it + 2)
        for j, p in enumerate(way):
            image[j] = image[j] + CENTER * p
            image[j + 1] = image[j + 1] + SPREAD * p
        alpha = norm / form(way, image)
        for j, p in enumerate(way):
            sol[j] = sol[j] + alpha * p
        for j, p in enumerate(image):
            res[j] = res[j] - alpha * p
        if it + 1 < ITERS:
            norm_next = form(res[: it + 2], res[: it + 2])
            ratio = norm_next / norm
            way = [res[j] + (ratio * way[j] if j < len(way) else 0.0) for j in range(it + 2)]
            norm = norm_next

    for i in range(COMP):
        for x in range(CX):
            b = [v[k, i, x] for k in range(ITERS + 1)]
            sol_v[i, x] = sum(sol[k] * b[k] for k in range(ITERS))
            res_v[i, x] = sum(res[k] * b[k] for k in range(ITERS + 1))
    spread = [
        (jnp.concatenate([sol[k]] * 2, axis=1) if k < ITERS else None,
         jnp.concatenate([res[k]] * 2, axis=1))
        for k in range(ITERS + 1)
    ]
    b = [w_all[k, 0:ECOMP, :] for k in range(ITERS + 1)]
    sol_w[...] = sum(spread[k][0] * b[k] for k in range(ITERS))
    res_w[...] = sum(spread[k][1] * b[k] for k in range(ITERS + 1))


def body(sizes, *args):
    v_in, w_in = args[0], args[1]
    vmem, dma = pltpu.VMEM, pltpu.SemaphoreType.DMA
    steps = ITERS
    basis = pl.pallas_call(
        functools.partial(kernel, sizes),
        name="krylov",
        out_shape=(
            vmem((steps + 1, COMP, CX, CY, CZ), F32),
            vmem((steps + 1, EPAD, ENB), F32),
            vmem((1, 128), F32),
        ),
        in_specs=[pl.BlockSpec(memory_space=pl.ANY)] * len(args),
        out_specs=[pl.BlockSpec(memory_space=pl.ANY)] * 2
        + [pl.BlockSpec(memory_space=pltpu.VMEM)],
        scratch_shapes=[
            vmem((steps + 1, COMP, CX, CY, CZ), F32),
            vmem((steps + 1, EPAD, ENB), F32),
            vmem((ECOMP, ENB), F32),
            vmem((CX, CY, CZ), F32),
            vmem((ECOMP, ENB), F32),
            vmem((ECOMP, ECOMP, ENB), F32),
            vmem((COMP, ECOMP, SLOTS), F32),
            vmem((3, 1, OWNERS, CAP), jnp.int32),
            vmem((OWNERS, 1, CAP), jnp.int32),
            vmem((OWNERS - 1, 1, CAP), jnp.int32),
            vmem((ENB, (OWNERS - 1) * CAP), BF16),
            vmem((COMP, CX, CY, CZ), F32),
            vmem((OWNERS, COMP, EPAD, CAP), F32),
            vmem((ECOMP, ECOMP, ENB), F32),
            vmem((OWNERS // 2, 2 * CZ, 2 * CAP), BF16),
            vmem((OWNERS, CZ, 2 * CAP), BF16),
            vmem((OWNERS, ROWS, CAP), BF16),
            vmem((OWNERS, ROWS, CAP), F32),
            vmem((OWNERS, ENB, CAP), BF16),
            vmem((OWNERS, COMP, CX, CY, 2 * CAP), BF16),
            vmem((steps, OWNERS - 1, EPAD, CAP), F32),
            vmem((steps, OWNERS - 1, EPAD, CAP), F32),
            vmem((OWNERS - 1, EPAD, ENB), F32),
            vmem((steps, OWNERS, EPAD, CAP), F32),
            vmem((steps, OWNERS - 1, EPAD, CAP), F32),
            vmem((EPAD, ENB), F32),
            vmem((steps, 2, COMP, CY, CZ), F32),
            vmem((steps, 2, 16, CZ), F32),
            vmem((steps, 2, 8, CZ), F32),
            vmem((steps, 2, 16, CZ), F32),
            vmem((steps, 2, 8, CZ), F32),
            vmem((sizes["gx"], 1, 128), F32),
            vmem((sizes["gy"] * sizes["ea"], 1, 128), F32),
            pltpu.SemaphoreType.REGULAR((TOKENS,)),
            dma((7,)),
            dma,
            dma,
            dma((2, 3)),
            dma((2,)),
            dma((2,)),
            dma,
            dma,
        ],
        compiler_params=pltpu.CompilerParams(collective_id=0, has_side_effects=True),
    )(*args)
    return pl.pallas_call(
        combine,
        name="combine",
        out_shape=(
            jax.ShapeDtypeStruct(v_in.shape, F32),
            jax.ShapeDtypeStruct(v_in.shape, F32),
            jax.ShapeDtypeStruct(w_in.shape, F32),
            jax.ShapeDtypeStruct(w_in.shape, F32),
        ),
        in_specs=[pl.BlockSpec(memory_space=pltpu.VMEM)] * 3,
        out_specs=[pl.BlockSpec(memory_space=pltpu.VMEM)] * 4,
        compiler_params=pltpu.CompilerParams(vmem_limit_bytes=VMEM_LIMIT),
    )(*(pltpu.with_memory_space_constraint(b, pltpu.VMEM) for b in basis))


def solution(mesh):
    sizes = {a: mesh.shape[a] for a in AXES}
    return jax.shard_map(
        functools.partial(body, sizes),
        mesh=mesh,
        in_specs=(
            P(None, "gx", "gy", "ea"),
            P(None, GX_GY_EA),
            P("gx", "gy", "ea"),
            P(None, GX_GY_EA),
            P(None, None, GX_GY_EA),
            P(None, None, GX_GY_EA),
            P(GX_GY_EA, None, None),
            P(GX_GY_EA, None, None),
            P(GX_GY_EA, None, None),
        ),
        out_specs=(
            P(None, "gx", "gy", "ea"),
            P(None, "gx", "gy", "ea"),
            P(None, GX_GY_EA),
            P(None, GX_GY_EA),
        ),
        check_vma=False,
    )
```

```python
import functools

import jax
import jax.numpy as jnp
from jax import lax
from jax.experimental import pallas as pl
from jax.experimental.pallas import tpu as pltpu
from jax.sharding import PartitionSpec as P

ITERS = 3
COMP = 3
CX = 4
CY = 16
CZ = 128
ROWS = CX * CY
FACES = COMP * CX
ECOMP = 15
EPAD = 16
ENB = 256
OWNERS = 4
CAP = 128
SLOTS = OWNERS * CAP
MOMENTS = 6
VMEM_LIMIT = 16 << 20
TOKENS = 3

CENTER = 12.0
SPREAD = 8.0
INV = 1.0 / SPREAD

F32 = jnp.float32
BF16 = jnp.bfloat16
GX_GY_EA = ("gx", "gy", "ea")
AXES = ("gx", "gy", "ea")


def two_parts(x):
    high = x.astype(BF16)
    low = (x - high.astype(F32)).astype(BF16)
    return high, low


def dot_nn(a, b):
    return lax.dot_general(a, b, (((1,), (0,)), ((), ())), preferred_element_type=F32)


def dot_nt(a, b):
    return lax.dot_general(a, b, (((1,), (1,)), ((), ())), preferred_element_type=F32)


def iota(shape, dim):
    return lax.broadcasted_iota(jnp.int32, shape, dim)


def kernel(
    sizes,
    v_in,
    w_in,
    shift_in,
    diag_in,
    off_in,
    coup_in,
    kind_in,
    cell_in,
    node_in,
    v_out,
    w_out,
    moments,
    v,
    w,
    w_first,
    shift,
    diag,
    off,
    coup,
    slots,
    node_rows,
    their_nodes,
    their_hot,
    acc,
    weights,
    stiff,
    gather_hot,
    scatter_hot,
    row_hot,
    row_mask,
    node_hot,
    spread_rows,
    wsend,
    wrecv,
    wfirst,
    tsend,
    trecv,
    came,
    hx,
    hy,
    hz,
    sy,
    sz,
    red_line,
    red_plane,
    tokens,
    in_sem,
    sent,
    node_recv,
    halo_recv,
    w_recv,
    t_recv,
    line_recv,
    plane_recv,
):
    scope = jax.named_scope
    me = {a: lax.axis_index(a) for a in AXES}
    ea = me["ea"]

    def other(axis, d):
        return lax.rem(me[axis] + d, sizes[axis])

    with scope("issue"):
        loads = {
            name: pltpu.make_async_copy(src, dst, in_sem.at[n])
            for name, n, src, dst in (
                ("v", 1, v_in, v.at[0]),
                ("cell", 0, cell_in, slots.at[0]),
                ("node", 0, node_in, slots.at[1]),
                ("kind", 0, kind_in, slots.at[2]),
                ("w", 2, w_in, w_first),
                ("coup", 3, coup_in, coup),
                ("shift", 4, shift_in, shift),
                ("diag", 5, diag_in, diag),
                ("off", 6, off_in, off),
            )
        }
        for load in loads.values():
            load.start()

    def hops(shifts):
        return sum(min(d, sizes[a] - d) for a, d in shifts.items())

    line = [{"gx": d} for d in range(1, sizes["gx"])]
    plane = [
        {"gy": dy, "ea": dx}
        for dy in range(sizes["gy"])
        for dx in range(sizes["ea"])
        if dy or dx
    ]
    line.sort(key=hops)
    plane.sort(key=hops, reverse=True)
    def near(axis, *reach):
        n = sizes[axis]
        return [{axis: d} for d in sorted({d % n for r in reach for d in (r, n - r)} - {0})]

    first = near("ea", 2) + near("ea", 1) + near("gy", 1) + near("gx", 1)
    rounds = [near("gx", r) + near("gy", r) for r in (1, 2, 4)]

    def signal(sem, shifts):
        pl.semaphore_signal(
            sem,
            inc=1,
            device_id={a: other(a, d) for a, d in shifts.items()},
            device_id_type=pl.DeviceIdType.MESH,
        )

    def send_token(t):
        for shifts in rounds[t]:
            signal(tokens.at[t], shifts)

    def wait_token(t):
        pl.semaphore_wait(tokens.at[t], len(rounds[t]))

    with scope("signals"):
        barrier = pltpu.get_barrier_semaphore()
        for shifts in first:
            signal(barrier, shifts)

    low_edge = [me[a] == 0 for a in AXES]
    high_edge = [me[a] == sizes[a] - 1 for a in AXES]
    halos = (hx, hy, hz)
    with scope("edges"):
        for n in range(3):

            @pl.when(low_edge[n])
            def _():
                halos[n][:, 0] = jnp.zeros_like(halos[n][:, 0])

            @pl.when(high_edge[n])
            def _():
                halos[n][:, 1] = jnp.zeros_like(halos[n][:, 1])

    def remote(src, dst, send_sem, recv_sem, shifts):
        return pltpu.make_async_remote_copy(
            src_ref=src,
            dst_ref=dst,
            send_sem=send_sem,
            recv_sem=recv_sem,
            device_id={a: other(a, d) for a, d in shifts.items()},
            device_id_type=pl.DeviceIdType.MESH,
        )

    def wait_bytes(ref, sem):
        pltpu.make_async_copy(ref, ref, sem).wait()

    def halo_copies(k, n):
        sources = (
            (v.at[k, :, CX - 1], v.at[k, :, 0]),
            (sy.at[k, 0], sy.at[k, 1]),
            (sz.at[k, 0], sz.at[k, 1]),
        )
        a = AXES[n]
        return [
            remote(
                sources[n][side],
                halos[n].at[k, side],
                sent,
                halo_recv.at[k % 2, n],
                {a: d},
            )
            for side, d in ((0, 1), (1, sizes[a] - 1))
        ]

    def on_halos(k, n, there, act):
        for copy, edge in zip(halo_copies(k, n), there[n]):

            @pl.when(jnp.logical_not(edge))
            def _():
                act(copy)

    going = list(zip(high_edge, low_edge))

    def w_copy(k, d):
        src, dst = (w.at[0], wfirst.at[d - 1]) if k == 0 else (wsend.at[k, d - 1], wrecv.at[k, d - 1])
        return remote(src, dst, sent, w_recv.at[k % 2], {"ea": d})

    def t_copy(k, d):
        src = tsend.at[k, other("ea", d)]
        return remote(src, trecv.at[k, d - 1], sent, t_recv.at[k % 2], {"ea": d})

    def node_copy(d):
        return remote(
            node_rows.at[other("ea", d)], their_nodes.at[d - 1], sent, node_recv, {"ea": d}
        )

    lane = iota((CY, CZ), 1)
    row = iota((CY, CZ), 0)

    half = iota((8, CZ), 1)

    def turned(tile, by):
        return pltpu.roll(tile, by % CZ, 1) if by % CZ else tile

    def pack_rows(k):
        for g in range(FACES):
            i, x = divmod(g, CX)
            sy[k, 0, pl.ds(g, 1), :] = v[k, i, x, pl.ds(CY - 1, 1), :]
            sy[k, 1, pl.ds(g, 1), :] = v[k, i, x, pl.ds(0, 1), :]

    def pack_lanes(k):
        last = jnp.zeros((8, CZ), F32)
        first = jnp.zeros((8, CZ), F32)
        for g in range(FACES):
            i, x = divmod(g, CX)
            for top in (0, 1):
                tile = v[k, i, x, pl.ds(8 * top, 8), :]
                at = g + FACES * top
                last = jnp.where(half == at, turned(tile, at + 1), last)
                first = jnp.where(half == at, turned(tile, at), first)
        sz[k, 0] = last
        sz[k, 1] = first

    def unpacked(faces, g, to):
        return jnp.concatenate(
            [turned(faces, to - g - FACES * top) for top in (0, 1)], axis=0
        )

    def terms_for_nodes(k):
        both_parts = jnp.concatenate(two_parts(v[k].reshape(COMP * ROWS, CZ)), axis=1)
        spread = [dot_nn(both_parts, gather_hot[n]) for n in range(OWNERS // 2)]
        for o in range(OWNERS):
            cols = slice(o % 2 * CAP, (o % 2 + 1) * CAP)
            term = jnp.zeros((EPAD, CAP), F32)
            for i in range(COMP):
                rows = spread[o // 2][i * ROWS : (i + 1) * ROWS, cols]
                picked = jnp.sum(rows * row_mask[o], axis=0, keepdims=True)
                term = term + weights[o, i] * picked
            tsend[k, o] = term
        return tsend[k, ea]

    def own_terms(term):
        both = dot_nt(jnp.concatenate(two_parts(term), axis=0), node_hot[ea])
        return both[:EPAD] + both[EPAD:]

    def values_at(values, hot):
        both = dot_nn(jnp.concatenate(two_parts(values), axis=0), hot)
        return both[:EPAD] + both[EPAD:]

    def terms_for_cells(k, distances):
        owners = {d: other("ea", OWNERS - d) for d in distances}
        value = {}
        for d in distances:
            if d == 0:
                value[d] = values_at(w[k], node_hot[ea])
            elif k == 0:
                value[d] = values_at(wfirst[d - 1], node_hot[owners[d]])
            else:
                value[d] = wrecv[k, d - 1]
        for d in distances:
            hot = row_hot[owners[d]]
            for i in range(COMP):
                total = jnp.sum(weights[owners[d], i] * value[d], axis=0, keepdims=True)
                for part, piece in enumerate(two_parts(jnp.broadcast_to(total, (CY, CAP)))):
                    for x in range(CX):
                        spread_rows[d, i, x, :, part * CAP : (part + 1) * CAP] = (
                            hot[x * CY : (x + 1) * CY] * piece
                        )
        added = sum(
            dot_nt(spread_rows[d].reshape(COMP * ROWS, 2 * CAP), scatter_hot[owners[d]])
            for d in distances
        )
        return added.reshape(COMP, CX, CY, CZ)

    def inner_part(k):
        for i in range(COMP):
            for x in range(CX):
                tile = v[k, i, x]
                beside = jnp.where(row > 0, pltpu.roll(tile, 1, 0), 0.0)
                beside += jnp.where(row < CY - 1, pltpu.roll(tile, CY - 1, 0), 0.0)
                beside += jnp.where(lane > 0, pltpu.roll(tile, 1, 1), 0.0)
                beside += jnp.where(lane < CZ - 1, pltpu.roll(tile, CZ - 1, 1), 0.0)
                if x > 0:
                    beside += v[k, i, x - 1]
                if x < CX - 1:
                    beside += v[k, i, x + 1]
                acc[i, x] = ((shift[x] + (6.0 - CENTER)) * tile - beside) * INV

    def outer_part(k, target):
        low_z, high_z = hz[k, 0], hz[k, 1]
        for i in range(COMP):
            for x in range(CX):
                g = i * CX + x
                beside = jnp.where(row == 0, hy[k, 0, pl.ds(g, 1), :], 0.0)
                beside += jnp.where(row == CY - 1, hy[k, 1, pl.ds(g, 1), :], 0.0)
                beside += jnp.where(lane == 0, unpacked(low_z, g, 0), 0.0)
                beside += jnp.where(lane == CZ - 1, unpacked(high_z, g, CZ - 1), 0.0)
                if x == 0:
                    beside += hx[k, 0, i]
                if x == CX - 1:
                    beside += hx[k, 1, i]
                target[i, x] = acc[i, x] - beside * INV

    def fold_v(left, right):
        return jnp.sum((left * right).reshape(FACES * CY // 8, 8, CZ), axis=0)

    def fold_w(prod):
        return prod[0:8, 0:128] + prod[0:8, 128:256] + prod[8:16, 0:128] + prod[8:16, 128:256]

    def local_product(j, k):
        return fold_v(v[j], v[k]) + fold_w(w[j] * w[k])

    with scope("tables_wait"):
        wait_bytes(slots, in_sem.at[0])
    with scope("tables"):
        for o in range(OWNERS):
            cells = slots[0, 0, o : o + 1, :]
            nodes = slots[1, 0, o : o + 1, :]
            node_rows[o] = nodes
            hot = (iota((CZ, CAP), 0) == jnp.bitwise_and(cells, CZ - 1)).astype(F32).astype(BF16)
            cols = slice(o % 2 * CAP, (o % 2 + 1) * CAP)
            gather_hot[o // 2, 0:CZ, cols] = hot
            gather_hot[o // 2, CZ : 2 * CZ, cols] = hot
            scatter_hot[o, :, 0:CAP] = hot
            scatter_hot[o, :, CAP : 2 * CAP] = hot
            mask = (iota((ROWS, CAP), 0) == lax.shift_right_logical(cells, 7)).astype(F32)
            row_mask[o] = mask
            row_hot[o] = mask.astype(BF16)
            node_hot[o] = (
                (iota((ENB, CAP), 0) == nodes).astype(F32).astype(BF16)
            )

    with scope("vw_wait"):
        loads["v"].wait()
        loads["w"].wait()
    with scope("pack_0"):
        for k in range(ITERS + 1):
            w[k, 8:16, :] = jnp.zeros((8, ENB), F32)
        w[0, 0:ECOMP, :] = w_first[...]
        pack_rows(0)
        pack_lanes(0)
    with scope("weights"):
        loads["coup"].wait()
        needed = jnp.where(iota((ECOMP, CAP), 0) < 3, 1, 2)
        for o in range(OWNERS):
            live = slots[2, 0, o : o + 1, :] >= needed
            for i in range(COMP):
                weights[o, i, 8:16] = jnp.zeros((8, CAP), F32)
                weights[o, i, 0:ECOMP] = jnp.where(
                    live, coup[i, :, o * CAP : (o + 1) * CAP] * INV, 0.0
                )
    with scope("nodes_0"):
        own = terms_for_nodes(0)
    with scope("barrier_wait"):
        pl.semaphore_wait(barrier, len(first))

    def send_halos(k, axes=(2, 1, 0)):
        for n in axes:
            on_halos(k, n, going, lambda copy: copy.start())

    def wait_halos(k):
        for n in range(3):
            sem = halo_recv.at[k % 2, n]
            low, high = low_edge[n], high_edge[n]

            @pl.when(jnp.logical_not(jnp.logical_or(low, high)))
            def _():
                wait_bytes(halos[n].at[k], sem)

            @pl.when(low)
            def _():
                wait_bytes(halos[n].at[k, 1], sem)

            @pl.when(high)
            def _():
                wait_bytes(halos[n].at[k, 0], sem)

    def send_terms(k):
        for d in (2, 1, 3):
            t_copy(k, d).start()

    def send_w(k):
        if k > 0:
            values = values_at(w[k], their_hot[...])
            for d in (2, 1, 3):
                wsend[k, OWNERS - d - 1] = values[:, (d - 1) * CAP : d * CAP]
        for d in (2, 1, 3):
            w_copy(k, d).start()

    def stiff_times(k):
        out = own_terms(own)[0:ECOMP]
        for q in range(ECOMP):
            out = out + stiff[q] * w[k, pl.ds(q, 1), :]
        return out

    def next_w(k, pushed):
        wait_bytes(trecv.at[k], t_recv.at[k % 2])
        pieces = [two_parts(trecv[k, d]) for d in range(OWNERS - 1)]
        rows = [jnp.concatenate([p[n] for p in pieces], axis=1) for n in (0, 1)]
        both = dot_nt(jnp.concatenate(rows, axis=0), their_hot[...])
        came[...] = both[:EPAD] + both[EPAD:]
        w[k + 1, 0:ECOMP, :] = pushed + came[0:ECOMP]

    def wait_w(k):
        wait_bytes(wfirst if k == 0 else wrecv.at[k], w_recv.at[k % 2])

    def next_v(k):
        with scope(f"w_wait_{k}"):
            wait_w(k)
        with scope(f"cells_{k}"):
            acc[...] += terms_for_cells(k, (1, 3, 2))
        if k == 1:
            with scope("token_2"):
                wait_token(1)
                send_token(2)
        with scope(f"halo_wait_{k}"):
            wait_halos(k)
        with scope(f"outer_{k}"):
            outer_part(k, v.at[k + 1])

    parts = [None] * (MOMENTS - 1)
    last = ITERS - 1

    with scope("send_0"):
        for d in (2, 1, 3):
            node_copy(d).start()
        send_halos(0)
        send_terms(0)
        send_w(0)
        send_token(0)
    with scope("inner_0"):
        loads["shift"].wait()
        inner_part(0)
    with scope("stiff"):
        loads["diag"].wait()
        loads["off"].wait()
        comp = iota((ECOMP, ENB), 0)
        for q in range(ECOMP):
            both = (off[q] + off[:, q, :]) * (0.5 * INV)
            stiff[q] = jnp.where(comp == q, (diag[...] - CENTER) * INV, both)
    with scope("pushed_0"):
        pushed = stiff_times(0)
        parts[0] = local_product(0, 0)
        acc[...] += terms_for_cells(0, (0,))
    with scope("their_nodes"):
        wait_bytes(their_nodes, node_recv)
        for d in range(OWNERS - 1):
            their_hot[:, d * CAP : (d + 1) * CAP] = (
                (iota((ENB, CAP), 0) == their_nodes[d]).astype(F32).astype(BF16)
            )
    with scope("w_next_0"):
        next_w(0, pushed)
        send_w(1)
    with scope("token_1"):
        wait_token(0)
        send_token(1)
    next_v(0)

    with scope("pack_1"):
        pack_rows(1)
        send_halos(1, (1, 0))
        pack_lanes(1)
        send_halos(1, (2,))
    with scope("nodes_1"):
        own = terms_for_nodes(1)
        send_terms(1)
    with scope("inner_1"):
        inner_part(1)
        parts[1] = local_product(0, 1)
        parts[2] = local_product(1, 1)
        acc[...] += terms_for_cells(1, (0,))
        pushed = stiff_times(1)
    next_v(1)

    with scope("nodes_2"):
        pack_rows(2)
        pack_lanes(2)
        own = terms_for_nodes(2)
        send_terms(2)
        send_halos(2)
    with scope("w_next_1"):
        next_w(1, pushed)
        send_w(2)
    with scope("inner_2"):
        inner_part(2)
        parts[3] = local_product(1, 2)
        parts[4] = local_product(2, 2)
        own_node_terms = own_terms(own)
        pushed = stiff_times(2)
        at = iota((8, 128), 1)
        tile = jnp.zeros((8, 128), F32)
        for m in range(MOMENTS - 1):
            tile = jnp.where(at == m, jnp.sum(parts[m], axis=1, keepdims=True), tile)
    with scope("halo_wait_2"):
        wait_halos(2)
    with scope("outer_2"):
        outer_part(2, acc)
        final = fold_v(v[last], acc[...])
    with scope("w_next_2"):
        next_w(2, pushed)

    with scope("moments"):
        twice = own_node_terms + came[...]
        final = final + fold_w(w[last] * (w[last + 1] + twice))
        tile = jnp.where(at == MOMENTS - 1, jnp.sum(final, axis=1, keepdims=True), tile)
        total = jnp.sum(tile, axis=0, keepdims=True)

    def send_total(buf, at, recv_sem, group):
        mine = buf.at[at]
        mine[...] = total
        copies = [
            remote(mine, mine, sent, recv_sem, shifts)
            for shifts in group
        ]
        for copy in copies:
            copy.start()
        return buf.at[pl.ds(0, len(group))]

    with scope("token_end"):
        wait_token(TOKENS - 1)
    with scope("line_send"):
        on_line = send_total(red_line, me["gx"], line_recv, line)
    with scope("cells_last"):
        wait_w(last)
        v[last + 1] = acc[...] + terms_for_cells(last, (0, 1, 3, 2))
    with scope("out_send"):
        out = [
            pltpu.make_async_copy(v, v_out, sent),
            pltpu.make_async_copy(w, w_out, sent),
        ]
        for copy in out:
            copy.start()
    with scope("line_wait"):
        wait_bytes(on_line, line_recv)
        total = jnp.sum(red_line[...], axis=0)
    with scope("plane_send"):
        on_plane = send_total(
            red_plane, me["gy"] * sizes["ea"] + ea, plane_recv, plane
        )
    with scope("plane_wait"):
        wait_bytes(on_plane, plane_recv)
        moments[...] = jnp.sum(red_plane[...], axis=0)
    with scope("ends"):
        for n in range(3):
            for side, edge in enumerate(going[n]):

                @pl.when(jnp.logical_not(edge))
                def _():
                    wait_bytes(halos[n].at[:, side], sent)

        for ref in (their_nodes, wfirst, wrecv.at[pl.ds(1, ITERS - 1)], trecv, on_line, on_plane, v, w):
            wait_bytes(ref, sent)


def combine(v, w_all, moments, sol_v, res_v, sol_w, res_w):
    total = moments[...]
    flat = iota((1, 128), 1)
    mu = [
        jnp.broadcast_to(
            jnp.sum(jnp.where(flat == m, total, 0.0), axis=1, keepdims=True), (1, 128)
        )
        for m in range(MOMENTS)
    ]

    def form(left, right):
        out = None
        for i, p in enumerate(left):
            for j, q in enumerate(right):
                term = p * q * mu[i + j]
                out = term if out is None else out + term
        return out

    zero = jnp.zeros((1, 128), F32)
    sol, res, way = [zero] * ITERS, [zero + 1.0] + [zero] * ITERS, [zero + 1.0]
    norm = mu[0]
    for it in range(ITERS):
        image = [zero] * (it + 2)
        for j, p in enumerate(way):
            image[j] = image[j] + CENTER * p
            image[j + 1] = image[j + 1] + SPREAD * p
        alpha = norm / form(way, image)
        for j, p in enumerate(way):
            sol[j] = sol[j] + alpha * p
        for j, p in enumerate(image):
            res[j] = res[j] - alpha * p
        if it + 1 < ITERS:
            norm_next = form(res[: it + 2], res[: it + 2])
            ratio = norm_next / norm
            way = [res[j] + (ratio * way[j] if j < len(way) else 0.0) for j in range(it + 2)]
            norm = norm_next

    for i in range(COMP):
        for x in range(CX):
            b = [v[k, i, x] for k in range(ITERS + 1)]
            sol_v[i, x] = sum(sol[k] * b[k] for k in range(ITERS))
            res_v[i, x] = sum(res[k] * b[k] for k in range(ITERS + 1))
    spread = [
        (jnp.concatenate([sol[k]] * 2, axis=1) if k < ITERS else None,
         jnp.concatenate([res[k]] * 2, axis=1))
        for k in range(ITERS + 1)
    ]
    b = [w_all[k, 0:ECOMP, :] for k in range(ITERS + 1)]
    sol_w[...] = sum(spread[k][0] * b[k] for k in range(ITERS))
    res_w[...] = sum(spread[k][1] * b[k] for k in range(ITERS + 1))


def body(sizes, *args):
    v_in, w_in = args[0], args[1]
    vmem, dma = pltpu.VMEM, pltpu.SemaphoreType.DMA
    steps = ITERS
    basis = pl.pallas_call(
        functools.partial(kernel, sizes),
        name="krylov",
        out_shape=(
            vmem((steps + 1, COMP, CX, CY, CZ), F32),
            vmem((steps + 1, EPAD, ENB), F32),
            vmem((1, 128), F32),
        ),
        in_specs=[pl.BlockSpec(memory_space=pl.ANY)] * len(args),
        out_specs=[pl.BlockSpec(memory_space=pl.ANY)] * 2
        + [pl.BlockSpec(memory_space=pltpu.VMEM)],
        scratch_shapes=[
            vmem((steps + 1, COMP, CX, CY, CZ), F32),
            vmem((steps + 1, EPAD, ENB), F32),
            vmem((ECOMP, ENB), F32),
            vmem((CX, CY, CZ), F32),
            vmem((ECOMP, ENB), F32),
            vmem((ECOMP, ECOMP, ENB), F32),
            vmem((COMP, ECOMP, SLOTS), F32),
            vmem((3, 1, OWNERS, CAP), jnp.int32),
            vmem((OWNERS, 1, CAP), jnp.int32),
            vmem((OWNERS - 1, 1, CAP), jnp.int32),
            vmem((ENB, (OWNERS - 1) * CAP), BF16),
            vmem((COMP, CX, CY, CZ), F32),
            vmem((OWNERS, COMP, EPAD, CAP), F32),
            vmem((ECOMP, ECOMP, ENB), F32),
            vmem((OWNERS // 2, 2 * CZ, 2 * CAP), BF16),
            vmem((OWNERS, CZ, 2 * CAP), BF16),
            vmem((OWNERS, ROWS, CAP), BF16),
            vmem((OWNERS, ROWS, CAP), F32),
            vmem((OWNERS, ENB, CAP), BF16),
            vmem((OWNERS, COMP, CX, CY, 2 * CAP), BF16),
            vmem((steps, OWNERS - 1, EPAD, CAP), F32),
            vmem((steps, OWNERS - 1, EPAD, CAP), F32),
            vmem((OWNERS - 1, EPAD, ENB), F32),
            vmem((steps, OWNERS, EPAD, CAP), F32),
            vmem((steps, OWNERS - 1, EPAD, CAP), F32),
            vmem((EPAD, ENB), F32),
            vmem((steps, 2, COMP, CY, CZ), F32),
            vmem((steps, 2, 16, CZ), F32),
            vmem((steps, 2, 8, CZ), F32),
            vmem((steps, 2, 16, CZ), F32),
            vmem((steps, 2, 8, CZ), F32),
            vmem((sizes["gx"], 1, 128), F32),
            vmem((sizes["gy"] * sizes["ea"], 1, 128), F32),
            pltpu.SemaphoreType.REGULAR((TOKENS,)),
            dma((7,)),
            dma,
            dma,
            dma((2, 3)),
            dma((2,)),
            dma((2,)),
            dma,
            dma,
        ],
        compiler_params=pltpu.CompilerParams(collective_id=0, has_side_effects=True),
    )(*args)
    return pl.pallas_call(
        combine,
        name="combine",
        out_shape=(
            jax.ShapeDtypeStruct(v_in.shape, F32),
            jax.ShapeDtypeStruct(v_in.shape, F32),
            jax.ShapeDtypeStruct(w_in.shape, F32),
            jax.ShapeDtypeStruct(w_in.shape, F32),
        ),
        in_specs=[pl.BlockSpec(memory_space=pltpu.VMEM)] * 3,
        out_specs=[pl.BlockSpec(memory_space=pltpu.VMEM)] * 4,
        compiler_params=pltpu.CompilerParams(vmem_limit_bytes=VMEM_LIMIT),
    )(*(pltpu.with_memory_space_constraint(b, pltpu.VMEM) for b in basis))


def solution(mesh):
    sizes = {a: mesh.shape[a] for a in AXES}
    return jax.shard_map(
        functools.partial(body, sizes),
        mesh=mesh,
        in_specs=(
            P(None, "gx", "gy", "ea"),
            P(None, GX_GY_EA),
            P("gx", "gy", "ea"),
            P(None, GX_GY_EA),
            P(None, None, GX_GY_EA),
            P(None, None, GX_GY_EA),
            P(GX_GY_EA, None, None),
            P(GX_GY_EA, None, None),
            P(GX_GY_EA, None, None),
        ),
        out_specs=(
            P(None, "gx", "gy", "ea"),
            P(None, "gx", "gy", "ea"),
            P(None, GX_GY_EA),
            P(None, GX_GY_EA),
        ),
        check_vma=False,
    )
```
